128 devices in a mesh: gx: 16 (over z_lo, x, core), gy: 8 (over y, z_hi).
Axes of the slice: x: 4, y: 4, z: 4 (z_hi: 2, z_lo: 2; z = z_hi * 2 + z_lo), core: 2. Of those that a mesh axis runs over, the one named last changes fastest.
Arguments:
- pair_in: bfloat16 [1024, 1024, 128], P(('gx', 'gy')), may hold values from -6 to 6
- residue_mask: int32 [1024], P(('gx', 'gy')), may hold values 0 or 1
- norm_start: float32 [128], replicated, may hold values from 0.25 to 1.75
- proj_start: bfloat16 [128, 512], replicated, may hold values from -0.5 to 0.5
- gate_bias_start: float32 [128], replicated, may hold values from -4 to 4
- bias_w_start: bfloat16 [128, 4], replicated, may hold values from -1.5 to 1.5
- out_w_start: bfloat16 [128, 128], replicated, may hold values from -1 to 1
- norm_end: float32 [128], replicated, may hold values from 0.25 to 1.75
- proj_end: bfloat16 [128, 512], replicated, may hold values from -0.5 to 0.5
- gate_bias_end: float32 [128], replicated, may hold values from -4 to 4
- bias_w_end: bfloat16 [128, 4], replicated, may hold values from -1.5 to 1.5
- out_w_end: bfloat16 [128, 128], replicated, may hold values from -1 to 1
- norm_trans: float32 [128], replicated, may hold values from 0.25 to 1.75
- trans_in: bfloat16 [128, 512], replicated, may hold values from -0.5 to 0.5
- trans_bias: float32 [512], replicated, may hold values from -4 to 4
- trans_out: bfloat16 [512, 128], replicated, may hold values from -0.375 to 0.375
Outputs:
- pair_out: bfloat16 [1024, 1024, 128], P(('gx', 'gy'))
The draws below stay inside these ranges and needn't reach their ends.
Inputs may be any that keep to these rules, and one draw needn't show every extreme that they name: residue_mask holds only 0 and 1.
All inputs are finite; a program needn't handle non-finite values.
Results may differ from the reference program's by a relative error of at most 0.02.
Values may be sent and summed in bfloat16 or wider, within the bound.
A program may use at most 192 MiB of HBM per device.

```python
import jax
import jax.numpy as jnp
from jax import lax

C = 128
HEADS = 4
HEAD_DIM = 32
FFN = 512
RES = 1024


def with_ends(array, key, smallest, top_value):
    place = [jax.random.randint(jax.random.fold_in(key, axis), (), 0, length) for axis, length in enumerate(array.shape)]
    longest = array.shape.index(max(array.shape))
    next_to = place[:longest] + [(place[longest] + 1) % array.shape[longest]] + place[longest + 1:]
    return array.at[tuple(place)].set(smallest).at[tuple(next_to)].set(top_value)


def block_scale(own_key, shape, split, least, high):
    loudness = 1.0
    for position, shards_of in split:
        steps = jax.random.uniform(jax.random.fold_in(jax.random.fold_in(own_key, 6), position), (shards_of,), jnp.float32, least / len(split), high / len(split))
        loudness = loudness * jnp.repeat(jnp.exp(steps), shape[position] // shards_of).reshape((-1,) + (1,) * (len(shape) - 1 - position))
    return loudness


def scatter_about(own_key, extent, deviation, bound, pieces=(), held_as=jnp.bfloat16):
    values = jax.random.normal(own_key, extent, jnp.float32) * deviation
    if len(pieces) > 0:
        values = block_scale(own_key, extent, pieces, -0.22, 0.18) * values
    return jnp.clip(values, min=-bound, max=bound).astype(held_as)


def setup_inputs(seed: int = 0) -> dict:
    streams_of = jax.random.split(jax.random.key(seed), 17)
    return {
        "pair_in": scatter_about(streams_of[0], (RES, RES, C), 1.0, 6.0, ((0, 128),)),
        "residue_mask": with_ends((jax.random.randint(streams_of[1], (RES,), 0, 8) < 7).astype(jnp.int32), jax.random.fold_in(streams_of[1], 1), 0, 1),
        "norm_start": jnp.clip(1.0 + 0.15 * jax.random.normal(streams_of[2], (C,), jnp.float32), 0.25, 1.75),
        "proj_start": scatter_about(streams_of[3], (C, 4 * C), C ** -0.5, 0.5),
        "gate_bias_start": scatter_about(streams_of[4], (C,), 1.0, 4.0, (), jnp.float32),
        "bias_w_start": scatter_about(streams_of[5], (C, HEADS), (C // 8) ** -0.5, 1.5),
        "out_w_start": scatter_about(streams_of[6], (C, C), (C // 4) ** -0.5, 1.0),
        "norm_end": jnp.clip(1.0 + 0.15 * jax.random.normal(streams_of[7], (C,), jnp.float32), 0.25, 1.75),
        "proj_end": scatter_about(streams_of[8], (C, 4 * C), C ** -0.5, 0.5),
        "gate_bias_end": scatter_about(streams_of[9], (C,), 1.0, 4.0, (), jnp.float32),
        "bias_w_end": scatter_about(streams_of[10], (C, HEADS), (C // 8) ** -0.5, 1.5),
        "out_w_end": scatter_about(streams_of[11], (C, C), (C // 4) ** -0.5, 1.0),
        "norm_trans": jnp.clip(1.0 + 0.15 * jax.random.normal(streams_of[12], (C,), jnp.float32), 0.25, 1.75),
        "trans_in": scatter_about(streams_of[13], (C, FFN), C ** -0.5, 0.5),
        "trans_bias": scatter_about(streams_of[14], (FFN,), 1.0, 4.0, (), jnp.float32),
        "trans_out": scatter_about(streams_of[15], (FFN, C), (FFN // 2) ** -0.5, 0.375),
    }


big_negative = 1000000000.0

def layer_norm(values, norm_gain):
    widened = values.astype(jnp.float32)
    row_mean = lax.optimization_barrier(jnp.mean(widened, axis=-1, keepdims=True))
    row_var = lax.optimization_barrier(jnp.mean(jnp.square(widened - row_mean), axis=-1, keepdims=True))
    return ((widened - row_mean) * lax.rsqrt(row_var + 1e-05) * norm_gain).astype(jnp.bfloat16)

def project(normed, weight):
    flat = normed.reshape(-1, normed.shape[-1])
    result = jnp.dot(flat, weight, preferred_element_type=jnp.float32)
    return result.reshape(normed.shape[:-1] + (weight.shape[1],))

def split_heads(merged):
    return merged.astype(jnp.bfloat16).reshape(merged.shape[:-1] + (HEADS, HEAD_DIM))

def attend_block(query, keys, values, pair_bias, key_bias):
    score_scale = HEAD_DIM ** (-0.5)
    scores = jnp.einsum('jhd,khd->hjk', query.astype(jnp.float32), keys.astype(jnp.float32), precision=lax.Precision.HIGHEST)
    scores = scores * score_scale + pair_bias + key_bias
    attn_weights = jax.nn.softmax(scores, axis=-1)
    mixed = jnp.einsum('hjk,khd->jhd', attn_weights, values.astype(jnp.float32), precision=lax.Precision.HIGHEST)
    return mixed.reshape(query.shape[0], HEADS * HEAD_DIM)

def gated_residual(residual, mixed, gate_logit, gate_bias, out_weight):
    gated = (mixed * jax.nn.sigmoid(gate_logit + gate_bias)).astype(jnp.bfloat16)
    return (residual.astype(jnp.float32) + project(gated, out_weight)).astype(jnp.bfloat16)

def projections(normed, weight, channels):
    projected = project(normed, weight)
    query = split_heads(projected[..., :channels])
    keys = split_heads(projected[..., channels:2 * channels])
    values = split_heads(projected[..., 2 * channels:3 * channels])
    return (query, keys, values, projected[..., 3 * channels:])

def reference(pair_in, residue_mask, norm_start, proj_start, gate_bias_start, bias_w_start, out_w_start, norm_end, proj_end, gate_bias_end, bias_w_end, out_w_end, norm_trans, trans_in, trans_bias, trans_out):
    channels = pair_in.shape[-1]
    key_bias = (residue_mask.astype(jnp.float32) - 1.0) * big_negative
    normed = layer_norm(pair_in, norm_start)
    query, keys, values, gate_logit = projections(normed, proj_start, channels)
    pair_bias = project(normed, bias_w_start).astype(jnp.bfloat16)
    start_bias = jnp.transpose(pair_bias, (2, 0, 1)).astype(jnp.float32)

    def per_row(operands):
        query_row, key_row, value_row = operands
        return attend_block(query_row, key_row, value_row, start_bias, key_bias)
    mixed = lax.map(per_row, (query, keys, values))
    after_start = gated_residual(pair_in, mixed, gate_logit, gate_bias_start, out_w_start)
    normed = layer_norm(after_start, norm_end)
    query, keys, values, gate_logit = projections(normed, proj_end, channels)
    pair_bias = project(normed, bias_w_end).astype(jnp.bfloat16)
    end_bias = jnp.transpose(pair_bias, (2, 1, 0)).astype(jnp.float32)

    def per_column(operands):
        query_col, key_col, value_col = operands
        return attend_block(query_col, key_col, value_col, end_bias, key_bias)
    mixed = lax.map(per_column, (jnp.swapaxes(query, 0, 1), jnp.swapaxes(keys, 0, 1), jnp.swapaxes(values, 0, 1)))
    mixed = jnp.swapaxes(mixed, 0, 1)
    after_end = gated_residual(after_start, mixed, gate_logit, gate_bias_end, out_w_end)
    normed = layer_norm(after_end, norm_trans)
    hidden = jax.nn.relu(project(normed, trans_in) + trans_bias).astype(jnp.bfloat16)
    return (after_end.astype(jnp.float32) + project(hidden, trans_out)).astype(jnp.bfloat16)
```

```python
import functools
import math

import jax
import jax.numpy as jnp
from jax import lax
from jax.experimental import pallas as pl
from jax.experimental.pallas import tpu as pltpu
from jax.sharding import PartitionSpec as P

HEADS = 4
HEAD_DIM = 32
BIG = 1000000000.0
LOG2E = math.log2(math.e)
QSCALE = HEAD_DIM ** (-0.5) * LOG2E
MESH = pl.DeviceIdType.MESH
F32 = jnp.float32
BF16 = jnp.bfloat16


def nn(a, b):
    return lax.dot_general(a, b, (((1,), (0,)), ((), ())), preferred_element_type=F32)


def nt(a, b):
    return lax.dot_general(a, b, (((1,), (1,)), ((), ())), preferred_element_type=F32)


def layer_norm(x, gain):
    mean = jnp.mean(x, axis=-1, keepdims=True)
    cent = x - mean
    var = jnp.mean(cent * cent, axis=-1, keepdims=True)
    return (cent * lax.rsqrt(var + 1e-05) * gain).astype(BF16)


def bias_rows(w, r, rows, normed):
    shape = (HEADS * rows, HEADS)
    place = lax.broadcasted_iota(jnp.int32, shape, 0) == (
        lax.broadcasted_iota(jnp.int32, shape, 1) * rows + r
    )
    spread = nn(place.astype(F32).astype(BF16), w).astype(BF16)
    return nt(spread, normed)


def attend_tile(tq, ck, t, q_ref, k_ref, v_ref, bias_ref, s_refs, finish):
    rows, res, ch = k_ref.shape
    lanes = pl.ds(pl.multiple_of(t * tq, tq), tq)
    chunks = res // ck

    def query(r, h):
        q = q_ref[r, :, lanes]
        row = lax.broadcasted_iota(jnp.int32, q.shape, 0)
        return jnp.where((row >= h * HEAD_DIM) & (row < (h + 1) * HEAD_DIM), q, jnp.zeros_like(q))

    def score(r, h, c, q, top):
        span = slice(c * ck, (c + 1) * ck)
        s = nn(k_ref[r, span, :], q) + bias_ref[h, span, lanes]
        s_refs[h % 2][span, :] = s
        m = jnp.max(s.reshape(ck // 8, 8, tq), axis=0)
        return m if top is None else jnp.maximum(top, m)

    def mix(r, h, c, top, acc):
        span = slice(c * ck, (c + 1) * ck)
        w = jnp.exp2((s_refs[h % 2][span, :] - top).astype(BF16))
        v = jnp.concatenate(
            [v_ref[r, h * HEAD_DIM : (h + 1) * HEAD_DIM, span], jnp.ones((16, ck), BF16)], axis=0
        )
        o = nn(v, w)
        return o if acc is None else acc + o

    q, top = query(0, 0), None
    for c in range(chunks):
        top = score(0, 0, c, q, top)

    def body(r, top):
        outs = []
        for h in range(HEADS):
            peak = jnp.max(top, axis=0, keepdims=True)
            nh = (h + 1) % HEADS
            nr = r if h < HEADS - 1 else jnp.minimum(r + 1, rows - 1)
            q, top, acc = query(nr, nh), None, None
            for c in range(chunks):
                top = score(nr, nh, c, q, top)
                acc = mix(r, h, c, peak, acc)
            outs.append(acc[:HEAD_DIM] / acc[HEAD_DIM : HEAD_DIM + 1])
        finish(r, lanes, jnp.concatenate(outs, axis=0))
        return top

    lax.fori_loop(0, rows, body, top)


def kernel(
    nx,
    ny,
    tq,
    ck,
    x_ref,
    mask_ref,
    g1_ref,
    w1_ref,
    gb1_ref,
    bw1_ref,
    ow1_ref,
    g2_ref,
    w2_ref,
    gb2_ref,
    bw2_ref,
    ow2_ref,
    g3_ref,
    ti_ref,
    tb_ref,
    to_ref,
    out_ref,
    q_ref,
    k_ref,
    v_ref,
    wt_ref,
    bias_ref,
    kb_ref,
    kc_ref,
    zs_ref,
    st_ref,
    rise_ref,
    sa_ref,
    sb_ref,
    recv_m,
    recv_a,
    recv_b,
    send_z,
    recv_z,
    recv_o,
    ssem,
    rsem,
    fsem,
    lsem,
):
    n = nx * ny
    rows, res, ch = x_ref.shape
    me = lax.axis_index("gx") * ny + lax.axis_index("gy")

    def peer_of(t):
        return lax.rem(me + t, n)

    def coords(p):
        return (p // ny, lax.rem(p, ny))


    def move(kind, src, dst, p, slot):
        return pltpu.make_async_remote_copy(
            src_ref=src,
            dst_ref=dst,
            send_sem=ssem.at[kind, slot],
            recv_sem=rsem.at[kind, slot],
            device_id=coords(p),
            device_id_type=MESH,
        )

    def share(kind, src, dst, p):
        return pltpu.make_async_remote_copy(
            src_ref=src,
            dst_ref=dst,
            send_sem=ssem.at[kind, p],
            recv_sem=rsem.at[kind, me],
            device_id=coords(p),
            device_id_type=MESH,
        )

    gx, gy = lax.axis_index("gx"), lax.axis_index("gy")
    a_ref = out_ref
    core = lax.rem(gx, 2)
    half = nx // 2
    partner = (gx + 1 - 2 * core) * ny + gy

    def line_peer(t):
        return gx * ny + lax.rem(gy + t, ny)

    def plane_peer(t):
        return (lax.rem(gx // 2 + t, half) * 2 + core) * ny + gy

    barrier = pltpu.get_barrier_semaphore()

    def greet(p):
        pl.semaphore_signal(barrier, inc=1, device_id=coords(p), device_id_type=MESH)

    for t in range(1, ny):
        greet(line_peer(t))
    for t in range(1, half):
        greet(plane_peer(t))
    greet(partner)

    def relay(kind, buf, t, s):
        @pl.loop(1, half)
        def _(u):
            q = plane_peer(u)
            pltpu.make_async_remote_copy(
                src_ref=buf.at[s],
                dst_ref=buf.at[s],
                send_sem=fsem.at[kind, t, u],
                recv_sem=rsem.at[kind, s],
                device_id=coords(q),
                device_id_type=MESH,
            ).start()

        hand(kind, buf, s).start()

    def hand(kind, buf, s):
        return move(kind, buf.at[s], buf.at[s], partner, s)

    def gather_start(kind, buf):
        @pl.loop(1, ny)
        def _(t):
            p = line_peer(t)
            pltpu.make_async_remote_copy(
                src_ref=buf.at[me],
                dst_ref=buf.at[me],
                send_sem=lsem.at[kind, t],
                recv_sem=rsem.at[kind, me],
                device_id=coords(p),
                device_id_type=MESH,
            ).start()

        relay(kind, buf, 0, me)

    def gather_finish(kind, buf):
        @pl.loop(1, ny)
        def _(t):
            p = line_peer(t)
            move(kind, buf.at[p], buf.at[p], p, p).wait_recv()
            relay(kind, buf, t, p)

        @pl.loop(0, ny)
        def _(t):
            @pl.loop(1, half)
            def _(u):
                s = plane_peer(u) - gy + lax.rem(gy + t, ny)
                move(kind, buf.at[s], buf.at[s], partner, s).wait_recv()
                hand(kind, buf, s).start()

        @pl.loop(0, ny)
        def _(t):
            @pl.loop(0, half)
            def _(u):
                s = plane_peer(u) - gy + lax.rem(gy + t, ny)
                o = s + (1 - 2 * core) * ny
                move(kind, buf.at[o], buf.at[o], partner, o).wait_recv()
                hand(kind, buf, s).wait_send()

            @pl.loop(1, half)
            def _(u):
                pltpu.make_async_remote_copy(
                    src_ref=buf.at[me],
                    dst_ref=buf.at[me],
                    send_sem=fsem.at[kind, t, u],
                    recv_sem=rsem.at[kind, me],
                    device_id=coords(partner),
                    device_id_type=MESH,
                ).wait_send()

        @pl.loop(1, ny)
        def _(t):
            pltpu.make_async_remote_copy(
                src_ref=buf.at[me],
                dst_ref=buf.at[me],
                send_sem=lsem.at[kind, t],
                recv_sem=rsem.at[kind, me],
                device_id=coords(partner),
                device_id_type=MESH,
            ).wait_send()

    per = tq // rows

    def spread_tile(kind, src, dst, t):
        @pl.loop(0, per)
        def _(u):
            p = t * per + lax.rem(me + u, per)

            @pl.when(p != me)
            def _():
                share(kind, src.at[p], dst.at[me], p).start()

    def spread_finish(kind, src, dst):
        @pl.loop(1, n)
        def _(t):
            p = peer_of(t)
            move(kind, src.at[p], dst.at[p], p, p).wait()

    lane = lax.broadcasted_iota(jnp.int32, (16, 128), 1)
    vec = jnp.zeros((16, 128), F32)
    for t in range(rows):
        vec = jnp.where(lane == lax.rem(me * rows, 128) + t, mask_ref[t].astype(F32), vec)
    recv_m[me] = vec.astype(BF16)

    def norm_row(r, acc):
        normed = layer_norm(x_ref[r].astype(F32), g1_ref[...])
        a_ref[r] = normed
        return acc + bias_rows(bw1_ref[...], r, rows, normed)

    acc = lax.fori_loop(0, rows, norm_row, jnp.zeros((HEADS * rows, res), F32))
    recv_a[me] = acc.astype(BF16)

    pl.semaphore_wait(barrier, ny + half - 1)

    gather_start(2, recv_m)
    gather_start(0, recv_a)

    def turn_weights(w_ref):
        wt_ref[...] = w_ref[...].astype(F32).T.astype(BF16)

    def project(r, normed, w_ref):
        k_ref[r] = nn(normed, w_ref[:, ch : 2 * ch]).astype(BF16)
        q_ref[r] = (nt(wt_ref[:ch], normed) * QSCALE).astype(BF16)
        v_ref[r] = nt(wt_ref[2 * ch : 3 * ch], normed).astype(BF16)

    def gate(r, lanes, o, gb_ref):
        gl = nt(wt_ref[3 * ch :], a_ref[r, lanes, :])
        return (o * jax.nn.sigmoid(gl + gb_ref[...])).T.astype(BF16)

    turn_weights(w1_ref)

    def project_row(r, carry):
        project(r, a_ref[r], w1_ref)
        return carry

    lax.fori_loop(0, rows, project_row, 0)

    gather_finish(2, recv_m)

    kd = 128 // rows
    for t in range(res // 128):
        mask = jnp.sum(recv_m[t * kd : (t + 1) * kd].astype(F32), axis=0)[:1]
        kb = (mask - 1.0) * BIG
        kb_ref[:, t * 128 : (t + 1) * 128] = kb
        kc_ref[t * 128 : (t + 1) * 128, :] = jnp.broadcast_to(kb, (128, 128)).T

    gather_finish(0, recv_a)

    def start_bias(g, carry):
        block = recv_a[pl.ds(g * kd, kd)].astype(F32)
        for h in range(HEADS):
            part = block[:, h * rows : (h + 1) * rows, :].reshape(128, res)
            bias_ref[h, :, pl.ds(pl.multiple_of(g * 128, 128), 128)] = (
                (part + kb_ref[...]) * LOG2E
            ).T
        return carry

    lax.fori_loop(0, res // 128, start_bias, 0)

    def stage(r, z):
        st_ref[:, pl.ds(pl.multiple_of(r * rows, rows), rows), :] = z.reshape(per, rows, ch)

    def start_finish(r, lanes, o):
        z1 = x_ref[r, lanes, :].astype(F32) + nn(gate(r, lanes, o, gb1_ref), ow1_ref[...])
        z1 = z1.astype(BF16).astype(F32)
        stage(r, z1)
        rise_ref[...] = rise_ref[...] + bias_rows(
            bw2_ref[...], r, rows, layer_norm(z1, g2_ref[...])
        )

    def start_tile(t, carry):
        rise_ref[...] = jnp.zeros_like(rise_ref)
        attend_tile(tq, ck, t, q_ref, k_ref, v_ref, bias_ref, (sa_ref, sb_ref), start_finish)
        recv_b[me, :, pl.ds(pl.multiple_of(t * tq, tq), tq)] = rise_ref[...].astype(BF16)
        send_z[pl.ds(t * per, per)] = st_ref[...].astype(BF16)
        spread_tile(3, send_z, recv_z, t)
        return carry

    lax.fori_loop(0, res // tq, start_tile, 0)
    recv_z[me] = send_z[me]
    gather_start(1, recv_b)
    turn_weights(w2_ref)
    spread_finish(3, send_z, recv_z)

    def end_project(d, carry):
        z1 = zs_ref[:, pl.ds(d, rows, stride=rows), :].reshape(res, ch)
        normed = layer_norm(z1, g2_ref[...])
        a_ref[d] = normed
        project(d, normed, w2_ref)
        return carry

    zs_ref[...] = recv_z[...].astype(F32)
    lax.fori_loop(0, rows, end_project, 0)
    gather_finish(1, recv_b)

    def end_bias(g, carry):
        block = recv_b[pl.ds(g * kd, kd)].astype(F32)
        keys = pl.ds(pl.multiple_of(g * 128, 128), 128)
        kc = kc_ref[keys, :]
        for h in range(HEADS):
            part = block[:, h * rows : (h + 1) * rows, :].reshape(128, res)
            for t in range(res // 128):
                span = slice(t * 128, (t + 1) * 128)
                bias_ref[h, keys, span] = (part[:, span] + kc) * LOG2E
        return carry

    lax.fori_loop(0, res // 128, end_bias, 0)

    def end_tile(t, carry):
        def end_finish(r, lanes, o):
            z1 = zs_ref[pl.ds(t * per, per), pl.ds(r, rows, stride=rows), :].reshape(tq, ch)
            z2 = z1 + nn(gate(r, lanes, o, gb2_ref), ow2_ref[...])
            z2 = z2.astype(BF16).astype(F32)
            hid = nn(layer_norm(z2, g3_ref[...]), ti_ref[...]) + tb_ref[...]
            hid = jnp.maximum(hid, 0.0).astype(BF16)
            stage(r, z2 + nn(hid, to_ref[...]))

        attend_tile(tq, ck, t, q_ref, k_ref, v_ref, bias_ref, (sa_ref, sb_ref), end_finish)
        send_z[pl.ds(t * per, per)] = st_ref[...].astype(BF16)
        spread_tile(4, send_z, recv_o, t)
        return carry

    lax.fori_loop(0, res // tq, end_tile, 0)
    recv_o[me] = send_z[me]
    spread_finish(4, send_z, recv_o)

    zs_ref[...] = recv_o[...].astype(F32)

    def out_row(r, carry):
        out_ref[r] = zs_ref[:, pl.ds(r, rows, stride=rows), :].reshape(res, ch).astype(BF16)
        return carry

    lax.fori_loop(0, rows, out_row, 0)


def solution(mesh):
    nx, ny = mesh.shape["gx"], mesh.shape["gy"]
    n = nx * ny

    def local(x, mask, g1, w1, gb1, bw1, ow1, g2, w2, gb2, bw2, ow2, g3, ti, tb, to):
        rows, res, ch = x.shape
        tq, ck = min(res, 256), min(res, 256)
        vmem = pl.BlockSpec(memory_space=pltpu.VMEM)
        row = lambda t: t.reshape(1, -1)
        return pl.pallas_call(
            functools.partial(kernel, nx, ny, tq, ck),
            out_shape=jax.ShapeDtypeStruct(x.shape, x.dtype),
            in_specs=[vmem, pl.BlockSpec(memory_space=pltpu.SMEM)] + [vmem] * 14,
            out_specs=vmem,
            scratch_shapes=[
                pltpu.VMEM((rows, ch, res), BF16),
                pltpu.VMEM((rows, res, ch), BF16),
                pltpu.VMEM((rows, ch, res), BF16),
                pltpu.VMEM((4 * ch, ch), BF16),
                pltpu.VMEM((HEADS, res, res), F32),
                pltpu.VMEM((1, res), F32),
                pltpu.VMEM((res, 128), F32),
                pltpu.VMEM((n, rows * rows, ch), F32),
                pltpu.VMEM((tq // rows, rows * rows, ch), F32),
                pltpu.VMEM((HEADS * rows, tq), F32),
                pltpu.VMEM((res, tq), F32),
                pltpu.VMEM((res, tq), F32),
                pltpu.VMEM((n, 16, 128), BF16),
                pltpu.VMEM((n, HEADS * rows, res), BF16),
                pltpu.VMEM((n, HEADS * rows, res), BF16),
                pltpu.VMEM((n, rows * rows, ch), BF16),
                pltpu.VMEM((n, rows * rows, ch), BF16),
                pltpu.VMEM((n, rows * rows, ch), BF16),
                pltpu.SemaphoreType.DMA((5, n)),
                pltpu.SemaphoreType.DMA((5, n)),
                pltpu.SemaphoreType.DMA((3, ny, nx // 2)),
                pltpu.SemaphoreType.DMA((3, ny)),
            ],
            compiler_params=pltpu.CompilerParams(
                collective_id=0, has_side_effects=True, vmem_limit_bytes=66 * 1000 * 1000
            ),
        )(
            x, mask, row(g1), w1, gb1.reshape(-1, 1), bw1.T, ow1, row(g2), w2,
            gb2.reshape(-1, 1), bw2.T, ow2,
            row(g3), ti, row(tb), to,
        )

    placed = (P(("gx", "gy"), None, None), P(("gx", "gy"))) + (P(),) * 14
    return jax.shard_map(
        local, mesh=mesh, in_specs=placed, out_specs=P(("gx", "gy"), None, None), check_vma=False
    )
```

```python
import functools
import math

import jax
import jax.numpy as jnp
from jax import lax
from jax.experimental import pallas as pl
from jax.experimental.pallas import tpu as pltpu
from jax.sharding import PartitionSpec as P

HEADS = 4
HEAD_DIM = 32
BIG = 1000000000.0
LOG2E = math.log2(math.e)
QSCALE = HEAD_DIM ** (-0.5) * LOG2E
MESH = pl.DeviceIdType.MESH
F32 = jnp.float32
BF16 = jnp.bfloat16


def nn(a, b):
    return lax.dot_general(a, b, (((1,), (0,)), ((), ())), preferred_element_type=F32)


def nt(a, b):
    return lax.dot_general(a, b, (((1,), (1,)), ((), ())), preferred_element_type=F32)


def layer_norm(x, gain):
    mean = jnp.mean(x, axis=-1, keepdims=True)
    cent = x - mean
    var = jnp.mean(cent * cent, axis=-1, keepdims=True)
    return (cent * lax.rsqrt(var + 1e-05) * gain).astype(BF16)


def bias_rows(w, r, rows, normed):
    shape = (HEADS * rows, HEADS)
    place = lax.broadcasted_iota(jnp.int32, shape, 0) == (
        lax.broadcasted_iota(jnp.int32, shape, 1) * rows + r
    )
    spread = nn(place.astype(F32).astype(BF16), w).astype(BF16)
    return nt(spread, normed)


def attend_tile(ck, t, q_ref, k_ref, v_ref, bias_ref, s_refs, finish):
    rows, res, ch = k_ref.shape
    tq = s_refs[0].shape[1]
    lanes = pl.ds(pl.multiple_of(t * tq, tq), tq)
    chunks = res // ck

    def query(r, h):
        q = q_ref[r, :, lanes]
        row = lax.broadcasted_iota(jnp.int32, q.shape, 0)
        return jnp.where((row >= h * HEAD_DIM) & (row < (h + 1) * HEAD_DIM), q, jnp.zeros_like(q))

    def score(r, h, c, q, top):
        span = slice(c * ck, (c + 1) * ck)
        s = nn(k_ref[r, span, :], q) + bias_ref[h, span, lanes]
        s_refs[h % 2][span, :] = s
        m = jnp.max(s.reshape(ck // 8, 8, tq), axis=0)
        return m if top is None else jnp.maximum(top, m)

    def mix(r, h, c, top, acc):
        span = slice(c * ck, (c + 1) * ck)
        w = jnp.exp2((s_refs[h % 2][span, :] - top).astype(BF16))
        v = jnp.concatenate(
            [v_ref[r, h * HEAD_DIM : (h + 1) * HEAD_DIM, span], jnp.ones((16, ck), BF16)], axis=0
        )
        o = nn(v, w)
        return o if acc is None else acc + o

    q, top = query(0, 0), None
    for c in range(chunks):
        top = score(0, 0, c, q, top)

    def body(r, top):
        outs = []
        for h in range(HEADS):
            peak = jnp.max(top, axis=0, keepdims=True)
            nh = (h + 1) % HEADS
            nr = r if h < HEADS - 1 else jnp.minimum(r + 1, rows - 1)
            q, top, acc = query(nr, nh), None, None
            for c in range(chunks):
                top = score(nr, nh, c, q, top)
                acc = mix(r, h, c, peak, acc)
            outs.append(acc[:HEAD_DIM] / acc[HEAD_DIM : HEAD_DIM + 1])
        finish(r, jnp.concatenate(outs, axis=0))
        return top

    lax.fori_loop(0, rows, body, top)


class Gather:
    def __init__(self, place, ssem, rsem):
        self.place, self.ssem, self.rsem = place, ssem, rsem

    def copy(self, inst, kind, src, dst, to):
        return pltpu.make_async_remote_copy(
            src_ref=src,
            dst_ref=dst,
            send_sem=self.ssem.at[inst, kind],
            recv_sem=self.rsem.at[inst, kind],
            device_id=self.place(*to),
            device_id_type=MESH,
        )

    def setup(self, me, sizes):
        self.x, self.core, self.plane = me
        self.xs, self.planes = sizes
        self.other = 1 - self.core

    def at(self, step):
        return lax.rem(self.x + step, self.xs)

    def fan(self, inst, kind, slot):
        @pl.loop(1, self.planes)
        def _(u):
            p = lax.rem(self.plane + u, self.planes)
            self.copy(inst, kind, slot, slot, (self.x, self.core, p)).start()

    def fanned(self, inst, kind, buf):
        rest = buf.at[self.x, self.core, pl.ds(0, self.planes - 1)]
        return self.copy(inst, kind, rest, rest, (self.x, self.other, self.plane))

    def line(self, inst, kind, buf, step):
        part = buf.at[self.x, self.core]
        return self.copy(inst, kind, part, part, (self.at(step), self.core, self.plane))

    def hand(self, inst, kind, buf, step, core=None):
        part = buf.at[self.at(step), self.core if core is None else core]
        return self.copy(inst, kind, part, part, (self.x, self.other, self.plane))

    def far(self, inst, slot):
        half = self.xs // 2
        return self.copy(inst, 1, slot, slot, (self.at(half), self.core, self.plane))

    def first(self, inst, buf):
        slot = buf.at[self.x, self.core, self.plane]
        self.far(inst, slot).start()
        self.fan(inst, 0, slot)

    def second(self, inst, buf, buf_far):
        slot = buf_far.at[self.at(self.xs // 2), self.core, self.plane]
        self.far(inst, slot).wait_recv()
        self.fan(inst, 2, slot)
        self.fanned(inst, 0, buf).wait_recv()
        self.hand(inst, 5, buf, 0).start()
        self.line(inst, 3, buf, 1).start()
        self.line(inst, 4, buf, self.xs - 1).start()

    def third_far(self, inst, buf_far):
        self.fanned(inst, 2, buf_far).wait_recv()
        self.hand(inst, 6, buf_far, self.xs // 2).start()

    def third_near(self, inst, buf_up, buf_down):
        self.line(inst, 4, buf_up, 1).wait_recv()
        self.hand(inst, 7, buf_up, 1).start()
        self.line(inst, 3, buf_down, 1).wait_recv()
        self.hand(inst, 8, buf_down, self.xs - 1).start()

    def handed(self, inst, kind, buf, step):
        self.hand(inst, kind, buf, step, self.other).wait_recv()

    def drain(self, inst, buf):
        slot = buf.at[self.x, self.core, self.plane]
        self.far(inst, slot).wait_send()
        self.fanned(inst, 0, buf).wait_send()
        self.fanned(inst, 2, buf).wait_send()
        self.line(inst, 3, buf, 1).wait_send()
        self.line(inst, 4, buf, 1).wait_send()
        for kind in (5, 6, 7, 8):
            self.hand(inst, kind, buf, 0).wait_send()


def kernel(
    nx,
    ny,
    ck,
    x_ref,
    mask_ref,
    g1_ref,
    w1_ref,
    gb1_ref,
    bw1_ref,
    ow1_ref,
    g2_ref,
    w2_ref,
    gb2_ref,
    bw2_ref,
    ow2_ref,
    g3_ref,
    ti_ref,
    tb_ref,
    to_ref,
    out_ref,
    q_ref,
    k_ref,
    v_ref,
    wt_ref,
    bias_ref,
    kb_ref,
    kc_ref,
    zs_ref,
    st_ref,
    rise_ref,
    sa_ref,
    sb_ref,
    recv_m,
    recv_a,
    recv_b,
    send_z,
    recv_z,
    recv_o,
    ssem,
    rsem,
    zsem,
):
    n = nx * ny
    xs, planes = nx // 4, 2 * ny
    rows, res, ch = x_ref.shape
    tq = res // xs
    a_ref = out_ref
    gx, gy = lax.axis_index("gx"), lax.axis_index("gy")
    me = gx * ny + gy
    core = lax.rem(gx, 2)
    x = lax.rem(gx // 2, xs)
    low = gx // (2 * xs)
    plane = low * ny + gy
    run = 2 * ny

    def place(x, core, plane):
        return (plane // ny * (2 * xs) + x * 2 + core, lax.rem(plane, ny))

    g = Gather(place, ssem, rsem)
    g.setup((x, core, plane), (xs, planes))
    barrier = pltpu.get_barrier_semaphore()

    def greet(*to):
        pl.semaphore_signal(barrier, inc=1, device_id=place(*to), device_id_type=MESH)

    for u in range(1, planes):
        greet(x, core, lax.rem(plane + u, planes))
    for u in range(1, xs):
        greet(g.at(u), core, plane)
    greet(x, 1 - core, plane)

    lane = lax.broadcasted_iota(jnp.int32, (16, 128), 1)
    vec = jnp.zeros((16, 128), F32)
    for t in range(rows):
        vec = jnp.where(lane == lax.rem(me * rows, 128) + t, mask_ref[t].astype(F32), vec)
    recv_m[x, core, plane] = vec.astype(BF16)

    pl.semaphore_wait(barrier, planes - 1 + xs - 1 + 1)
    g.first(0, recv_m)

    def norm_row(r, acc):
        normed = layer_norm(x_ref[r].astype(F32), g1_ref[...])
        a_ref[r] = normed
        return acc + bias_rows(bw1_ref[...], r, rows, normed)

    with jax.named_scope("norm"):
        acc = lax.fori_loop(0, rows, norm_row, jnp.zeros((HEADS * rows, res), F32))
        recv_a[x, core, plane] = acc.astype(BF16)

    g.first(1, recv_a)
    with jax.named_scope("mask2"):
        g.second(0, recv_m, recv_m)

    def turn_weights(w_ref):
        wt_ref[...] = w_ref[...].astype(F32).T.astype(BF16)

    def project(r, normed, w_ref):
        k_ref[r] = nn(normed, w_ref[:, ch : 2 * ch]).astype(BF16)
        q = (nt(wt_ref[:ch], normed) * QSCALE).astype(BF16)
        for b in range(2 * xs):
            to = (b % xs * 2 + b // xs) * 128
            q_ref[r, :, to : to + 128] = q[:, b * 128 : (b + 1) * 128]
        v_ref[r] = nt(wt_ref[2 * ch : 3 * ch], normed).astype(BF16)

    def both(t, size):
        return [pl.ds(pl.multiple_of((t + e * xs) * size, size), size) for e in range(2)]

    def gate(r, t, o, gb_ref):
        a = jnp.concatenate([a_ref[r, span, :] for span in both(t, 128)], axis=0)
        gl = nt(wt_ref[3 * ch :], a)
        return (o * jax.nn.sigmoid(gl + gb_ref[...])).T.astype(BF16)

    turn_weights(w1_ref)

    def project_row(r, carry):
        project(r, a_ref[r], w1_ref)
        return carry

    with jax.named_scope("project"):
        lax.fori_loop(0, rows, project_row, 0)
    with jax.named_scope("mask3"):
        g.third_far(0, recv_m)
        g.third_near(0, recv_m, recv_m)
    with jax.named_scope("a2"):
        g.second(1, recv_a, recv_a)
    with jax.named_scope("mask4"):
        g.handed(0, 5, recv_m, 0)
        g.handed(0, 6, recv_m, xs // 2)
        g.handed(0, 7, recv_m, 1)
        g.handed(0, 8, recv_m, xs - 1)

    for b in range(2 * xs):
        part = recv_m[b % xs, :, b // xs * ny : (b // xs + 1) * ny].astype(F32)
        mask = jnp.sum(jnp.sum(part, axis=0), axis=0)[:1]
        kb = (mask - 1.0) * BIG
        kb_ref[:, b * 128 : (b + 1) * 128] = kb
        kc_ref[b * 128 : (b + 1) * 128, :] = jnp.broadcast_to(kb, (128, 128)).T

    def start_bias(t):
        for e in range(2):
            blocks = [
                recv_a[t, c, e * ny : (e + 1) * ny].astype(F32) for c in range(2)
            ]
            for h in range(HEADS):
                part = jnp.concatenate(
                    [b[:, h * rows : (h + 1) * rows, :].reshape(64, res) for b in blocks], axis=0
                )
                to = pl.ds(pl.multiple_of(t * tq + e * 128, 128), 128)
                bias_ref[h, :, to] = ((part + kb_ref[...]) * LOG2E).T

    def stage(r, z):
        st_ref[:, pl.ds(pl.multiple_of(r * rows, rows), rows), :] = z.reshape(
            tq // rows, rows, ch
        )

    def ship(kind, dst, t):
        for e, span in enumerate(both(t, run)):
            send_z[span] = st_ref[e * run : (e + 1) * run].astype(BF16)

        @pl.loop(0, 2 * run)
        def _(u):
            v = lax.rem(u + plane * 2 + core, 2 * run)
            c, p = lax.rem(v, 2), v // 2
            to = place(t, c, p)
            d = to[0] * ny + to[1]

            @pl.when(d != me)
            def _():
                pltpu.make_async_remote_copy(
                    src_ref=send_z.at[d],
                    dst_ref=dst.at[me],
                    send_sem=zsem.at[kind, 0],
                    recv_sem=zsem.at[kind, 1],
                    device_id=to,
                    device_id_type=MESH,
                ).start()

    def shipped(kind, dst):
        dst[me] = send_z[me]
        rest = pl.ds(0, n - 1)
        pltpu.make_async_remote_copy(
            src_ref=send_z.at[rest],
            dst_ref=dst.at[rest],
            send_sem=zsem.at[kind, 0],
            recv_sem=zsem.at[kind, 1],
            device_id=place(x, 1 - core, plane),
            device_id_type=MESH,
        ).wait()

    def tile_of(s, step=0):
        away = jnp.where(s == 0, 0, jnp.where(s == 1, xs // 2, jnp.where(s == 2, 1, xs - 1)))
        return lax.rem(x + step + away, xs)

    def rise_second(s):
        t = tile_of(s)
        g.second(2 + s, recv_b.at[t], recv_b.at[tile_of(s, xs // 2)])

    def rise_third(s):
        g.third_far(2 + s, recv_b.at[tile_of(s, xs // 2)])
        g.third_near(2 + s, recv_b.at[tile_of(s, 1)], recv_b.at[tile_of(s, xs - 1)])

    def start_tile(s, carry):
        t = tile_of(s)

        @pl.when(s == 0)
        def _():
            with jax.named_scope("wait0"):
                g.handed(1, 5, recv_a, 0)

        @pl.when(s == 1)
        def _():
            with jax.named_scope("wait1"):
                g.third_far(1, recv_a)
                g.handed(1, 6, recv_a, xs // 2)

        @pl.when(s == 2)
        def _():
            with jax.named_scope("wait2"):
                g.third_near(1, recv_a, recv_a)
                g.handed(1, 7, recv_a, 1)

        @pl.when(s == 3)
        def _():
            with jax.named_scope("wait3"):
                g.handed(1, 8, recv_a, xs - 1)

        with jax.named_scope("biasa"):
            start_bias(t)
        rise_ref[...] = jnp.zeros_like(rise_ref)

        def start_finish(r, o):
            old = jnp.concatenate([x_ref[r, span, :] for span in both(t, 128)], axis=0)
            z1 = old.astype(F32) + nn(gate(r, t, o, gb1_ref), ow1_ref[...])
            z1 = z1.astype(BF16).astype(F32)
            stage(r, z1)
            rise_ref[...] = rise_ref[...] + bias_rows(
                bw2_ref[...], r, rows, layer_norm(z1, g2_ref[...])
            )

            @pl.when((s > 0) & (r == rows // 2 - 1))
            def _():
                with jax.named_scope("rise2"):
                    rise_second(s - 1)

            @pl.when((s > 0) & (r == rows - 1))
            def _():
                with jax.named_scope("rise3"):
                    rise_third(s - 1)

        with jax.named_scope("att1"):
            attend_tile(ck, t, q_ref, k_ref, v_ref, bias_ref, (sa_ref, sb_ref), start_finish)
        recv_b[t, x, core, plane] = rise_ref[...].astype(BF16)
        with jax.named_scope("ship1"):
            g.first(2 + s, recv_b.at[t])
            ship(0, recv_z, t)
        return carry

    lax.fori_loop(0, xs, start_tile, 0)
    turn_weights(w2_ref)
    with jax.named_scope("rise2e"):
        rise_second(xs - 1)
    with jax.named_scope("waitz"):
        shipped(0, recv_z)
    zs_ref[...] = recv_z[...].astype(F32)

    def end_project(d, carry):
        z1 = zs_ref[:, pl.ds(d, rows, stride=rows), :].reshape(res, ch)
        normed = layer_norm(z1, g2_ref[...])
        a_ref[d] = normed
        project(d, normed, w2_ref)
        return carry

    with jax.named_scope("rise3e"):
        rise_third(xs - 1)
    with jax.named_scope("project2"):
        lax.fori_loop(0, rows, end_project, 0)

    def rise_done(s, carry):
        g.handed(2 + s, 5, recv_b.at[tile_of(s)], 0)
        g.handed(2 + s, 6, recv_b.at[tile_of(s, xs // 2)], xs // 2)
        g.handed(2 + s, 7, recv_b.at[tile_of(s, 1)], 1)
        g.handed(2 + s, 8, recv_b.at[tile_of(s, xs - 1)], xs - 1)
        return carry

    with jax.named_scope("handed"):
        lax.fori_loop(0, xs, rise_done, 0)

    def end_bias(t):
        def keys_of(b, carry):
            e, c = lax.rem(b // 2, 2), lax.rem(b, 2)
            keys = pl.ds(pl.multiple_of((e * 2 * xs + b // 4 * 2 + c) * 64, 64), 64)
            kc = kc_ref[keys, :]
            block = recv_b[t, b // 4, c, pl.ds(e * ny, ny)].astype(F32)
            for h in range(HEADS):
                part = block[:, h * rows : (h + 1) * rows, :].reshape(64, tq)
                for w in range(tq // 128):
                    to = pl.ds(pl.multiple_of(t * tq + w * 128, 128), 128)
                    bias_ref[h, keys, to] = (part[:, w * 128 : (w + 1) * 128] + kc) * LOG2E
            return carry

        lax.fori_loop(0, 4 * xs, keys_of, 0)

    def end_tile(s, carry):
        t = tile_of(s)
        with jax.named_scope("biasb"):
            end_bias(t)

        def end_finish(r, o):
            z1 = jnp.concatenate(
                [
                    zs_ref[span, pl.ds(r, rows, stride=rows), :].reshape(128, ch)
                    for span in both(t, run)
                ],
                axis=0,
            )
            z2 = z1 + nn(gate(r, t, o, gb2_ref), ow2_ref[...])
            z2 = z2.astype(BF16).astype(F32)
            hid = nn(layer_norm(z2, g3_ref[...]), ti_ref[...]) + tb_ref[...]
            hid = jnp.maximum(hid, 0.0).astype(BF16)
            stage(r, z2 + nn(hid, to_ref[...]))

        with jax.named_scope("att2"):
            attend_tile(ck, t, q_ref, k_ref, v_ref, bias_ref, (sa_ref, sb_ref), end_finish)
        with jax.named_scope("ship2"):
            ship(1, recv_o, t)
        return carry

    lax.fori_loop(0, xs, end_tile, 0)
    with jax.named_scope("drain"):
        g.drain(0, recv_m)
        g.drain(1, recv_a)

        def drain_rise(s, carry):
            g.drain(2 + s, recv_b.at[tile_of(s)])
            return carry

        lax.fori_loop(0, xs, drain_rise, 0)
    with jax.named_scope("waito"):
        shipped(1, recv_o)

    zs_ref[...] = recv_o[...].astype(F32)

    def out_row(r, carry):
        out_ref[r] = zs_ref[:, pl.ds(r, rows, stride=rows), :].reshape(res, ch).astype(BF16)
        return carry

    with jax.named_scope("outrow"):
        lax.fori_loop(0, rows, out_row, 0)


def solution(mesh):
    nx, ny = mesh.shape["gx"], mesh.shape["gy"]
    n, xs = nx * ny, nx // 4

    def local(x, mask, g1, w1, gb1, bw1, ow1, g2, w2, gb2, bw2, ow2, g3, ti, tb, to):
        rows, res, ch = x.shape
        tq, ck = res // xs, 256
        vmem = pl.BlockSpec(memory_space=pltpu.VMEM)
        row = lambda t: t.reshape(1, -1)
        return pl.pallas_call(
            functools.partial(kernel, nx, ny, ck),
            out_shape=jax.ShapeDtypeStruct(x.shape, x.dtype),
            in_specs=[vmem, pl.BlockSpec(memory_space=pltpu.SMEM)] + [vmem] * 14,
            out_specs=vmem,
            scratch_shapes=[
                pltpu.VMEM((rows, ch, res), BF16),
                pltpu.VMEM((rows, res, ch), BF16),
                pltpu.VMEM((rows, ch, res), BF16),
                pltpu.VMEM((4 * ch, ch), BF16),
                pltpu.VMEM((HEADS, res, res), F32),
                pltpu.VMEM((1, res), F32),
                pltpu.VMEM((res, 128), F32),
                pltpu.VMEM((n, rows * rows, ch), F32),
                pltpu.VMEM((tq // rows, rows * rows, ch), F32),
                pltpu.VMEM((HEADS * rows, tq), F32),
                pltpu.VMEM((res, tq), F32),
                pltpu.VMEM((res, tq), F32),
                pltpu.VMEM((xs, 2, 2 * ny, 16, 128), BF16),
                pltpu.VMEM((xs, 2, 2 * ny, HEADS * rows, res), BF16),
                pltpu.VMEM((xs, xs, 2, 2 * ny, HEADS * rows, tq), BF16),
                pltpu.VMEM((n, rows * rows, ch), BF16),
                pltpu.VMEM((n, rows * rows, ch), BF16),
                pltpu.VMEM((n, rows * rows, ch), BF16),
                pltpu.SemaphoreType.DMA((2 + xs, 9)),
                pltpu.SemaphoreType.DMA((2 + xs, 9)),
                pltpu.SemaphoreType.DMA((2, 2)),
            ],
            compiler_params=pltpu.CompilerParams(
                collective_id=0, has_side_effects=True, vmem_limit_bytes=66 * 1000 * 1000
            ),
        )(
            x, mask, row(g1), w1, gb1.reshape(-1, 1), bw1.T, ow1, row(g2), w2,
            gb2.reshape(-1, 1), bw2.T, ow2, row(g3), ti, row(tb), to,
        )

    placed = (P(("gx", "gy"), None, None), P(("gx", "gy"))) + (P(),) * 14
    return jax.shard_map(
        local, mesh=mesh, in_specs=placed, out_specs=P(("gx", "gy"), None, None), check_vma=False
    )
```

```python
import functools
import math

import jax
import jax.numpy as jnp
from jax import lax
from jax.experimental import pallas as pl
from jax.experimental.pallas import tpu as pltpu
from jax.sharding import PartitionSpec as P

HEADS = 4
HEAD_DIM = 32
BIG = 1000000000.0
LOG2E = math.log2(math.e)
QSCALE = HEAD_DIM ** (-0.5) * LOG2E
MESH = pl.DeviceIdType.MESH
F32 = jnp.float32
BF16 = jnp.bfloat16


def nn(a, b):
    return lax.dot_general(a, b, (((1,), (0,)), ((), ())), preferred_element_type=F32)


def nt(a, b):
    return lax.dot_general(a, b, (((1,), (1,)), ((), ())), preferred_element_type=F32)


def layer_norm(x, gain):
    mean = jnp.mean(x, axis=-1, keepdims=True)
    cent = x - mean
    var = jnp.mean(cent * cent, axis=-1, keepdims=True)
    return (cent * lax.rsqrt(var + 1e-05) * gain).astype(BF16)


def bias_rows(w, r, rows, normed):
    shape = (HEADS * rows, HEADS)
    place = lax.broadcasted_iota(jnp.int32, shape, 0) == (
        lax.broadcasted_iota(jnp.int32, shape, 1) * rows + r
    )
    spread = nn(place.astype(F32).astype(BF16), w).astype(BF16)
    return nt(spread, normed)


def attend_tile(ck, t, q_ref, k_ref, v_ref, bias_ref, s_refs, o_ref, after):
    rows, res, ch = k_ref.shape
    tq = s_refs[0].shape[1]
    lanes = pl.ds(pl.multiple_of(t * tq, tq), tq)
    chunks = res // ck

    def query(r, h):
        q = q_ref[r, :, lanes]
        row = lax.broadcasted_iota(jnp.int32, q.shape, 0)
        return jnp.where((row >= h * HEAD_DIM) & (row < (h + 1) * HEAD_DIM), q, jnp.zeros_like(q))

    def score(r, h, c, q, top):
        span = slice(c * ck, (c + 1) * ck)
        s = nn(k_ref[r, span, :], q) + bias_ref[h, span, lanes]
        s_refs[h % 2][span, :] = s
        m = jnp.max(s.reshape(ck // 8, 8, tq), axis=0)
        return m if top is None else jnp.maximum(top, m)

    def mix(r, h, c, top, acc):
        span = slice(c * ck, (c + 1) * ck)
        w = jnp.exp2((s_refs[h % 2][span, :] - top).astype(BF16))
        v = jnp.concatenate(
            [v_ref[r, h * HEAD_DIM : (h + 1) * HEAD_DIM, span], jnp.ones((16, ck), BF16)], axis=0
        )
        o = nn(v, w)
        return o if acc is None else acc + o

    q, top = query(0, 0), None
    for c in range(chunks):
        top = score(0, 0, c, q, top)

    def body(r, top):
        outs = []
        for h in range(HEADS):
            peak = jnp.max(top, axis=0, keepdims=True)
            nh = (h + 1) % HEADS
            nr = r if h < HEADS - 1 else jnp.minimum(r + 1, rows - 1)
            q, top, acc = query(nr, nh), None, None
            for c in range(chunks):
                top = score(nr, nh, c, q, top)
                acc = mix(r, h, c, peak, acc)
            outs.append(acc[:HEAD_DIM] / acc[HEAD_DIM : HEAD_DIM + 1])
        o_ref[r] = jnp.concatenate(outs, axis=0)
        after(r)
        return top

    lax.fori_loop(0, rows, body, top)


class Gather:
    def __init__(self, place, ssem, rsem):
        self.place, self.ssem, self.rsem = place, ssem, rsem

    def copy(self, inst, kind, src, dst, to):
        return pltpu.make_async_remote_copy(
            src_ref=src,
            dst_ref=dst,
            send_sem=self.ssem.at[inst, kind],
            recv_sem=self.rsem.at[inst, kind],
            device_id=self.place(*to),
            device_id_type=MESH,
        )

    def setup(self, me, sizes):
        self.x, self.core, self.plane = me
        self.xs, self.planes = sizes
        self.other = 1 - self.core

    def at(self, step):
        return lax.rem(self.x + step, self.xs)

    def fan(self, inst, kind, slot):
        @pl.loop(1, self.planes)
        def _(u):
            p = lax.rem(self.plane + u, self.planes)
            self.copy(inst, kind, slot, slot, (self.x, self.core, p)).start()

    def fanned(self, inst, kind, buf):
        rest = buf.at[self.x, self.core, pl.ds(0, self.planes - 1)]
        return self.copy(inst, kind, rest, rest, (self.x, self.other, self.plane))

    def line(self, inst, kind, buf, step):
        part = buf.at[self.x, self.core]
        return self.copy(inst, kind, part, part, (self.at(step), self.core, self.plane))

    def hand(self, inst, kind, buf, step, core=None):
        part = buf.at[self.at(step), self.core if core is None else core]
        return self.copy(inst, kind, part, part, (self.x, self.other, self.plane))

    def far(self, inst, slot):
        half = self.xs // 2
        return self.copy(inst, 1, slot, slot, (self.at(half), self.core, self.plane))

    def first(self, inst, buf):
        slot = buf.at[self.x, self.core, self.plane]
        self.far(inst, slot).start()
        self.fan(inst, 0, slot)

    def second(self, inst, buf, buf_far):
        slot = buf_far.at[self.at(self.xs // 2), self.core, self.plane]
        self.far(inst, slot).wait_recv()
        self.fan(inst, 2, slot)
        self.fanned(inst, 0, buf).wait_recv()
        self.hand(inst, 5, buf, 0).start()
        self.line(inst, 3, buf, 1).start()
        self.line(inst, 4, buf, self.xs - 1).start()

    def third_far(self, inst, buf_far):
        self.fanned(inst, 2, buf_far).wait_recv()
        self.hand(inst, 6, buf_far, self.xs // 2).start()

    def third_near(self, inst, buf_up, buf_down):
        self.line(inst, 4, buf_up, 1).wait_recv()
        self.hand(inst, 7, buf_up, 1).start()
        self.line(inst, 3, buf_down, 1).wait_recv()
        self.hand(inst, 8, buf_down, self.xs - 1).start()

    def handed(self, inst, kind, buf, step):
        self.hand(inst, kind, buf, step, self.other).wait_recv()

    def drain(self, inst, buf):
        slot = buf.at[self.x, self.core, self.plane]
        self.far(inst, slot).wait_send()
        self.fanned(inst, 0, buf).wait_send()
        self.fanned(inst, 2, buf).wait_send()
        self.line(inst, 3, buf, 1).wait_send()
        self.line(inst, 4, buf, 1).wait_send()
        for kind in (5, 6, 7, 8):
            self.hand(inst, kind, buf, 0).wait_send()


def kernel(
    nx,
    ny,
    ck,
    x_ref,
    mask_ref,
    g1_ref,
    w1_ref,
    gb1_ref,
    bw1_ref,
    ow1_ref,
    g2_ref,
    w2_ref,
    gb2_ref,
    bw2_ref,
    ow2_ref,
    g3_ref,
    ti_ref,
    tb_ref,
    to_ref,
    out_ref,
    q_ref,
    k_ref,
    v_ref,
    wt_ref,
    bias_ref,
    kb_ref,
    kc_ref,
    zs_ref,
    st_ref,
    rise_ref,
    sa_ref,
    sb_ref,
    o_ref,
    recv_m,
    recv_a,
    recv_b,
    send_z,
    recv_z,
    recv_o,
    ssem,
    rsem,
    zsem,
):
    n = nx * ny
    xs, planes = nx // 4, 2 * ny
    rows, res, ch = x_ref.shape
    tq = res // xs
    a_ref = out_ref
    gx, gy = lax.axis_index("gx"), lax.axis_index("gy")
    me = gx * ny + gy
    core = lax.rem(gx, 2)
    x = lax.rem(gx // 2, xs)
    low = gx // (2 * xs)
    plane = low * ny + gy
    run = 2 * ny

    def place(x, core, plane):
        return (plane // ny * (2 * xs) + x * 2 + core, lax.rem(plane, ny))

    g = Gather(place, ssem, rsem)
    g.setup((x, core, plane), (xs, planes))
    barrier = pltpu.get_barrier_semaphore()

    def greet(*to):
        pl.semaphore_signal(barrier, inc=1, device_id=place(*to), device_id_type=MESH)

    for u in range(1, planes):
        greet(x, core, lax.rem(plane + u, planes))
    for u in range(1, xs):
        greet(g.at(u), core, plane)
    greet(x, 1 - core, plane)

    lane = lax.broadcasted_iota(jnp.int32, (16, 128), 1)
    vec = jnp.zeros((16, 128), F32)
    for t in range(rows):
        vec = jnp.where(lane == lax.rem(me * rows, 128) + t, mask_ref[t].astype(F32), vec)
    recv_m[x, core, plane] = vec.astype(BF16)

    pl.semaphore_wait(barrier, planes - 1 + xs - 1 + 1)
    g.first(0, recv_m)

    def norm_row(r, acc):
        normed = layer_norm(x_ref[r].astype(F32), g1_ref[...])
        a_ref[r] = normed
        return acc + bias_rows(bw1_ref[...], r, rows, normed)

    with jax.named_scope("norm"):
        acc = lax.fori_loop(0, rows, norm_row, jnp.zeros((HEADS * rows, res), F32))
        recv_a[x, core, plane] = acc.astype(BF16)

    g.first(1, recv_a)
    with jax.named_scope("mask2"):
        g.second(0, recv_m, recv_m)

    def turn_weights(w_ref):
        wt_ref[...] = w_ref[...].astype(F32).T.astype(BF16)

    def project(r, normed, w_ref):
        k_ref[r] = nn(normed, w_ref[:, ch : 2 * ch]).astype(BF16)
        q = (nt(wt_ref[:ch], normed) * QSCALE).astype(BF16)
        for b in range(2 * xs):
            to = (b % xs * 2 + b // xs) * 128
            q_ref[r, :, to : to + 128] = q[:, b * 128 : (b + 1) * 128]
        v_ref[r] = nt(wt_ref[2 * ch : 3 * ch], normed).astype(BF16)

    def both(t, size):
        return [pl.ds(pl.multiple_of((t + e * xs) * size, size), size) for e in range(2)]

    def mixed(batch, t, gb_ref, ow_ref):
        a = [jnp.concatenate([a_ref[r, span, :] for span in both(t, 128)], axis=0) for r in batch]
        gl = [nt(wt_ref[3 * ch :], v) for v in a]
        gated = [o_ref[r] * jax.nn.sigmoid(v + gb_ref[...]) for r, v in zip(batch, gl)]
        gated = [v.T.astype(BF16) for v in gated]
        return [nn(v, ow_ref[...]) for v in gated]

    def batches(fn):
        def run(i, carry):
            fn([i * 8 + e for e in range(8)])
            return carry

        lax.fori_loop(0, rows // 8, run, 0)

    turn_weights(w1_ref)

    def project_row(r, carry):
        project(r, a_ref[r], w1_ref)
        return carry

    with jax.named_scope("project"):
        lax.fori_loop(0, rows, project_row, 0)
    with jax.named_scope("mask3"):
        g.third_far(0, recv_m)
        g.third_near(0, recv_m, recv_m)
    with jax.named_scope("a2"):
        g.second(1, recv_a, recv_a)
    with jax.named_scope("mask4"):
        g.handed(0, 5, recv_m, 0)
        g.handed(0, 6, recv_m, xs // 2)
        g.handed(0, 7, recv_m, 1)
        g.handed(0, 8, recv_m, xs - 1)

    for b in range(2 * xs):
        part = recv_m[b % xs, :, b // xs * ny : (b // xs + 1) * ny].astype(F32)
        mask = jnp.sum(jnp.sum(part, axis=0), axis=0)[:1]
        kb = (mask - 1.0) * BIG
        kb_ref[:, b * 128 : (b + 1) * 128] = kb
        kc_ref[b * 128 : (b + 1) * 128, :] = jnp.broadcast_to(kb, (128, 128)).T

    def start_bias(t):
        for e in range(2):
            blocks = [
                recv_a[t, c, e * ny : (e + 1) * ny].astype(F32) for c in range(2)
            ]
            for h in range(HEADS):
                part = jnp.concatenate(
                    [b[:, h * rows : (h + 1) * rows, :].reshape(64, res) for b in blocks], axis=0
                )
                to = pl.ds(pl.multiple_of(t * tq + e * 128, 128), 128)
                bias_ref[h, :, to] = ((part + kb_ref[...]) * LOG2E).T

    def stage(r, z):
        st_ref[:, pl.ds(pl.multiple_of(r * rows, rows), rows), :] = z.reshape(
            tq // rows, rows, ch
        )

    def ship(kind, dst, t):
        for e, span in enumerate(both(t, run)):
            send_z[span] = st_ref[e * run : (e + 1) * run].astype(BF16)

        @pl.loop(0, 2 * run)
        def _(u):
            v = lax.rem(u + plane * 2 + core, 2 * run)
            c, p = lax.rem(v, 2), v // 2
            to = place(t, c, p)
            d = to[0] * ny + to[1]

            @pl.when(d != me)
            def _():
                pltpu.make_async_remote_copy(
                    src_ref=send_z.at[d],
                    dst_ref=dst.at[me],
                    send_sem=zsem.at[kind, 0],
                    recv_sem=zsem.at[kind, 1],
                    device_id=to,
                    device_id_type=MESH,
                ).start()

    def shipped(kind, dst):
        dst[me] = send_z[me]
        rest = pl.ds(0, n - 1)
        pltpu.make_async_remote_copy(
            src_ref=send_z.at[rest],
            dst_ref=dst.at[rest],
            send_sem=zsem.at[kind, 0],
            recv_sem=zsem.at[kind, 1],
            device_id=place(x, 1 - core, plane),
            device_id_type=MESH,
        ).wait()

    def tile_of(s, step=0):
        away = jnp.where(s == 0, 0, jnp.where(s == 1, xs // 2, jnp.where(s == 2, 1, xs - 1)))
        return lax.rem(x + step + away, xs)

    def rise_second(s):
        t = tile_of(s)
        g.second(2 + s, recv_b.at[t], recv_b.at[tile_of(s, xs // 2)])

    def rise_third(s):
        g.third_far(2 + s, recv_b.at[tile_of(s, xs // 2)])
        g.third_near(2 + s, recv_b.at[tile_of(s, 1)], recv_b.at[tile_of(s, xs - 1)])

    def start_tile(s, carry):
        t = tile_of(s)

        @pl.when(s == 0)
        def _():
            with jax.named_scope("wait0"):
                g.handed(1, 5, recv_a, 0)

        @pl.when(s == 1)
        def _():
            with jax.named_scope("wait1"):
                g.third_far(1, recv_a)
                g.handed(1, 6, recv_a, xs // 2)

        @pl.when(s == 2)
        def _():
            with jax.named_scope("wait2"):
                g.third_near(1, recv_a, recv_a)
                g.handed(1, 7, recv_a, 1)

        @pl.when(s == 3)
        def _():
            with jax.named_scope("wait3"):
                g.handed(1, 8, recv_a, xs - 1)

        with jax.named_scope("biasa"):
            start_bias(t)
        def start_finish(batch):
            out = mixed(batch, t, gb1_ref, ow1_ref)
            old = [jnp.concatenate([x_ref[r, p, :] for p in both(t, 128)], axis=0) for r in batch]
            z1 = [(u.astype(F32) + v).astype(BF16).astype(F32) for u, v in zip(old, out)]
            for r, v in zip(batch, z1):
                stage(r, v)
            normed = [layer_norm(v, g2_ref[...]) for v in z1]
            part = [bias_rows(bw2_ref[...], r, rows, v) for r, v in zip(batch, normed)]
            rise_ref[...] = rise_ref[...] + sum(part[1:], part[0])

        def start_after(r):
            @pl.when((s > 0) & (r == rows // 2 - 1))
            def _():
                with jax.named_scope("rise2"):
                    rise_second(s - 1)

            @pl.when((s > 0) & (r == rows - 1))
            def _():
                with jax.named_scope("rise3"):
                    rise_third(s - 1)

        with jax.named_scope("att1"):
            attend_tile(ck, t, q_ref, k_ref, v_ref, bias_ref, (sa_ref, sb_ref), o_ref,
                start_after)
        with jax.named_scope("tail1"):
            rise_ref[...] = jnp.zeros_like(rise_ref)
            batches(start_finish)
        recv_b[t, x, core, plane] = rise_ref[...].astype(BF16)
        with jax.named_scope("ship1"):
            g.first(2 + s, recv_b.at[t])
            ship(0, recv_z, t)
        return carry

    lax.fori_loop(0, xs, start_tile, 0)
    turn_weights(w2_ref)
    with jax.named_scope("rise2e"):
        rise_second(xs - 1)
    with jax.named_scope("waitz"):
        shipped(0, recv_z)
    zs_ref[...] = recv_z[...].astype(F32)

    def end_project(d, carry):
        z1 = zs_ref[:, pl.ds(d, rows, stride=rows), :].reshape(res, ch)
        normed = layer_norm(z1, g2_ref[...])
        a_ref[d] = normed
        project(d, normed, w2_ref)
        return carry

    with jax.named_scope("rise3e"):
        rise_third(xs - 1)
    with jax.named_scope("project2"):
        lax.fori_loop(0, rows, end_project, 0)

    def rise_done(s, carry):
        g.handed(2 + s, 5, recv_b.at[tile_of(s)], 0)
        g.handed(2 + s, 6, recv_b.at[tile_of(s, xs // 2)], xs // 2)
        g.handed(2 + s, 7, recv_b.at[tile_of(s, 1)], 1)
        g.handed(2 + s, 8, recv_b.at[tile_of(s, xs - 1)], xs - 1)
        return carry

    with jax.named_scope("handed"):
        lax.fori_loop(0, xs, rise_done, 0)

    def end_bias(t):
        def keys_of(b, carry):
            e, c = lax.rem(b // 2, 2), lax.rem(b, 2)
            keys = pl.ds(pl.multiple_of((e * 2 * xs + b // 4 * 2 + c) * 64, 64), 64)
            kc = kc_ref[keys, :]
            block = recv_b[t, b // 4, c, pl.ds(e * ny, ny)].astype(F32)
            for h in range(HEADS):
                part = block[:, h * rows : (h + 1) * rows, :].reshape(64, tq)
                for w in range(tq // 128):
                    to = pl.ds(pl.multiple_of(t * tq + w * 128, 128), 128)
                    bias_ref[h, keys, to] = (part[:, w * 128 : (w + 1) * 128] + kc) * LOG2E
            return carry

        lax.fori_loop(0, 4 * xs, keys_of, 0)

    def end_tile(s, carry):
        t = tile_of(s)
        with jax.named_scope("biasb"):
            end_bias(t)

        def end_finish(batch):
            out = mixed(batch, t, gb2_ref, ow2_ref)
            z1 = [
                jnp.concatenate(
                    [
                        zs_ref[span, pl.ds(r, rows, stride=rows), :].reshape(128, ch)
                        for span in both(t, run)
                    ],
                    axis=0,
                )
                for r in batch
            ]
            z2 = [(u + v).astype(BF16).astype(F32) for u, v in zip(z1, out)]
            normed = [layer_norm(v, g3_ref[...]) for v in z2]
            hid = [nn(v, ti_ref[...]) + tb_ref[...] for v in normed]
            hid = [jnp.maximum(v, 0.0).astype(BF16) for v in hid]
            last = [nn(v, to_ref[...]) for v in hid]
            for r, u, v in zip(batch, z2, last):
                stage(r, u + v)

        with jax.named_scope("att2"):
            attend_tile(ck, t, q_ref, k_ref, v_ref, bias_ref, (sa_ref, sb_ref), o_ref,
                lambda r: None)
        with jax.named_scope("tail2"):
            batches(end_finish)
        with jax.named_scope("ship2"):
            ship(1, recv_o, t)
        return carry

    lax.fori_loop(0, xs, end_tile, 0)
    with jax.named_scope("drain"):
        g.drain(0, recv_m)
        g.drain(1, recv_a)

        def drain_rise(s, carry):
            g.drain(2 + s, recv_b.at[tile_of(s)])
            return carry

        lax.fori_loop(0, xs, drain_rise, 0)
    with jax.named_scope("waito"):
        shipped(1, recv_o)

    zs_ref[...] = recv_o[...].astype(F32)

    def out_row(r, carry):
        out_ref[r] = zs_ref[:, pl.ds(r, rows, stride=rows), :].reshape(res, ch).astype(BF16)
        return carry

    with jax.named_scope("outrow"):
        lax.fori_loop(0, rows, out_row, 0)


def solution(mesh):
    nx, ny = mesh.shape["gx"], mesh.shape["gy"]
    n, xs = nx * ny, nx // 4

    def local(x, mask, g1, w1, gb1, bw1, ow1, g2, w2, gb2, bw2, ow2, g3, ti, tb, to):
        rows, res, ch = x.shape
        tq, ck = res // xs, 512
        vmem = pl.BlockSpec(memory_space=pltpu.VMEM)
        row = lambda t: t.reshape(1, -1)
        return pl.pallas_call(
            functools.partial(kernel, nx, ny, ck),
            out_shape=jax.ShapeDtypeStruct(x.shape, x.dtype),
            in_specs=[vmem, pl.BlockSpec(memory_space=pltpu.SMEM)] + [vmem] * 14,
            out_specs=vmem,
            scratch_shapes=[
                pltpu.VMEM((rows, ch, res), BF16),
                pltpu.VMEM((rows, res, ch), BF16),
                pltpu.VMEM((rows, ch, res), BF16),
                pltpu.VMEM((4 * ch, ch), BF16),
                pltpu.VMEM((HEADS, res, res), F32),
                pltpu.VMEM((1, res), F32),
                pltpu.VMEM((res, 128), F32),
                pltpu.VMEM((n, rows * rows, ch), F32),
                pltpu.VMEM((tq // rows, rows * rows, ch), F32),
                pltpu.VMEM((HEADS * rows, tq), F32),
                pltpu.VMEM((res, tq), F32),
                pltpu.VMEM((res, tq), F32),
                pltpu.VMEM((rows, ch, tq), F32),
                pltpu.VMEM((xs, 2, 2 * ny, 16, 128), BF16),
                pltpu.VMEM((xs, 2, 2 * ny, HEADS * rows, res), BF16),
                pltpu.VMEM((xs, xs, 2, 2 * ny, HEADS * rows, tq), BF16),
                pltpu.VMEM((n, rows * rows, ch), BF16),
                pltpu.VMEM((n, rows * rows, ch), BF16),
                pltpu.VMEM((n, rows * rows, ch), BF16),
                pltpu.SemaphoreType.DMA((2 + xs, 9)),
                pltpu.SemaphoreType.DMA((2 + xs, 9)),
                pltpu.SemaphoreType.DMA((2, 2)),
            ],
            compiler_params=pltpu.CompilerParams(
                collective_id=0, has_side_effects=True, vmem_limit_bytes=66 * 1000 * 1000
            ),
        )(
            x, mask, row(g1), w1, gb1.reshape(-1, 1), bw1.T, ow1, row(g2), w2,
            gb2.reshape(-1, 1), bw2.T, ow2, row(g3), ti, row(tb), to,
        )

    placed = (P(("gx", "gy"), None, None), P(("gx", "gy"))) + (P(),) * 14
    return jax.shard_map(
        local, mesh=mesh, in_specs=placed, out_specs=P(("gx", "gy"), None, None), check_vma=False
    )
```

```python
import functools
import math

import jax
import jax.numpy as jnp
from jax import lax
from jax.experimental import pallas as pl
from jax.experimental.pallas import tpu as pltpu
from jax.sharding import PartitionSpec as P

HEADS = 4
HEAD_DIM = 32
BIG = 1000000000.0
LOG2E = math.log2(math.e)
QSCALE = HEAD_DIM ** (-0.5) * LOG2E
MESH = pl.DeviceIdType.MESH
F32 = jnp.float32
BF16 = jnp.bfloat16


def nn(a, b):
    return lax.dot_general(a, b, (((1,), (0,)), ((), ())), preferred_element_type=F32)


def nt(a, b):
    return lax.dot_general(a, b, (((1,), (1,)), ((), ())), preferred_element_type=F32)


def layer_norm(x, gain):
    mean = jnp.mean(x, axis=-1, keepdims=True)
    cent = x - mean
    var = jnp.mean(cent * cent, axis=-1, keepdims=True)
    return (cent * lax.rsqrt(var + 1e-05) * gain).astype(BF16)


def bias_rows(w, r, rows, normed):
    shape = (HEADS * rows, HEADS)
    place = lax.broadcasted_iota(jnp.int32, shape, 0) == (
        lax.broadcasted_iota(jnp.int32, shape, 1) * rows + r
    )
    spread = nn(place.astype(F32).astype(BF16), w).astype(BF16)
    return nt(spread, normed)


def attend_tile(ck, t, q_ref, k_ref, v_ref, bias_ref, s_refs, o_ref, after):
    rows, res, ch = k_ref.shape
    tq = s_refs[0].shape[1]
    lanes = pl.ds(pl.multiple_of(t * tq, tq), tq)
    chunks = res // ck

    def query(r, h):
        q = q_ref[r, :, lanes]
        row = lax.broadcasted_iota(jnp.int32, q.shape, 0)
        return jnp.where((row >= h * HEAD_DIM) & (row < (h + 1) * HEAD_DIM), q, jnp.zeros_like(q))

    def score(r, h, c, q, top):
        span = slice(c * ck, (c + 1) * ck)
        s = nn(k_ref[r, span, :], q) + bias_ref[h, span, lanes]
        s_refs[h % 2][span, :] = s
        m = jnp.max(s.reshape(ck // 8, 8, tq), axis=0)
        return m if top is None else jnp.maximum(top, m)

    def mix(r, h, c, top, acc):
        span = slice(c * ck, (c + 1) * ck)
        w = jnp.exp2((s_refs[h % 2][span, :] - top).astype(BF16))
        v = jnp.concatenate(
            [v_ref[r, h * HEAD_DIM : (h + 1) * HEAD_DIM, span], jnp.ones((16, ck), BF16)], axis=0
        )
        o = nn(v, w)
        return o if acc is None else acc + o

    q, top = query(0, 0), None
    for c in range(chunks):
        top = score(0, 0, c, q, top)

    def body(r, top):
        outs = []
        for h in range(HEADS):
            peak = jnp.max(top, axis=0, keepdims=True)
            nh = (h + 1) % HEADS
            nr = r if h < HEADS - 1 else jnp.minimum(r + 1, rows - 1)
            q, top, acc = query(nr, nh), None, None
            for c in range(chunks):
                top = score(nr, nh, c, q, top)
                acc = mix(r, h, c, peak, acc)
            outs.append(acc[:HEAD_DIM] / acc[HEAD_DIM : HEAD_DIM + 1])
        o_ref[r] = jnp.concatenate(outs, axis=0)
        after(r)
        return top

    lax.fori_loop(0, rows, body, top)


class Gather:
    def __init__(self, place, ssem, rsem):
        self.place, self.ssem, self.rsem = place, ssem, rsem

    def copy(self, inst, kind, src, dst, to):
        return pltpu.make_async_remote_copy(
            src_ref=src,
            dst_ref=dst,
            send_sem=self.ssem.at[inst, kind],
            recv_sem=self.rsem.at[inst, kind],
            device_id=self.place(*to),
            device_id_type=MESH,
        )

    def setup(self, me, sizes):
        self.x, self.core, self.plane = me
        self.xs, self.planes = sizes
        self.other = 1 - self.core

    def at(self, step):
        return lax.rem(self.x + step, self.xs)

    def fan(self, inst, kind, slot):
        @pl.loop(1, self.planes)
        def _(u):
            p = lax.rem(self.plane + u, self.planes)
            self.copy(inst, kind, slot, slot, (self.x, self.core, p)).start()

    def fanned(self, inst, kind, buf):
        rest = buf.at[self.x, self.core, pl.ds(0, self.planes - 1)]
        return self.copy(inst, kind, rest, rest, (self.x, self.other, self.plane))

    def line(self, inst, kind, buf, step):
        part = buf.at[self.x, self.core]
        return self.copy(inst, kind, part, part, (self.at(step), self.core, self.plane))

    def hand(self, inst, kind, buf, step, core=None):
        part = buf.at[self.at(step), self.core if core is None else core]
        return self.copy(inst, kind, part, part, (self.x, self.other, self.plane))

    def far(self, inst, slot):
        half = self.xs // 2
        return self.copy(inst, 1, slot, slot, (self.at(half), self.core, self.plane))

    def first(self, inst, buf):
        slot = buf.at[self.x, self.core, self.plane]
        self.far(inst, slot).start()
        self.fan(inst, 0, slot)

    def second(self, inst, buf, buf_far):
        slot = buf_far.at[self.at(self.xs // 2), self.core, self.plane]
        self.far(inst, slot).wait_recv()
        self.fan(inst, 2, slot)
        self.fanned(inst, 0, buf).wait_recv()
        self.hand(inst, 5, buf, 0).start()
        self.line(inst, 3, buf, 1).start()
        self.line(inst, 4, buf, self.xs - 1).start()

    def third_far(self, inst, buf_far):
        self.fanned(inst, 2, buf_far).wait_recv()
        self.hand(inst, 6, buf_far, self.xs // 2).start()

    def third_near(self, inst, buf_up, buf_down):
        self.line(inst, 4, buf_up, 1).wait_recv()
        self.hand(inst, 7, buf_up, 1).start()
        self.line(inst, 3, buf_down, 1).wait_recv()
        self.hand(inst, 8, buf_down, self.xs - 1).start()

    def handed(self, inst, kind, buf, step):
        self.hand(inst, kind, buf, step, self.other).wait_recv()

    def drain(self, inst, buf):
        slot = buf.at[self.x, self.core, self.plane]
        self.far(inst, slot).wait_send()
        self.fanned(inst, 0, buf).wait_send()
        self.fanned(inst, 2, buf).wait_send()
        self.line(inst, 3, buf, 1).wait_send()
        self.line(inst, 4, buf, 1).wait_send()
        for kind in (5, 6, 7, 8):
            self.hand(inst, kind, buf, 0).wait_send()


def kernel(
    nx,
    ny,
    ck,
    x_ref,
    mask_ref,
    g1_ref,
    w1_ref,
    gb1_ref,
    bw1_ref,
    ow1_ref,
    g2_ref,
    w2_ref,
    gb2_ref,
    bw2_ref,
    ow2_ref,
    g3_ref,
    ti_ref,
    tb_ref,
    to_ref,
    out_ref,
    q_ref,
    k_ref,
    v_ref,
    wt_ref,
    bias_ref,
    kb_ref,
    kc_ref,
    zs_ref,
    st_ref,
    rise_ref,
    first_ref,
    gc_ref,
    sa_ref,
    sb_ref,
    o_ref,
    recv_m,
    recv_a,
    recv_b,
    send_z,
    recv_z,
    recv_o,
    ssem,
    rsem,
    zsem,
):
    n = nx * ny
    xs, planes = nx // 4, 2 * ny
    rows, res, ch = x_ref.shape
    tq = res // xs
    a_ref = out_ref
    gx, gy = lax.axis_index("gx"), lax.axis_index("gy")
    me = gx * ny + gy
    core = lax.rem(gx, 2)
    x = lax.rem(gx // 2, xs)
    low = gx // (2 * xs)
    plane = low * ny + gy
    run = 2 * ny

    def place(x, core, plane):
        return (plane // ny * (2 * xs) + x * 2 + core, lax.rem(plane, ny))

    g = Gather(place, ssem, rsem)
    g.setup((x, core, plane), (xs, planes))
    barrier = pltpu.get_barrier_semaphore()

    def greet(*to):
        pl.semaphore_signal(barrier, inc=1, device_id=place(*to), device_id_type=MESH)

    for u in range(1, planes):
        greet(x, core, lax.rem(plane + u, planes))
    for u in range(1, xs):
        greet(g.at(u), core, plane)
    greet(x, 1 - core, plane)

    lane = lax.broadcasted_iota(jnp.int32, (16, 128), 1)
    vec = jnp.zeros((16, 128), F32)
    for t in range(rows):
        vec = jnp.where(lane == lax.rem(me * rows, 128) + t, mask_ref[t].astype(F32), vec)
    recv_m[x, core, plane] = vec.astype(BF16)

    pl.semaphore_wait(barrier, planes - 1 + xs - 1 + 1)
    g.first(0, recv_m)

    def grouped(lo, hi, fn, size=2):
        def step(i, carry):
            fn([lo + i * size + e for e in range(size)])
            return carry

        lax.fori_loop(0, (hi - lo) // size, step, 0)

    def start_norm(batch):
        normed = [layer_norm(v.astype(F32), g1_ref[...]) for v in [x_ref[r] for r in batch]]
        for r, v in zip(batch, normed):
            a_ref[r] = v
        part = [bias_rows(bw1_ref[...], r, rows, v) for r, v in zip(batch, normed)]
        first_ref[...] = first_ref[...] + sum(part[1:], part[0])

    with jax.named_scope("norm"):
        first_ref[...] = jnp.zeros_like(first_ref)
        grouped(0, rows, start_norm)
        recv_a[x, core, plane] = first_ref[...].astype(BF16)

    g.first(1, recv_a)
    with jax.named_scope("mask2"):
        g.second(0, recv_m, recv_m)

    def turn_weights(w_ref, gb_ref):
        wt_ref[...] = w_ref[...].astype(F32).T.astype(BF16)
        column = jnp.broadcast_to(gb_ref[...], (128, ch)).T
        for b in range(tq // 128):
            gc_ref[:, b * 128 : (b + 1) * 128] = column

    def project(batch, w_ref):
        normed = [a_ref[r] for r in batch]
        for r, v in zip(batch, [nn(v, w_ref[:, ch : 2 * ch]) for v in normed]):
            k_ref[r] = v.astype(BF16)
        for r, v in zip(batch, [nt(wt_ref[:ch], v) for v in normed]):
            q = (v * QSCALE).astype(BF16)
            for b in range(2 * xs):
                to = (b % xs * 2 + b // xs) * 128
                q_ref[r, :, to : to + 128] = q[:, b * 128 : (b + 1) * 128]
        for r, v in zip(batch, [nt(wt_ref[2 * ch : 3 * ch], v) for v in normed]):
            v_ref[r] = v.astype(BF16)

    def both(t, size):
        return [pl.ds(pl.multiple_of((t + e * xs) * size, size), size) for e in range(2)]

    def mixed(batch, t, ow_ref):
        a = [jnp.concatenate([a_ref[r, span, :] for span in both(t, 128)], axis=0) for r in batch]
        gl = [nt(wt_ref[3 * ch :], v) for v in a]
        gated = [o_ref[r] * jax.nn.sigmoid(v + gc_ref[...]) for r, v in zip(batch, gl)]
        gated = [v.T.astype(BF16) for v in gated]
        return [nn(v, ow_ref[...]) for v in gated]

    def batches(fn):
        def run(i, carry):
            fn([i * 8 + e for e in range(8)])
            return carry

        lax.fori_loop(0, rows // 8, run, 0)

    turn_weights(w1_ref, gb1_ref)

    with jax.named_scope("project"):
        grouped(0, rows, lambda batch: project(batch, w1_ref))
    with jax.named_scope("mask3"):
        g.third_far(0, recv_m)
        g.third_near(0, recv_m, recv_m)
    with jax.named_scope("a2"):
        g.second(1, recv_a, recv_a)
    with jax.named_scope("mask4"):
        g.handed(0, 5, recv_m, 0)
        g.handed(0, 6, recv_m, xs // 2)
        g.handed(0, 7, recv_m, 1)
        g.handed(0, 8, recv_m, xs - 1)

    for b in range(2 * xs):
        part = recv_m[b % xs, :, b // xs * ny : (b // xs + 1) * ny].astype(F32)
        mask = jnp.sum(jnp.sum(part, axis=0), axis=0)[:1]
        kb = (mask - 1.0) * BIG
        kb_ref[:, b * 128 : (b + 1) * 128] = kb
        kc_ref[b * 128 : (b + 1) * 128, :] = jnp.broadcast_to(kb, (128, 128)).T

    def start_bias(t):
        for e in range(2):
            blocks = [
                recv_a[t, c, e * ny : (e + 1) * ny].astype(F32) for c in range(2)
            ]
            for h in range(HEADS):
                part = jnp.concatenate(
                    [b[:, h * rows : (h + 1) * rows, :].reshape(64, res) for b in blocks], axis=0
                )
                to = pl.ds(pl.multiple_of(t * tq + e * 128, 128), 128)
                bias_ref[h, :, to] = ((part + kb_ref[...]) * LOG2E).T

    def stage(r, z):
        st_ref[:, pl.ds(pl.multiple_of(r * rows, rows), rows), :] = z.reshape(
            tq // rows, rows, ch
        )

    def ship(kind, dst, t):
        for e, span in enumerate(both(t, run)):
            send_z[span] = st_ref[e * run : (e + 1) * run].astype(BF16)

        @pl.loop(0, 2 * run)
        def _(u):
            v = lax.rem(u + plane * 2 + core, 2 * run)
            c, p = lax.rem(v, 2), v // 2
            to = place(t, c, p)
            d = to[0] * ny + to[1]

            @pl.when(d != me)
            def _():
                pltpu.make_async_remote_copy(
                    src_ref=send_z.at[d],
                    dst_ref=dst.at[me],
                    send_sem=zsem.at[kind, 0],
                    recv_sem=zsem.at[kind, 1],
                    device_id=to,
                    device_id_type=MESH,
                ).start()

    def shipped(kind, dst):
        dst[me] = send_z[me]
        rest = pl.ds(0, n - 1)
        pltpu.make_async_remote_copy(
            src_ref=send_z.at[rest],
            dst_ref=dst.at[rest],
            send_sem=zsem.at[kind, 0],
            recv_sem=zsem.at[kind, 1],
            device_id=place(x, 1 - core, plane),
            device_id_type=MESH,
        ).wait()

    near = 1 + core * (xs - 2)

    def tile_of(s, step=0, swap=False):
        side = xs - near if swap else near
        away = jnp.where(s == 0, 0, jnp.where(s == 1, xs // 2, jnp.where(s == 2, side, xs - side)))
        return lax.rem(x + step + away, xs)

    def rise_second(s):
        t = tile_of(s)
        g.second(2 + s, recv_b.at[t], recv_b.at[tile_of(s, xs // 2)])

    def rise_third(s):
        g.third_far(2 + s, recv_b.at[tile_of(s, xs // 2)])
        g.third_near(2 + s, recv_b.at[tile_of(s, 1)], recv_b.at[tile_of(s, xs - 1)])

    def start_tile(s, carry):
        t = tile_of(s)

        @pl.when(s == 0)
        def _():
            with jax.named_scope("wait0"):
                g.handed(1, 5, recv_a, 0)

        @pl.when(s == 1)
        def _():
            with jax.named_scope("wait1"):
                g.third_far(1, recv_a)
                g.handed(1, 6, recv_a, xs // 2)

        @pl.when(s == 2)
        def _():
            with jax.named_scope("wait2"):
                g.third_near(1, recv_a, recv_a)
                g.handed(1, 7, recv_a, 1)
                g.handed(1, 8, recv_a, xs - 1)

        with jax.named_scope("biasa"):
            start_bias(t)
        def start_finish(batch):
            out = mixed(batch, t, ow1_ref)
            old = [jnp.concatenate([x_ref[r, p, :] for p in both(t, 128)], axis=0) for r in batch]
            z1 = [(u.astype(F32) + v).astype(BF16).astype(F32) for u, v in zip(old, out)]
            for r, v in zip(batch, z1):
                stage(r, v)
            normed = [layer_norm(v, g2_ref[...]) for v in z1]
            part = [bias_rows(bw2_ref[...], r, rows, v) for r, v in zip(batch, normed)]
            rise_ref[...] = rise_ref[...] + sum(part[1:], part[0])

        def start_after(r):
            @pl.when((s > 0) & (r == rows // 2 - 1))
            def _():
                with jax.named_scope("rise2"):
                    rise_second(s - 1)

            @pl.when((s > 1) & (r == rows // 4))
            def _():
                with jax.named_scope("rise3"):
                    rise_third(s - 2)

        with jax.named_scope("att1"):
            attend_tile(ck, t, q_ref, k_ref, v_ref, bias_ref, (sa_ref, sb_ref), o_ref,
                start_after)
        with jax.named_scope("tail1"):
            rise_ref[...] = jnp.zeros_like(rise_ref)
            batches(start_finish)
        recv_b[t, x, core, plane] = rise_ref[...].astype(BF16)
        with jax.named_scope("ship1"):
            g.first(2 + s, recv_b.at[t])
            ship(0, recv_z, t)
        return carry

    lax.fori_loop(0, xs, start_tile, 0)
    turn_weights(w2_ref, gb2_ref)
    with jax.named_scope("rise3d"):
        rise_third(xs - 2)
    with jax.named_scope("rise2e"):
        rise_second(xs - 1)
    with jax.named_scope("waitz"):
        shipped(0, recv_z)
    zs_ref[...] = recv_z[...].astype(F32)

    def end_norm(batch):
        z1 = [zs_ref[:, pl.ds(d, rows, stride=rows), :].reshape(res, ch) for d in batch]
        for d, v in zip(batch, [layer_norm(v, g2_ref[...]) for v in z1]):
            a_ref[d] = v

    with jax.named_scope("norm2"):
        grouped(0, rows, end_norm)
    with jax.named_scope("rise3e"):
        rise_third(xs - 1)
    with jax.named_scope("project2"):
        grouped(0, rows, lambda batch: project(batch, w2_ref))

    def rise_done(s, carry):
        g.handed(2 + s, 5, recv_b.at[tile_of(s, 0, True)], 0)
        g.handed(2 + s, 6, recv_b.at[tile_of(s, xs // 2, True)], xs // 2)
        g.handed(2 + s, 7, recv_b.at[tile_of(s, 1, True)], 1)
        g.handed(2 + s, 8, recv_b.at[tile_of(s, xs - 1, True)], xs - 1)
        return carry

    with jax.named_scope("handed"):
        lax.fori_loop(0, xs, rise_done, 0)

    def end_bias(t):
        def keys_of(b, carry):
            e, c = lax.rem(b // 2, 2), lax.rem(b, 2)
            keys = pl.ds(pl.multiple_of((e * 2 * xs + b // 4 * 2 + c) * 64, 64), 64)
            kc = kc_ref[keys, :]
            block = recv_b[t, b // 4, c, pl.ds(e * ny, ny)].astype(F32)
            for h in range(HEADS):
                part = block[:, h * rows : (h + 1) * rows, :].reshape(64, tq)
                for w in range(tq // 128):
                    to = pl.ds(pl.multiple_of(t * tq + w * 128, 128), 128)
                    bias_ref[h, keys, to] = (part[:, w * 128 : (w + 1) * 128] + kc) * LOG2E
            return carry

        lax.fori_loop(0, 4 * xs, keys_of, 0)

    def end_tile(s, carry):
        t = tile_of(lax.rem(s + 1, xs))
        with jax.named_scope("biasb"):
            end_bias(t)

        def end_finish(batch):
            out = mixed(batch, t, ow2_ref)
            z1 = [
                jnp.concatenate(
                    [
                        zs_ref[span, pl.ds(r, rows, stride=rows), :].reshape(128, ch)
                        for span in both(t, run)
                    ],
                    axis=0,
                )
                for r in batch
            ]
            z2 = [(u + v).astype(BF16).astype(F32) for u, v in zip(z1, out)]
            normed = [layer_norm(v, g3_ref[...]) for v in z2]
            hid = [nn(v, ti_ref[...]) + tb_ref[...] for v in normed]
            hid = [jnp.maximum(v, 0.0).astype(BF16) for v in hid]
            last = [nn(v, to_ref[...]) for v in hid]
            for r, u, v in zip(batch, z2, last):
                stage(r, u + v)

        with jax.named_scope("att2"):
            attend_tile(ck, t, q_ref, k_ref, v_ref, bias_ref, (sa_ref, sb_ref), o_ref,
                lambda r: None)
        with jax.named_scope("tail2"):
            batches(end_finish)
        with jax.named_scope("ship2"):
            ship(1, recv_o, t)
        return carry

    lax.fori_loop(0, xs, end_tile, 0)
    with jax.named_scope("drain"):
        g.drain(0, recv_m)
        g.drain(1, recv_a)

        def drain_rise(s, carry):
            g.drain(2 + s, recv_b.at[tile_of(s)])
            return carry

        lax.fori_loop(0, xs, drain_rise, 0)
    with jax.named_scope("waito"):
        shipped(1, recv_o)

    zs_ref[...] = recv_o[...].astype(F32)

    def out_row(r, carry):
        out_ref[r] = zs_ref[:, pl.ds(r, rows, stride=rows), :].reshape(res, ch).astype(BF16)
        return carry

    with jax.named_scope("outrow"):
        lax.fori_loop(0, rows, out_row, 0)


def solution(mesh):
    nx, ny = mesh.shape["gx"], mesh.shape["gy"]
    n, xs = nx * ny, nx // 4

    def local(x, mask, g1, w1, gb1, bw1, ow1, g2, w2, gb2, bw2, ow2, g3, ti, tb, to):
        rows, res, ch = x.shape
        tq, ck = res // xs, 512
        vmem = pl.BlockSpec(memory_space=pltpu.VMEM)
        row = lambda t: t.reshape(1, -1)
        return pl.pallas_call(
            functools.partial(kernel, nx, ny, ck),
            out_shape=jax.ShapeDtypeStruct(x.shape, x.dtype),
            in_specs=[vmem, pl.BlockSpec(memory_space=pltpu.SMEM)] + [vmem] * 14,
            out_specs=vmem,
            scratch_shapes=[
                pltpu.VMEM((rows, ch, res), BF16),
                pltpu.VMEM((rows, res, ch), BF16),
                pltpu.VMEM((rows, ch, res), BF16),
                pltpu.VMEM((4 * ch, ch), BF16),
                pltpu.VMEM((HEADS, res, res), F32),
                pltpu.VMEM((1, res), F32),
                pltpu.VMEM((res, 128), F32),
                pltpu.VMEM((n, rows * rows, ch), F32),
                pltpu.VMEM((tq // rows, rows * rows, ch), F32),
                pltpu.VMEM((HEADS * rows, tq), F32),
                pltpu.VMEM((HEADS * rows, res), F32),
                pltpu.VMEM((ch, tq), F32),
                pltpu.VMEM((res, tq), F32),
                pltpu.VMEM((res, tq), F32),
                pltpu.VMEM((rows, ch, tq), F32),
                pltpu.VMEM((xs, 2, 2 * ny, 16, 128), BF16),
                pltpu.VMEM((xs, 2, 2 * ny, HEADS * rows, res), BF16),
                pltpu.VMEM((xs, xs, 2, 2 * ny, HEADS * rows, tq), BF16),
                pltpu.VMEM((n, rows * rows, ch), BF16),
                pltpu.VMEM((n, rows * rows, ch), BF16),
                pltpu.VMEM((n, rows * rows, ch), BF16),
                pltpu.SemaphoreType.DMA((2 + xs, 9)),
                pltpu.SemaphoreType.DMA((2 + xs, 9)),
                pltpu.SemaphoreType.DMA((2, 2)),
            ],
            compiler_params=pltpu.CompilerParams(
                collective_id=0, has_side_effects=True, vmem_limit_bytes=66 * 1000 * 1000,
            ),
        )(
            x, mask, row(g1), w1, row(gb1), bw1.T, ow1, row(g2), w2,
            row(gb2), bw2.T, ow2, row(g3), ti, row(tb), to,
        )

    placed = (P(("gx", "gy"), None, None), P(("gx", "gy"))) + (P(),) * 14
    return jax.shard_map(
        local, mesh=mesh, in_specs=placed, out_specs=P(("gx", "gy"), None, None), check_vma=False
    )
```

```python
import functools
import math

import jax
import jax.numpy as jnp
from jax import lax
from jax.experimental import pallas as pl
from jax.experimental.pallas import tpu as pltpu
from jax.sharding import PartitionSpec as P

HEADS = 4
HEAD_DIM = 32
BIG = 1000000000.0
LOG2E = math.log2(math.e)
QSCALE = HEAD_DIM ** (-0.5) * LOG2E
MESH = pl.DeviceIdType.MESH
F32 = jnp.float32
BF16 = jnp.bfloat16


def nn(a, b):
    return lax.dot_general(a, b, (((1,), (0,)), ((), ())), preferred_element_type=F32)


def nt(a, b):
    return lax.dot_general(a, b, (((1,), (1,)), ((), ())), preferred_element_type=F32)


def layer_norm(x, gain):
    mean = jnp.mean(x, axis=-1, keepdims=True)
    cent = x - mean
    var = jnp.mean(cent * cent, axis=-1, keepdims=True)
    return (cent * lax.rsqrt(var + 1e-05) * gain).astype(BF16)


def bias_rows(w, r, rows, normed):
    shape = (HEADS * rows, HEADS)
    place = lax.broadcasted_iota(jnp.int32, shape, 0) == (
        lax.broadcasted_iota(jnp.int32, shape, 1) * rows + r
    )
    spread = nn(place.astype(F32).astype(BF16), w).astype(BF16)
    return nt(spread, normed)


def attend_tile(ck, group, t, q_ref, k_ref, v_ref, bias_ref, s_ref, o_ref, after):
    rows, res, ch = k_ref.shape
    tq = s_ref.shape[1]
    s_refs = [s_ref.at[:res], s_ref.at[res:]]
    lanes = pl.ds(pl.multiple_of(t * tq, tq), tq)
    chunks = res // ck

    def query(r, h):
        q = q_ref[r, :, lanes]
        row = lax.broadcasted_iota(jnp.int32, q.shape, 0)
        return jnp.where((row >= h * HEAD_DIM) & (row < (h + 1) * HEAD_DIM), q, jnp.zeros_like(q))

    def score(r, h, c, q, top):
        span = slice(c * ck, (c + 1) * ck)
        s = nn(k_ref[r, span, :], q) + bias_ref[t, h, span, :]
        s_refs[h % 2][span, :] = s
        m = jnp.max(s.reshape(ck // 8, 8, tq), axis=0)
        return m if top is None else jnp.maximum(top, m)

    def mix(r, h, c, top, acc):
        span = slice(c * ck, (c + 1) * ck)
        w = jnp.exp2((s_refs[h % 2][span, :] - top).astype(BF16))
        v = jnp.concatenate(
            [v_ref[r, h * HEAD_DIM : (h + 1) * HEAD_DIM, span], jnp.ones((16, ck), BF16)], axis=0
        )
        o = nn(v, w)
        return o if acc is None else acc + o

    q, top = query(0, 0), None
    for c in range(chunks):
        top = score(0, 0, c, q, top)

    def row(r, top):
        outs = []
        for h in range(HEADS):
            peak = jnp.max(top, axis=0, keepdims=True)
            nh = (h + 1) % HEADS
            nr = r if h < HEADS - 1 else jnp.minimum(r + 1, rows - 1)
            q, top, acc = query(nr, nh), None, None
            for c in range(chunks):
                top = score(nr, nh, c, q, top)
                acc = mix(r, h, c, peak, acc)
            outs.append(acc[:HEAD_DIM] / acc[HEAD_DIM : HEAD_DIM + 1])
        o_ref[r] = jnp.concatenate(outs, axis=0)
        return top

    def body(i, top):
        for e in range(group):
            top = row(i * group + e, top)
        after(i)
        return top

    lax.fori_loop(0, rows // group, body, top)


class Gather:
    def __init__(self, place, ssem, rsem):
        self.place, self.ssem, self.rsem = place, ssem, rsem

    def copy(self, inst, kind, src, dst, to):
        return pltpu.make_async_remote_copy(
            src_ref=src,
            dst_ref=dst,
            send_sem=self.ssem.at[inst, kind],
            recv_sem=self.rsem.at[inst, kind],
            device_id=self.place(*to),
            device_id_type=MESH,
        )

    def setup(self, me, sizes):
        self.x, self.core, self.plane = me
        self.xs, self.planes = sizes
        self.other = 1 - self.core

    def at(self, step):
        return lax.rem(self.x + step, self.xs)

    def fan(self, inst, kind, slot):
        @pl.loop(1, self.planes)
        def _(u):
            p = lax.rem(self.plane + u, self.planes)
            self.copy(inst, kind, slot, slot, (self.x, self.core, p)).start()

    def fanned(self, inst, kind, buf):
        rest = buf.at[self.x, self.core, pl.ds(0, self.planes - 1)]
        return self.copy(inst, kind, rest, rest, (self.x, self.other, self.plane))

    def line(self, inst, kind, buf, step):
        part = buf.at[self.x, self.core]
        return self.copy(inst, kind, part, part, (self.at(step), self.core, self.plane))

    def hand(self, inst, kind, buf, step, core=None):
        part = buf.at[self.at(step), self.core if core is None else core]
        return self.copy(inst, kind, part, part, (self.x, self.other, self.plane))

    def far(self, inst, slot):
        half = self.xs // 2
        return self.copy(inst, 1, slot, slot, (self.at(half), self.core, self.plane))

    def first(self, inst, buf):
        slot = buf.at[self.x, self.core, self.plane]
        self.far(inst, slot).start()
        self.fan(inst, 0, slot)

    def second(self, inst, buf, buf_far):
        slot = buf_far.at[self.at(self.xs // 2), self.core, self.plane]
        self.far(inst, slot).wait_recv()
        self.fan(inst, 2, slot)
        self.fanned(inst, 0, buf).wait_recv()
        self.hand(inst, 5, buf, 0).start()
        self.line(inst, 3, buf, 1).start()
        self.line(inst, 4, buf, self.xs - 1).start()

    def third_far(self, inst, buf_far):
        self.fanned(inst, 2, buf_far).wait_recv()
        self.hand(inst, 6, buf_far, self.xs // 2).start()

    def third_near(self, inst, buf_up, buf_down):
        self.line(inst, 4, buf_up, 1).wait_recv()
        self.hand(inst, 7, buf_up, 1).start()
        self.line(inst, 3, buf_down, 1).wait_recv()
        self.hand(inst, 8, buf_down, self.xs - 1).start()

    def handed(self, inst, kind, buf, step):
        self.hand(inst, kind, buf, step, self.other).wait_recv()

    def drain(self, inst, buf):
        slot = buf.at[self.x, self.core, self.plane]
        self.far(inst, slot).wait_send()
        self.fanned(inst, 0, buf).wait_send()
        self.fanned(inst, 2, buf).wait_send()
        self.line(inst, 3, buf, 1).wait_send()
        self.line(inst, 4, buf, 1).wait_send()
        for kind in (5, 6, 7, 8):
            self.hand(inst, kind, buf, 0).wait_send()


def kernel(
    nx,
    ny,
    ck,
    group,
    x_ref,
    mask_ref,
    g1_ref,
    w1_ref,
    gb1_ref,
    bw1_ref,
    ow1_ref,
    g2_ref,
    w2_ref,
    gb2_ref,
    bw2_ref,
    ow2_ref,
    g3_ref,
    ti_ref,
    tb_ref,
    to_ref,
    out_ref,
    q_ref,
    k_ref,
    v_ref,
    wt_ref,
    bias_ref,
    kb_ref,
    kc_ref,
    zs_ref,
    st_ref,
    rise_ref,
    first_ref,
    gc_ref,
    s_ref,
    o_ref,
    recv_m,
    recv_a,
    recv_b,
    send_z,
    recv_z,
    send_o,
    a_ref,
    ssem,
    rsem,
    zsem,
):
    n = nx * ny
    xs, planes = nx // 4, 2 * ny
    rows, res, ch = x_ref.shape
    tq = res // xs
    gx, gy = lax.axis_index("gx"), lax.axis_index("gy")
    me = gx * ny + gy
    core = lax.rem(gx, 2)
    x = lax.rem(gx // 2, xs)
    low = gx // (2 * xs)
    plane = low * ny + gy
    run = 2 * ny

    def place(x, core, plane):
        return (plane // ny * (2 * xs) + x * 2 + core, lax.rem(plane, ny))

    g = Gather(place, ssem, rsem)
    g.setup((x, core, plane), (xs, planes))
    barrier = pltpu.get_barrier_semaphore()

    def greet(*to):
        pl.semaphore_signal(barrier, inc=1, device_id=place(*to), device_id_type=MESH)

    for u in range(1, planes):
        greet(x, core, lax.rem(plane + u, planes))
    for u in range(1, xs):
        greet(g.at(u), core, plane)
    greet(x, 1 - core, plane)

    lane = lax.broadcasted_iota(jnp.int32, (16, 128), 1)
    vec = jnp.zeros((16, 128), F32)
    for t in range(rows):
        vec = jnp.where(lane == lax.rem(me * rows, 128) + t, mask_ref[t].astype(F32), vec)
    recv_m[x, core, plane] = vec.astype(BF16)


    def grouped(lo, hi, fn, size=2):
        def step(i, carry):
            fn([lo + i * size + e for e in range(size)])
            return carry

        lax.fori_loop(0, (hi - lo) // size, step, 0)

    def start_norm(batch):
        normed = [layer_norm(v.astype(F32), g1_ref[...]) for v in [x_ref[r] for r in batch]]
        for r, v in zip(batch, normed):
            a_ref[r] = v
        part = [bias_rows(bw1_ref[...], r, rows, v) for r, v in zip(batch, normed)]
        first_ref[...] = first_ref[...] + sum(part[1:], part[0])

    with jax.named_scope("norm"):
        first_ref[...] = jnp.zeros_like(first_ref)
        grouped(0, rows, start_norm)
        recv_a[x, core, plane] = first_ref[...].astype(BF16)

    with jax.named_scope("barrier"):
        pl.semaphore_wait(barrier, planes - 1 + xs - 1 + 1)
    g.first(0, recv_m)
    g.first(1, recv_a)
    with jax.named_scope("mask2"):
        g.second(0, recv_m, recv_m)

    def turn_weights(w_ref, gb_ref):
        wt_ref[...] = w_ref[...].astype(F32).T.astype(BF16)
        column = jnp.broadcast_to(gb_ref[...], (128, ch)).T
        for b in range(tq // 128):
            gc_ref[:, b * 128 : (b + 1) * 128] = column

    def project(batch, w_ref):
        normed = [a_ref[r] for r in batch]
        for r, v in zip(batch, [nn(v, w_ref[:, ch : 2 * ch]) for v in normed]):
            k_ref[r] = v.astype(BF16)
        for r, v in zip(batch, [nt(wt_ref[:ch], v) for v in normed]):
            q = (v * QSCALE).astype(BF16)
            for b in range(2 * xs):
                to = (b % xs * 2 + b // xs) * 128
                q_ref[r, :, to : to + 128] = q[:, b * 128 : (b + 1) * 128]
        for r, v in zip(batch, [nt(wt_ref[2 * ch : 3 * ch], v) for v in normed]):
            v_ref[r] = v.astype(BF16)

    def both(t, size):
        return [pl.ds(pl.multiple_of((t + e * xs) * size, size), size) for e in range(2)]

    def mixed(batch, t, ow_ref):
        a = [jnp.concatenate([a_ref[r, span, :] for span in both(t, 128)], axis=0) for r in batch]
        gl = [nt(wt_ref[3 * ch :], v) for v in a]
        gated = [o_ref[r] * jax.nn.sigmoid(v + gc_ref[...]) for r, v in zip(batch, gl)]
        gated = [v.T.astype(BF16) for v in gated]
        return [nn(v, ow_ref[...]) for v in gated]

    def batches(fn):
        def run(i, carry):
            fn([i * 8 + e for e in range(8)])
            return carry

        lax.fori_loop(0, rows // 8, run, 0)

    turn_weights(w1_ref, gb1_ref)

    with jax.named_scope("project"):
        grouped(0, rows, lambda batch: project(batch, w1_ref))
    with jax.named_scope("mask3"):
        g.third_far(0, recv_m)
        g.third_near(0, recv_m, recv_m)
    with jax.named_scope("a2"):
        g.second(1, recv_a, recv_a)
    with jax.named_scope("mask4"):
        g.handed(0, 5, recv_m, 0)
        g.handed(0, 6, recv_m, xs // 2)
        g.handed(0, 7, recv_m, 1)
        g.handed(0, 8, recv_m, xs - 1)

    for b in range(2 * xs):
        part = recv_m[b % xs, :, b // xs * ny : (b // xs + 1) * ny].astype(F32)
        mask = jnp.sum(jnp.sum(part, axis=0), axis=0)[:1]
        kb = (mask - 1.0) * BIG
        kb_ref[:, b * 128 : (b + 1) * 128] = kb
        kc_ref[b * 128 : (b + 1) * 128, :] = jnp.broadcast_to(kb, (128, 128)).T

    def start_bias(t):
        for e in range(2):
            blocks = [
                recv_a[t, c, e * ny : (e + 1) * ny].astype(F32) for c in range(2)
            ]
            for h in range(HEADS):
                part = jnp.concatenate(
                    [b[:, h * rows : (h + 1) * rows, :].reshape(64, res) for b in blocks], axis=0
                )
                to = slice(e * 128, (e + 1) * 128)
                bias_ref[t, h, :, to] = ((part + kb_ref[...]) * LOG2E).T

    def stage(r, z):
        st_ref[:, pl.ds(pl.multiple_of(r * rows, rows), rows), :] = z.reshape(
            tq // rows, rows, ch
        )

    def stage_turned(r, z):
        st_ref[:, pl.ds(r, rows, stride=rows), :] = z.reshape(tq // rows, rows, ch)

    mine = out_ref.at[:, pl.ds(pl.multiple_of(me * rows, rows), rows), :]

    def ship(kind, src, dst, t):
        for e, span in enumerate(both(t, run)):
            src[span] = st_ref[e * run : (e + 1) * run].astype(BF16).reshape(run, *src.shape[1:])

        @pl.loop(0, 2 * run)
        def _(u):
            v = lax.rem(u + plane * 2 + core, 2 * run)
            c, p = lax.rem(v, 2), v // 2
            to = place(t, c, p)
            d = to[0] * ny + to[1]

            @pl.when(d != me)
            def _():
                pltpu.make_async_remote_copy(
                    src_ref=src.at[d],
                    dst_ref=dst,
                    send_sem=zsem.at[kind, 0],
                    recv_sem=zsem.at[kind, 1],
                    device_id=to,
                    device_id_type=MESH,
                ).start()

    def shipped(kind, src, dst):
        rest = src.at[pl.ds(0, n - 1)]
        to = place(x, 1 - core, plane)
        for part, sem in ((rest, 0), (dst, 1)):
            copy = pltpu.make_async_remote_copy(
                src_ref=part,
                dst_ref=part,
                send_sem=zsem.at[kind, 0],
                recv_sem=zsem.at[kind, 1],
                device_id=to,
                device_id_type=MESH,
            )
            copy.wait_recv() if sem else copy.wait_send()

    near = 1 + core * (xs - 2)

    def tile_of(s, step=0, swap=False):
        side = xs - near if swap else near
        away = jnp.where(s == 0, 0, jnp.where(s == 1, xs // 2, jnp.where(s == 2, side, xs - side)))
        return lax.rem(x + step + away, xs)

    def rise_second(s):
        t = tile_of(s)
        g.second(2 + s, recv_b.at[t], recv_b.at[tile_of(s, xs // 2)])

    def rise_third(s):
        g.third_far(2 + s, recv_b.at[tile_of(s, xs // 2)])
        g.third_near(2 + s, recv_b.at[tile_of(s, 1)], recv_b.at[tile_of(s, xs - 1)])

    def start_tile(s, carry):
        t = tile_of(s)

        @pl.when(s == 0)
        def _():
            with jax.named_scope("wait0"):
                g.handed(1, 5, recv_a, 0)

        @pl.when(s == 1)
        def _():
            with jax.named_scope("wait1"):
                g.third_far(1, recv_a)
                g.handed(1, 6, recv_a, xs // 2)

        @pl.when(s == 2)
        def _():
            with jax.named_scope("wait2"):
                g.third_near(1, recv_a, recv_a)
                g.handed(1, 7, recv_a, 1)
                g.handed(1, 8, recv_a, xs - 1)

        with jax.named_scope("biasa"):
            start_bias(t)
        def start_finish(batch):
            out = mixed(batch, t, ow1_ref)
            old = [jnp.concatenate([x_ref[r, p, :] for p in both(t, 128)], axis=0) for r in batch]
            z1 = [(u.astype(F32) + v).astype(BF16).astype(F32) for u, v in zip(old, out)]
            for r, v in zip(batch, z1):
                stage(r, v)
            normed = [layer_norm(v, g2_ref[...]) for v in z1]
            part = [bias_rows(bw2_ref[...], r, rows, v) for r, v in zip(batch, normed)]
            rise_ref[...] = rise_ref[...] + sum(part[1:], part[0])

        def start_after(i):
            @pl.when((s > 1) & (i == 0))
            def _():
                with jax.named_scope("rise3"):
                    rise_third(s - 2)

            @pl.when((s > 0) & (i == (rows // 2 - 1) // group))
            def _():
                with jax.named_scope("rise2"):
                    rise_second(s - 1)

        with jax.named_scope("att1"):
            attend_tile(ck, group, t, q_ref, k_ref, v_ref, bias_ref, s_ref, o_ref,
                start_after)
        with jax.named_scope("tail1"):
            rise_ref[...] = jnp.zeros_like(rise_ref)
            batches(start_finish)
        recv_b[t, x, core, plane] = rise_ref[...].astype(BF16)
        with jax.named_scope("ship1"):
            g.first(2 + s, recv_b.at[t])
            ship(0, send_z, recv_z.at[me], t)
        return carry

    lax.fori_loop(0, xs, start_tile, 0)
    turn_weights(w2_ref, gb2_ref)
    with jax.named_scope("rise3d"):
        rise_third(xs - 2)
    with jax.named_scope("rise2e"):
        rise_second(xs - 1)
    with jax.named_scope("waitz"):
        shipped(0, send_z, recv_z.at[pl.ds(0, n - 1)])
    recv_z[me] = send_z[me]
    zs_ref[...] = recv_z[...].astype(F32)

    def end_norm(batch):
        z1 = [zs_ref[:, pl.ds(d, rows, stride=rows), :].reshape(res, ch) for d in batch]
        for d, v in zip(batch, [layer_norm(v, g2_ref[...]) for v in z1]):
            a_ref[d] = v

    with jax.named_scope("norm2"):
        grouped(0, rows, end_norm)
    with jax.named_scope("rise3e"):
        rise_third(xs - 1)
    with jax.named_scope("project2"):
        grouped(0, rows, lambda batch: project(batch, w2_ref))

    def rise_done(s, carry):
        g.handed(2 + s, 5, recv_b.at[tile_of(s, 0, True)], 0)
        g.handed(2 + s, 6, recv_b.at[tile_of(s, xs // 2, True)], xs // 2)
        g.handed(2 + s, 7, recv_b.at[tile_of(s, 1, True)], 1)
        g.handed(2 + s, 8, recv_b.at[tile_of(s, xs - 1, True)], xs - 1)
        return carry

    with jax.named_scope("handed"):
        lax.fori_loop(0, xs, rise_done, 0)

    def end_bias(t):
        def keys_of(b, carry):
            e, c = lax.rem(b // 2, 2), lax.rem(b, 2)
            keys = pl.ds(pl.multiple_of((e * 2 * xs + b // 4 * 2 + c) * 64, 64), 64)
            kc = kc_ref[keys, :]
            block = recv_b[t, b // 4, c, pl.ds(e * ny, ny)].astype(F32)
            for h in range(HEADS):
                part = block[:, h * rows : (h + 1) * rows, :].reshape(64, tq)
                for w in range(tq // 128):
                    to = slice(w * 128, (w + 1) * 128)
                    bias_ref[t, h, keys, to] = (part[:, to] + kc) * LOG2E
            return carry

        lax.fori_loop(0, 4 * xs, keys_of, 0)

    def end_tile(s, carry):
        t = tile_of(lax.rem(s + 1, xs))
        with jax.named_scope("biasb"):
            end_bias(t)

        def end_finish(batch):
            out = mixed(batch, t, ow2_ref)
            z1 = [
                jnp.concatenate(
                    [
                        zs_ref[span, pl.ds(r, rows, stride=rows), :].reshape(128, ch)
                        for span in both(t, run)
                    ],
                    axis=0,
                )
                for r in batch
            ]
            z2 = [(u + v).astype(BF16).astype(F32) for u, v in zip(z1, out)]
            normed = [layer_norm(v, g3_ref[...]) for v in z2]
            hid = [nn(v, ti_ref[...]) + tb_ref[...] for v in normed]
            hid = [jnp.maximum(v, 0.0).astype(BF16) for v in hid]
            last = [nn(v, to_ref[...]) for v in hid]
            for r, u, v in zip(batch, z2, last):
                stage_turned(r, u + v)

        with jax.named_scope("att2"):
            attend_tile(ck, group, t, q_ref, k_ref, v_ref, bias_ref, s_ref, o_ref,
                lambda r: None)
        with jax.named_scope("tail2"):
            batches(end_finish)
        with jax.named_scope("ship2"):
            ship(1, send_o, mine, t)
        return carry

    lax.fori_loop(0, xs, end_tile, 0)
    with jax.named_scope("drain"):
        g.drain(0, recv_m)
        g.drain(1, recv_a)

        def drain_rise(s, carry):
            g.drain(2 + s, recv_b.at[tile_of(s)])
            return carry

        lax.fori_loop(0, xs, drain_rise, 0)
    with jax.named_scope("waito"):
        own = pltpu.make_async_copy(send_o.at[me], mine, zsem.at[0, 0])
        own.start()
        shipped(1, send_o, out_ref.at[:, pl.ds(0, res - rows), :])
        own.wait()


def solution(mesh):
    nx, ny = mesh.shape["gx"], mesh.shape["gy"]
    n, xs = nx * ny, nx // 4

    def local(x, mask, g1, w1, gb1, bw1, ow1, g2, w2, gb2, bw2, ow2, g3, ti, tb, to):
        rows, res, ch = x.shape
        tq, ck = res // xs, 512
        vmem = pl.BlockSpec(memory_space=pltpu.VMEM)
        row = lambda t: t.reshape(1, -1)
        return pl.pallas_call(
            functools.partial(kernel, nx, ny, ck, min(rows, 4)),
            out_shape=jax.ShapeDtypeStruct(x.shape, x.dtype),
            in_specs=[vmem, pl.BlockSpec(memory_space=pltpu.SMEM)] + [vmem] * 14,
            out_specs=pl.BlockSpec(memory_space=pl.ANY),
            scratch_shapes=[
                pltpu.VMEM((rows, ch, res), BF16),
                pltpu.VMEM((rows, res, ch), BF16),
                pltpu.VMEM((rows, ch, res), BF16),
                pltpu.VMEM((4 * ch, ch), BF16),
                pltpu.VMEM((xs, HEADS, res, tq), F32),
                pltpu.VMEM((1, res), F32),
                pltpu.VMEM((res, 128), F32),
                pltpu.VMEM((n, rows * rows, ch), F32),
                pltpu.VMEM((tq // rows, rows * rows, ch), F32),
                pltpu.VMEM((HEADS * rows, tq), F32),
                pltpu.VMEM((HEADS * rows, res), F32),
                pltpu.VMEM((ch, tq), F32),
                pltpu.VMEM((2 * res, tq), F32),
                pltpu.VMEM((rows, ch, tq), F32),
                pltpu.VMEM((xs, 2, 2 * ny, 16, 128), BF16),
                pltpu.VMEM((xs, 2, 2 * ny, HEADS * rows, res), BF16),
                pltpu.VMEM((xs, xs, 2, 2 * ny, HEADS * rows, tq), BF16),
                pltpu.VMEM((n, rows * rows, ch), BF16),
                pltpu.VMEM((n, rows * rows, ch), BF16),
                pltpu.VMEM((n, rows, rows, ch), BF16),
                pltpu.VMEM((rows, res, ch), BF16),
                pltpu.SemaphoreType.DMA((2 + xs, 9)),
                pltpu.SemaphoreType.DMA((2 + xs, 9)),
                pltpu.SemaphoreType.DMA((2, 2)),
            ],
            compiler_params=pltpu.CompilerParams(
                collective_id=0, has_side_effects=True, vmem_limit_bytes=66 * 1000 * 1000,
            ),
        )(
            x, mask, row(g1), w1, row(gb1), bw1.T, ow1, row(g2), w2,
            row(gb2), bw2.T, ow2, row(g3), ti, row(tb), to,
        )

    placed = (P(("gx", "gy"), None, None), P(("gx", "gy"))) + (P(),) * 14
    return jax.shard_map(
        local, mesh=mesh, in_specs=placed, out_specs=P(("gx", "gy"), None, None), check_vma=False
    )
```

```python
import functools
import math

import jax
import jax.numpy as jnp
from jax import lax
from jax.experimental import pallas as pl
from jax.experimental.pallas import tpu as pltpu
from jax.sharding import PartitionSpec as P

HEADS = 4
HEAD_DIM = 32
BIG = 1000000000.0
LOG2E = math.log2(math.e)
QSCALE = HEAD_DIM ** (-0.5) * LOG2E
MESH = pl.DeviceIdType.MESH
F32 = jnp.float32
BF16 = jnp.bfloat16


def nn(a, b):
    return lax.dot_general(a, b, (((1,), (0,)), ((), ())), preferred_element_type=F32)


def nt(a, b):
    return lax.dot_general(a, b, (((1,), (1,)), ((), ())), preferred_element_type=F32)


def layer_norm(x, gain):
    mean = jnp.mean(x, axis=-1, keepdims=True)
    cent = x - mean
    var = jnp.mean(cent * cent, axis=-1, keepdims=True)
    return (cent * lax.rsqrt(var + 1e-05) * gain).astype(BF16)


def bias_rows(w, r, rows, normed):
    shape = (HEADS * rows, HEADS)
    place = lax.broadcasted_iota(jnp.int32, shape, 0) == (
        lax.broadcasted_iota(jnp.int32, shape, 1) * rows + r
    )
    spread = nn(place.astype(F32).astype(BF16), w).astype(BF16)
    return nt(spread, normed)


def attend_tile(ck, group, t, q_ref, k_ref, v_ref, bias_ref, s_ref, o_ref, after):
    rows, res, ch = k_ref.shape
    tq = s_ref.shape[1]
    s_refs = [s_ref.at[:res], s_ref.at[res:]]
    lanes = pl.ds(pl.multiple_of(t * tq, tq), tq)
    chunks = res // ck

    def query(r, h):
        q = q_ref[r, :, lanes]
        row = lax.broadcasted_iota(jnp.int32, q.shape, 0)
        return jnp.where((row >= h * HEAD_DIM) & (row < (h + 1) * HEAD_DIM), q, jnp.zeros_like(q))

    def score(r, h, c, q, top):
        span = slice(c * ck, (c + 1) * ck)
        s = nn(k_ref[r, span, :], q) + bias_ref[t, h, span, :]
        s_refs[h % 2][span, :] = s
        m = jnp.max(s.reshape(ck // 8, 8, tq), axis=0)
        return m if top is None else jnp.maximum(top, m)

    def mix(r, h, c, top, acc):
        span = slice(c * ck, (c + 1) * ck)
        w = jnp.exp2((s_refs[h % 2][span, :] - top).astype(BF16))
        v = jnp.concatenate(
            [v_ref[r, h * HEAD_DIM : (h + 1) * HEAD_DIM, span], jnp.ones((16, ck), BF16)], axis=0
        )
        o = nn(v, w)
        return o if acc is None else acc + o

    q, top = query(0, 0), None
    for c in range(chunks):
        top = score(0, 0, c, q, top)

    def row(r, top):
        outs = []
        for h in range(HEADS):
            peak = jnp.max(top, axis=0, keepdims=True)
            nh = (h + 1) % HEADS
            nr = r if h < HEADS - 1 else jnp.minimum(r + 1, rows - 1)
            q, top, acc = query(nr, nh), None, None
            for c in range(chunks):
                top = score(nr, nh, c, q, top)
                acc = mix(r, h, c, peak, acc)
            outs.append(acc[:HEAD_DIM] / acc[HEAD_DIM : HEAD_DIM + 1])
        o_ref[r] = jnp.concatenate(outs, axis=0)
        return top

    def body(i, top):
        for e in range(group):
            top = row(i * group + e, top)
        after(i)
        return top

    lax.fori_loop(0, rows // group, body, top)


class Gather:
    def __init__(self, place, ssem, rsem):
        self.place, self.ssem, self.rsem = place, ssem, rsem

    def copy(self, inst, kind, src, dst, to):
        return pltpu.make_async_remote_copy(
            src_ref=src,
            dst_ref=dst,
            send_sem=self.ssem.at[inst, kind],
            recv_sem=self.rsem.at[inst, kind],
            device_id=self.place(*to),
            device_id_type=MESH,
        )

    def setup(self, me, sizes):
        self.x, self.core, self.plane = me
        self.xs, self.planes = sizes
        self.other = 1 - self.core

    def at(self, step):
        return lax.rem(self.x + step, self.xs)

    def fan(self, inst, kind, slot):
        @pl.loop(1, self.planes)
        def _(u):
            p = lax.rem(self.plane + u, self.planes)
            self.copy(inst, kind, slot, slot, (self.x, self.core, p)).start()

    def fanned(self, inst, kind, buf):
        rest = buf.at[self.x, self.core, pl.ds(0, self.planes - 1)]
        return self.copy(inst, kind, rest, rest, (self.x, self.other, self.plane))

    def line(self, inst, kind, buf, step):
        part = buf.at[self.x, self.core]
        return self.copy(inst, kind, part, part, (self.at(step), self.core, self.plane))

    def hand(self, inst, kind, buf, step, core=None):
        part = buf.at[self.at(step), self.core if core is None else core]
        return self.copy(inst, kind, part, part, (self.x, self.other, self.plane))

    def far(self, inst, slot):
        half = self.xs // 2
        return self.copy(inst, 1, slot, slot, (self.at(half), self.core, self.plane))

    def first(self, inst, buf):
        slot = buf.at[self.x, self.core, self.plane]
        self.far(inst, slot).start()
        self.fan(inst, 0, slot)

    def second(self, inst, buf, buf_far):
        slot = buf_far.at[self.at(self.xs // 2), self.core, self.plane]
        self.far(inst, slot).wait_recv()
        self.fan(inst, 2, slot)
        self.fanned(inst, 0, buf).wait_recv()
        self.hand(inst, 5, buf, 0).start()
        self.line(inst, 3, buf, 1).start()
        self.line(inst, 4, buf, self.xs - 1).start()

    def third_far(self, inst, buf_far):
        self.fanned(inst, 2, buf_far).wait_recv()
        self.hand(inst, 6, buf_far, self.xs // 2).start()

    def third_near(self, inst, buf_of):
        for step in (1 + self.other * (self.xs - 2), 1 + self.core * (self.xs - 2)):
            down = (step - 1) // (self.xs - 2)
            buf = buf_of(step)
            self.line(inst, 4 - down, buf, 1).wait_recv()
            self.hand(inst, 7 + down, buf, step).start()

    def handed(self, inst, kind, buf, step):
        self.hand(inst, kind, buf, step, self.other).wait_recv()

    def drain(self, inst, buf):
        slot = buf.at[self.x, self.core, self.plane]
        self.far(inst, slot).wait_send()
        self.fanned(inst, 0, buf).wait_send()
        self.fanned(inst, 2, buf).wait_send()
        self.line(inst, 3, buf, 1).wait_send()
        self.line(inst, 4, buf, 1).wait_send()
        for kind in (5, 6, 7, 8):
            self.hand(inst, kind, buf, 0).wait_send()


def kernel(
    nx,
    ny,
    ck,
    group,
    x_ref,
    mask_ref,
    g1_ref,
    w1_ref,
    gb1_ref,
    bw1_ref,
    ow1_ref,
    g2_ref,
    w2_ref,
    gb2_ref,
    bw2_ref,
    ow2_ref,
    g3_ref,
    ti_ref,
    tb_ref,
    to_ref,
    out_ref,
    q_ref,
    k_ref,
    v_ref,
    wt_ref,
    bias_ref,
    kb_ref,
    kc_ref,
    zs_ref,
    st_ref,
    rise_ref,
    first_ref,
    gc_ref,
    s_ref,
    o_ref,
    recv_m,
    recv_a,
    recv_b,
    send_z,
    recv_z,
    send_o,
    a_ref,
    ssem,
    rsem,
    zsem,
):
    n = nx * ny
    xs, planes = nx // 4, 2 * ny
    rows, res, ch = x_ref.shape
    tq = res // xs
    gx, gy = lax.axis_index("gx"), lax.axis_index("gy")
    me = gx * ny + gy
    core = lax.rem(gx, 2)
    x = lax.rem(gx // 2, xs)
    low = gx // (2 * xs)
    plane = low * ny + gy
    run = 2 * ny

    def place(x, core, plane):
        return (plane // ny * (2 * xs) + x * 2 + core, lax.rem(plane, ny))

    g = Gather(place, ssem, rsem)
    g.setup((x, core, plane), (xs, planes))
    barrier = pltpu.get_barrier_semaphore()

    def greet(*to):
        pl.semaphore_signal(barrier, inc=1, device_id=place(*to), device_id_type=MESH)

    for u in range(1, planes):
        greet(x, core, lax.rem(plane + u, planes))
    for u in range(1, xs):
        greet(g.at(u), core, plane)
    greet(x, 1 - core, plane)

    lane = lax.broadcasted_iota(jnp.int32, (16, 128), 1)
    vec = jnp.zeros((16, 128), F32)
    for t in range(rows):
        vec = jnp.where(lane == lax.rem(me * rows, 128) + t, mask_ref[t].astype(F32), vec)
    recv_m[x, core, plane] = vec.astype(BF16)


    def grouped(lo, hi, fn, size=2):
        def step(i, carry):
            fn([lo + i * size + e for e in range(size)])
            return carry

        lax.fori_loop(0, (hi - lo) // size, step, 0)

    def start_norm(batch):
        normed = [layer_norm(v.astype(F32), g1_ref[...]) for v in [x_ref[r] for r in batch]]
        for r, v in zip(batch, normed):
            a_ref[r] = v
        part = [bias_rows(bw1_ref[...], r, rows, v) for r, v in zip(batch, normed)]
        first_ref[...] = first_ref[...] + sum(part[1:], part[0])

    with jax.named_scope("norm"):
        first_ref[...] = jnp.zeros_like(first_ref)
        grouped(0, rows, start_norm)
        recv_a[x, core, plane] = first_ref[...].astype(BF16)

    with jax.named_scope("barrier"):
        pl.semaphore_wait(barrier, planes - 1 + xs - 1 + 1)
    g.first(0, recv_m)
    g.first(1, recv_a)
    def turn_weights(w_ref, gb_ref):
        wt_ref[...] = w_ref[...].astype(F32).T.astype(BF16)
        column = jnp.broadcast_to(gb_ref[...], (128, ch)).T
        for b in range(tq // 128):
            gc_ref[:, b * 128 : (b + 1) * 128] = column

    def project(batch, w_ref):
        normed = [a_ref[r] for r in batch]
        for r, v in zip(batch, [nn(v, w_ref[:, ch : 2 * ch]) for v in normed]):
            k_ref[r] = v.astype(BF16)
        for r, v in zip(batch, [nt(wt_ref[:ch], v) for v in normed]):
            q = (v * QSCALE).astype(BF16)
            for b in range(2 * xs):
                to = (b % xs * 2 + b // xs) * 128
                q_ref[r, :, to : to + 128] = q[:, b * 128 : (b + 1) * 128]
        for r, v in zip(batch, [nt(wt_ref[2 * ch : 3 * ch], v) for v in normed]):
            v_ref[r] = v.astype(BF16)

    def both(t, size):
        return [pl.ds(pl.multiple_of((t + e * xs) * size, size), size) for e in range(2)]

    def mixed(batch, t, ow_ref):
        a = [jnp.concatenate([a_ref[r, span, :] for span in both(t, 128)], axis=0) for r in batch]
        gl = [nt(wt_ref[3 * ch :], v) for v in a]
        gated = [o_ref[r] * jax.nn.sigmoid(v + gc_ref[...]) for r, v in zip(batch, gl)]
        gated = [v.T.astype(BF16) for v in gated]
        return [nn(v, ow_ref[...]) for v in gated]

    def batches(fn):
        def run(i, carry):
            fn([i * 8 + e for e in range(8)])
            return carry

        lax.fori_loop(0, rows // 8, run, 0)

    turn_weights(w1_ref, gb1_ref)

    with jax.named_scope("project"):
        grouped(0, rows, lambda batch: project(batch, w1_ref))
    with jax.named_scope("mask2"):
        g.second(0, recv_m, recv_m)
    with jax.named_scope("mask3"):
        g.third_far(0, recv_m)
        g.third_near(0, lambda step: recv_m)
    with jax.named_scope("a2"):
        g.second(1, recv_a, recv_a)
    with jax.named_scope("mask4"):
        g.handed(0, 5, recv_m, 0)
        g.handed(0, 6, recv_m, xs // 2)
        g.handed(0, 7, recv_m, 1)
        g.handed(0, 8, recv_m, xs - 1)

    for b in range(2 * xs):
        part = recv_m[b % xs, :, b // xs * ny : (b // xs + 1) * ny].astype(F32)
        mask = jnp.sum(jnp.sum(part, axis=0), axis=0)[:1]
        kb = (mask - 1.0) * BIG
        kb_ref[:, b * 128 : (b + 1) * 128] = kb
        kc_ref[b * 128 : (b + 1) * 128, :] = jnp.broadcast_to(kb, (128, 128)).T

    def start_bias(t):
        for e in range(2):
            blocks = [
                recv_a[t, c, e * ny : (e + 1) * ny].astype(F32) for c in range(2)
            ]
            for h in range(HEADS):
                part = jnp.concatenate(
                    [b[:, h * rows : (h + 1) * rows, :].reshape(64, res) for b in blocks], axis=0
                )
                to = slice(e * 128, (e + 1) * 128)
                bias_ref[t, h, :, to] = ((part + kb_ref[...]) * LOG2E).T

    def stage(r, z):
        st_ref[:, pl.ds(pl.multiple_of(r * rows, rows), rows), :] = z.reshape(
            tq // rows, rows, ch
        )

    def stage_turned(r, z):
        st_ref[:, pl.ds(r, rows, stride=rows), :] = z.reshape(tq // rows, rows, ch)

    mine = out_ref.at[:, pl.ds(pl.multiple_of(me * rows, rows), rows), :]

    def load(src, t):
        for e, span in enumerate(both(t, run)):
            src[span] = st_ref[e * run : (e + 1) * run].astype(BF16).reshape(run, *src.shape[1:])

    def spread(kind, src, dst, t):
        def send(v):
            c, p = lax.rem(v, 2), v // 2
            to = place(t, c, p)
            d = to[0] * ny + to[1]
            return pltpu.make_async_remote_copy(
                src_ref=src.at[d],
                dst_ref=dst,
                send_sem=zsem.at[kind, 0],
                recv_sem=zsem.at[kind, 1],
                device_id=to,
                device_id_type=MESH,
            )

        here = plane * 2 + core

        @pl.when(t != x)
        def _():
            send(here).start()

        @pl.loop(1, 2 * run)
        def _(u):
            send(lax.rem(here + u, 2 * run)).start()

    def shipped(kind, src, dst):
        rest = src.at[pl.ds(0, n - 1)]
        to = place(x, 1 - core, plane)
        for part, sem in ((rest, 0), (dst, 1)):
            copy = pltpu.make_async_remote_copy(
                src_ref=part,
                dst_ref=part,
                send_sem=zsem.at[kind, 0],
                recv_sem=zsem.at[kind, 1],
                device_id=to,
                device_id_type=MESH,
            )
            copy.wait_recv() if sem else copy.wait_send()

    near = 1 + core * (xs - 2)

    def tile_of(s, step=0, swap=False):
        side = xs - near if swap else near
        away = jnp.where(s == 0, 0, jnp.where(s == 1, xs // 2, jnp.where(s == 2, side, xs - side)))
        return lax.rem(x + step + away, xs)

    def rise_second(s):
        t = tile_of(s)
        g.second(2 + s, recv_b.at[t], recv_b.at[tile_of(s, xs // 2)])

    def rise_third(s):
        g.third_far(2 + s, recv_b.at[tile_of(s, xs // 2)])
        g.third_near(2 + s, lambda step: recv_b.at[tile_of(s, step)])

    def start_tile(s, carry):
        t = tile_of(s)

        @pl.when(s == 0)
        def _():
            with jax.named_scope("wait0"):
                g.handed(1, 5, recv_a, 0)

        @pl.when(s == 1)
        def _():
            with jax.named_scope("wait1"):
                g.handed(1, 6, recv_a, xs // 2)

        @pl.when(s == 2)
        def _():
            with jax.named_scope("wait2"):
                g.handed(1, 7 + core, recv_a, near)

        @pl.when(s == 3)
        def _():
            with jax.named_scope("wait3"):
                g.handed(1, 8 - core, recv_a, xs - near)

        with jax.named_scope("biasa"):
            start_bias(t)
        def start_finish(batch):
            out = mixed(batch, t, ow1_ref)
            old = [jnp.concatenate([x_ref[r, p, :] for p in both(t, 128)], axis=0) for r in batch]
            z1 = [(u.astype(F32) + v).astype(BF16).astype(F32) for u, v in zip(old, out)]
            for r, v in zip(batch, z1):
                stage(r, v)
            normed = [layer_norm(v, g2_ref[...]) for v in z1]
            part = [bias_rows(bw2_ref[...], r, rows, v) for r, v in zip(batch, normed)]
            rise_ref[...] = rise_ref[...] + sum(part[1:], part[0])

        def start_after(i):
            @pl.when((s > 1) & (i == 0))
            def _():
                with jax.named_scope("rise3"):
                    rise_third(s - 2)

            @pl.when((s > 0) & (i == (rows // 2 - 1) // group))
            def _():
                with jax.named_scope("rise2"):
                    rise_second(s - 1)

            @pl.when((s == 1) & (i == rows // group - 1))
            def _():
                with jax.named_scope("near1"):
                    g.third_near(1, lambda step: recv_a)

        with jax.named_scope("att1"):
            attend_tile(ck, group, t, q_ref, k_ref, v_ref, bias_ref, s_ref, o_ref,
                start_after)
        with jax.named_scope("tail1"):
            rise_ref[...] = jnp.zeros_like(rise_ref)
            batches(start_finish)
        recv_b[t, x, core, plane] = rise_ref[...].astype(BF16)
        with jax.named_scope("ship1"):
            g.first(2 + s, recv_b.at[t])

        @pl.when(s == 0)
        def _():
            with jax.named_scope("far1"):
                g.third_far(1, recv_a)

        with jax.named_scope("ship1"):
            load(send_z, t)
            spread(0, send_z, recv_z.at[me], t)

        return carry

    lax.fori_loop(0, xs, start_tile, 0)
    turn_weights(w2_ref, gb2_ref)
    with jax.named_scope("rise2e"):
        rise_second(xs - 1)
    with jax.named_scope("rise3d"):
        rise_third(xs - 2)
    with jax.named_scope("waitz"):
        shipped(0, send_z, recv_z.at[pl.ds(0, n - 1)])
    recv_z[me] = send_z[me]
    zs_ref[...] = recv_z[...].astype(F32)

    def end_norm(batch):
        z1 = [zs_ref[:, pl.ds(d, rows, stride=rows), :].reshape(res, ch) for d in batch]
        for d, v in zip(batch, [layer_norm(v, g2_ref[...]) for v in z1]):
            a_ref[d] = v

    with jax.named_scope("norm2"):
        grouped(0, rows, end_norm)
    with jax.named_scope("rise3e"):
        rise_third(xs - 1)
    with jax.named_scope("project2"):
        grouped(0, rows, lambda batch: project(batch, w2_ref))

    def rise_done(s, carry):
        g.handed(2 + s, 5, recv_b.at[tile_of(s, 0, True)], 0)
        g.handed(2 + s, 6, recv_b.at[tile_of(s, xs // 2, True)], xs // 2)
        g.handed(2 + s, 7, recv_b.at[tile_of(s, 1, True)], 1)
        g.handed(2 + s, 8, recv_b.at[tile_of(s, xs - 1, True)], xs - 1)
        return carry

    with jax.named_scope("handed"):
        lax.fori_loop(0, xs, rise_done, 0)

    def end_bias(t):
        def keys_of(b, carry):
            e, c = lax.rem(b // 2, 2), lax.rem(b, 2)
            keys = pl.ds(pl.multiple_of((e * 2 * xs + b // 4 * 2 + c) * 64, 64), 64)
            kc = kc_ref[keys, :]
            block = recv_b[t, b // 4, c, pl.ds(e * ny, ny)].astype(F32)
            for h in range(HEADS):
                part = block[:, h * rows : (h + 1) * rows, :].reshape(64, tq)
                for w in range(tq // 128):
                    to = slice(w * 128, (w + 1) * 128)
                    bias_ref[t, h, keys, to] = (part[:, to] + kc) * LOG2E
            return carry

        lax.fori_loop(0, 4 * xs, keys_of, 0)

    def end_tile(s, carry):
        t = tile_of(lax.rem(s + 1, xs))
        with jax.named_scope("biasb"):
            end_bias(t)

        def end_finish(batch):
            out = mixed(batch, t, ow2_ref)
            z1 = [
                jnp.concatenate(
                    [
                        zs_ref[span, pl.ds(r, rows, stride=rows), :].reshape(128, ch)
                        for span in both(t, run)
                    ],
                    axis=0,
                )
                for r in batch
            ]
            z2 = [(u + v).astype(BF16).astype(F32) for u, v in zip(z1, out)]
            normed = [layer_norm(v, g3_ref[...]) for v in z2]
            hid = [nn(v, ti_ref[...]) + tb_ref[...] for v in normed]
            hid = [jnp.maximum(v, 0.0).astype(BF16) for v in hid]
            last = [nn(v, to_ref[...]) for v in hid]
            for r, u, v in zip(batch, z2, last):
                stage_turned(r, u + v)

        with jax.named_scope("att2"):
            attend_tile(ck, group, t, q_ref, k_ref, v_ref, bias_ref, s_ref, o_ref,
                lambda r: None)
        with jax.named_scope("tail2"):
            batches(end_finish)
        with jax.named_scope("ship2"):
            load(send_o, t)
            spread(1, send_o, mine, t)
        return carry

    lax.fori_loop(0, xs, end_tile, 0)
    with jax.named_scope("drain"):
        g.drain(0, recv_m)
        g.drain(1, recv_a)

        def drain_rise(s, carry):
            g.drain(2 + s, recv_b.at[tile_of(s)])
            return carry

        lax.fori_loop(0, xs, drain_rise, 0)
    with jax.named_scope("waito"):
        own = pltpu.make_async_copy(send_o.at[me], mine, zsem.at[0, 0])
        own.start()
        shipped(1, send_o, out_ref.at[:, pl.ds(0, res - rows), :])
        own.wait()


def solution(mesh):
    nx, ny = mesh.shape["gx"], mesh.shape["gy"]
    n, xs = nx * ny, nx // 4

    def local(x, mask, g1, w1, gb1, bw1, ow1, g2, w2, gb2, bw2, ow2, g3, ti, tb, to):
        rows, res, ch = x.shape
        tq, ck = res // xs, 512
        vmem = pl.BlockSpec(memory_space=pltpu.VMEM)
        row = lambda t: t.reshape(1, -1)
        return pl.pallas_call(
            functools.partial(kernel, nx, ny, ck, min(rows, 4)),
            out_shape=jax.ShapeDtypeStruct(x.shape, x.dtype),
            in_specs=[vmem, pl.BlockSpec(memory_space=pltpu.SMEM)] + [vmem] * 14,
            out_specs=pl.BlockSpec(memory_space=pl.ANY),
            scratch_shapes=[
                pltpu.VMEM((rows, ch, res), BF16),
                pltpu.VMEM((rows, res, ch), BF16),
                pltpu.VMEM((rows, ch, res), BF16),
                pltpu.VMEM((4 * ch, ch), BF16),
                pltpu.VMEM((xs, HEADS, res, tq), F32),
                pltpu.VMEM((1, res), F32),
                pltpu.VMEM((res, 128), F32),
                pltpu.VMEM((n, rows * rows, ch), F32),
                pltpu.VMEM((tq // rows, rows * rows, ch), F32),
                pltpu.VMEM((HEADS * rows, tq), F32),
                pltpu.VMEM((HEADS * rows, res), F32),
                pltpu.VMEM((ch, tq), F32),
                pltpu.VMEM((2 * res, tq), F32),
                pltpu.VMEM((rows, ch, tq), F32),
                pltpu.VMEM((xs, 2, 2 * ny, 16, 128), BF16),
                pltpu.VMEM((xs, 2, 2 * ny, HEADS * rows, res), BF16),
                pltpu.VMEM((xs, xs, 2, 2 * ny, HEADS * rows, tq), BF16),
                pltpu.VMEM((n, rows * rows, ch), BF16),
                pltpu.VMEM((n, rows * rows, ch), BF16),
                pltpu.VMEM((n, rows, rows, ch), BF16),
                pltpu.VMEM((rows, res, ch), BF16),
                pltpu.SemaphoreType.DMA((2 + xs, 9)),
                pltpu.SemaphoreType.DMA((2 + xs, 9)),
                pltpu.SemaphoreType.DMA((2, 2)),
            ],
            compiler_params=pltpu.CompilerParams(
                collective_id=0, has_side_effects=True, vmem_limit_bytes=66 * 1000 * 1000,
            ),
        )(
            x, mask, row(g1), w1, row(gb1), bw1.T, ow1, row(g2), w2,
            row(gb2), bw2.T, ow2, row(g3), ti, row(tb), to,
        )

    placed = (P(("gx", "gy"), None, None), P(("gx", "gy"))) + (P(),) * 14
    return jax.shard_map(
        local, mesh=mesh, in_specs=placed, out_specs=P(("gx", "gy"), None, None), check_vma=False
    )
```

```python
import functools
import math

import jax
import jax.numpy as jnp
from jax import lax
from jax.experimental import pallas as pl
from jax.experimental.pallas import tpu as pltpu
from jax.sharding import PartitionSpec as P

HEADS = 4
HEAD_DIM = 32
BIG = 1000000000.0
LOG2E = math.log2(math.e)
QSCALE = HEAD_DIM ** (-0.5) * LOG2E
MESH = pl.DeviceIdType.MESH
F32 = jnp.float32
BF16 = jnp.bfloat16


def nn(a, b):
    return lax.dot_general(a, b, (((1,), (0,)), ((), ())), preferred_element_type=F32)


def nt(a, b):
    return lax.dot_general(a, b, (((1,), (1,)), ((), ())), preferred_element_type=F32)


def layer_norm(x, gain):
    mean = jnp.mean(x, axis=-1, keepdims=True)
    cent = x - mean
    var = jnp.mean(cent * cent, axis=-1, keepdims=True)
    return (cent * lax.rsqrt(var + 1e-05) * gain).astype(BF16)


def bias_rows(w, r, rows, normed):
    shape = (HEADS * rows, HEADS)
    place = lax.broadcasted_iota(jnp.int32, shape, 0) == (
        lax.broadcasted_iota(jnp.int32, shape, 1) * rows + r
    )
    spread = nn(place.astype(F32).astype(BF16), w).astype(BF16)
    return nt(spread, normed)


def attend_tile(ck, group, t, q_ref, k_ref, v_ref, bias_ref, s_ref, o_ref, after, heads):
    rows, res, ch = k_ref.shape
    pairs = len(heads)
    tq = s_ref.shape[1]
    s_refs = [s_ref.at[:res], s_ref.at[res:]]
    lanes = pl.ds(pl.multiple_of(t * tq, tq), tq)
    chunks = res // ck

    def query(r, h):
        q = q_ref[r, :, lanes]
        row = lax.broadcasted_iota(jnp.int32, q.shape, 0)
        return jnp.where((row >= h * HEAD_DIM) & (row < (h + 1) * HEAD_DIM), q, jnp.zeros_like(q))

    def score(r, h, c, q, top):
        span = slice(c * ck, (c + 1) * ck)
        s = nn(k_ref[r, span, :], q) + bias_ref[t, h, span, :]
        s_refs[h % 2][span, :] = s
        m = jnp.max(s.reshape(ck // 8, 8, tq), axis=0)
        return m if top is None else jnp.maximum(top, m)

    def mix(r, h, c, top, acc):
        span = slice(c * ck, (c + 1) * ck)
        w = jnp.exp2((s_refs[h % 2][span, :] - top).astype(BF16))
        v = jnp.concatenate(
            [v_ref[r, h * HEAD_DIM : (h + 1) * HEAD_DIM, span], jnp.ones((16, ck), BF16)], axis=0
        )
        o = nn(v, w)
        return o if acc is None else acc + o

    q, top = query(0, heads[0]), None
    for c in range(chunks):
        top = score(0, heads[0], c, q, top)

    def row(r, top):
        outs = []
        for at, h in enumerate(heads):
            peak = jnp.max(top, axis=0, keepdims=True)
            nh = heads[(at + 1) % pairs]
            nr = r if at < pairs - 1 else jnp.minimum(r + 1, rows - 1)
            q, top, acc = query(nr, nh), None, None
            for c in range(chunks):
                top = score(nr, nh, c, q, top)
                acc = mix(r, h, c, peak, acc)
            outs.append(acc[:HEAD_DIM] / acc[HEAD_DIM : HEAD_DIM + 1])
        span = slice(heads[0] * HEAD_DIM, (heads[-1] + 1) * HEAD_DIM)
        o_ref[r, span, :] = jnp.concatenate(outs, axis=0)
        return top

    def body(i, top):
        for e in range(group):
            top = row(i * group + e, top)
        after(i)
        return top

    lax.fori_loop(0, rows // group, body, top)


class Gather:
    def __init__(self, place, ssem, rsem):
        self.place, self.ssem, self.rsem = place, ssem, rsem

    def copy(self, inst, kind, src, dst, to):
        return pltpu.make_async_remote_copy(
            src_ref=src,
            dst_ref=dst,
            send_sem=self.ssem.at[inst, kind],
            recv_sem=self.rsem.at[inst, kind],
            device_id=self.place(*to),
            device_id_type=MESH,
        )

    def setup(self, me, sizes):
        self.x, self.core, self.plane = me
        self.xs, self.planes = sizes
        self.other = 1 - self.core

    def at(self, step):
        return lax.rem(self.x + step, self.xs)

    def fan(self, inst, kind, slot):
        @pl.loop(1, self.planes)
        def _(u):
            p = lax.rem(self.plane + u, self.planes)
            self.copy(inst, kind, slot, slot, (self.x, self.core, p)).start()

    def fanned(self, inst, kind, buf):
        rest = buf.at[self.x, self.core, pl.ds(0, self.planes - 1)]
        return self.copy(inst, kind, rest, rest, (self.x, self.other, self.plane))

    def line(self, inst, kind, buf, step):
        part = buf.at[self.x, self.core]
        return self.copy(inst, kind, part, part, (self.at(step), self.core, self.plane))

    def hand(self, inst, kind, buf, step, core=None):
        part = buf.at[self.at(step), self.core if core is None else core]
        return self.copy(inst, kind, part, part, (self.x, self.other, self.plane))

    def far(self, inst, slot):
        half = self.xs // 2
        return self.copy(inst, 1, slot, slot, (self.at(half), self.core, self.plane))

    def first(self, inst, buf):
        slot = buf.at[self.x, self.core, self.plane]
        self.far(inst, slot).start()
        self.fan(inst, 0, slot)

    def halves(self, buf, planes):
        half = buf.shape[3] // 2
        return [buf.at[self.x, self.core, planes, pl.ds(e * half, half)] for e in range(2)]

    def piece(self, inst, kind, part):
        return self.copy(inst, kind, part, part, (self.x, self.other, self.plane))

    def first_upper(self, inst, buf):
        self.fan(inst, 0, self.halves(buf, self.plane)[0])
        self.far(inst, buf.at[self.x, self.core, self.plane]).start()

    def first_lower(self, inst, buf):
        self.fan(inst, 10, self.halves(buf, self.plane)[1])
        slot = buf.at[self.at(self.xs // 2), self.core, self.plane]
        self.far(inst, slot).wait_recv()
        self.fan(inst, 2, slot)

    def split_one(self, inst, buf):
        self.piece(inst, 0, self.halves(buf, pl.ds(0, self.planes - 1))[0]).wait_recv()
        upper = self.halves(buf, pl.ds(0, self.planes))[0]
        self.piece(inst, 9, upper).start()
        self.line_part(inst, 3, upper, 1).start()
        self.line_part(inst, 4, upper, self.xs - 1).start()

    def line_part(self, inst, kind, part, step):
        return self.copy(inst, kind, part, part, (self.at(step), self.core, self.plane))

    def split_two(self, inst, buf):
        self.piece(inst, 10, self.halves(buf, pl.ds(0, self.planes - 1))[1]).wait_recv()
        lower = self.halves(buf, pl.ds(0, self.planes))[1]
        self.piece(inst, 5, lower).start()
        self.line_part(inst, 11, lower, 1).start()
        self.line_part(inst, 12, lower, self.xs - 1).start()

    def handed_half(self, inst, kind, buf, e):
        half = buf.shape[3] // 2
        part = buf.at[self.x, self.other, :, pl.ds(e * half, half)]
        self.piece(inst, kind, part).wait_recv()

    def drain_split(self, inst, buf):
        self.far(inst, buf.at[self.x, self.core, self.plane]).wait_send()
        for e, (fan, hand) in enumerate(((0, 9), (10, 5))):
            self.piece(inst, fan, self.halves(buf, pl.ds(0, self.planes - 1))[e]).wait_send()
            self.piece(inst, hand, self.halves(buf, pl.ds(0, self.planes))[e]).wait_send()
        self.fanned(inst, 2, buf).wait_send()
        for e, part in enumerate(self.halves(buf, pl.ds(0, self.planes))):
            self.line_part(inst, 3 + 8 * e, part, 1).wait_send()
            self.line_part(inst, 4 + 8 * e, part, 1).wait_send()
        for kind in (6, 7, 8):
            self.hand(inst, kind, buf, 0).wait_send()

    def second(self, inst, buf, buf_far):
        slot = buf_far.at[self.at(self.xs // 2), self.core, self.plane]
        self.far(inst, slot).wait_recv()
        self.fan(inst, 2, slot)
        self.fanned(inst, 0, buf).wait_recv()
        self.hand(inst, 5, buf, 0).start()
        self.line(inst, 3, buf, 1).start()
        self.line(inst, 4, buf, self.xs - 1).start()

    def third_far(self, inst, buf_far):
        self.fanned(inst, 2, buf_far).wait_recv()
        self.hand(inst, 6, buf_far, self.xs // 2).start()

    def third_near(self, inst, buf_of):
        for step in (1 + self.other * (self.xs - 2), 1 + self.core * (self.xs - 2)):
            down = (step - 1) // (self.xs - 2)
            buf = buf_of(step)
            self.line(inst, 4 - down, buf, 1).wait_recv()
            self.hand(inst, 7 + down, buf, step).start()

    def third_near_split(self, inst, buf):
        for step in (1 + self.other * (self.xs - 2), 1 + self.core * (self.xs - 2)):
            down = (step - 1) // (self.xs - 2)
            for e, part in enumerate(self.halves(buf, pl.ds(0, self.planes))):
                self.line_part(inst, 4 + 8 * e - down, part, 1).wait_recv()
            self.hand(inst, 7 + down, buf, step).start()

    def handed(self, inst, kind, buf, step):
        self.hand(inst, kind, buf, step, self.other).wait_recv()

    def drain(self, inst, buf):
        slot = buf.at[self.x, self.core, self.plane]
        self.far(inst, slot).wait_send()
        self.fanned(inst, 0, buf).wait_send()
        self.fanned(inst, 2, buf).wait_send()
        self.line(inst, 3, buf, 1).wait_send()
        self.line(inst, 4, buf, 1).wait_send()
        for kind in (5, 6, 7, 8):
            self.hand(inst, kind, buf, 0).wait_send()


def kernel(
    nx,
    ny,
    ck,
    group,
    x_ref,
    mask_ref,
    g1_ref,
    w1_ref,
    gb1_ref,
    bw1_ref,
    ow1_ref,
    g2_ref,
    w2_ref,
    gb2_ref,
    bw2_ref,
    ow2_ref,
    g3_ref,
    ti_ref,
    tb_ref,
    to_ref,
    out_ref,
    q_ref,
    k_ref,
    v_ref,
    wt_ref,
    bias_ref,
    kb_ref,
    kc_ref,
    zs_ref,
    st_ref,
    rise_ref,
    first_ref,
    gc_ref,
    s_ref,
    o_ref,
    recv_m,
    recv_a,
    recv_b,
    send_z,
    recv_z,
    send_o,
    a_ref,
    ssem,
    rsem,
    zsem,
):
    n = nx * ny
    xs, planes = nx // 4, 2 * ny
    rows, res, ch = x_ref.shape
    tq = res // xs
    gx, gy = lax.axis_index("gx"), lax.axis_index("gy")
    me = gx * ny + gy
    core = lax.rem(gx, 2)
    x = lax.rem(gx // 2, xs)
    low = gx // (2 * xs)
    plane = low * ny + gy
    run = 2 * ny

    def place(x, core, plane):
        return (plane // ny * (2 * xs) + x * 2 + core, lax.rem(plane, ny))

    g = Gather(place, ssem, rsem)
    g.setup((x, core, plane), (xs, planes))
    barrier = pltpu.get_barrier_semaphore()

    def greet(*to):
        pl.semaphore_signal(barrier, inc=1, device_id=place(*to), device_id_type=MESH)

    for u in range(1, planes):
        greet(x, core, lax.rem(plane + u, planes))
    for u in range(1, xs):
        greet(g.at(u), core, plane)
    greet(x, 1 - core, plane)

    lane = lax.broadcasted_iota(jnp.int32, (16, 128), 1)
    vec = jnp.zeros((16, 128), F32)
    for t in range(rows):
        vec = jnp.where(lane == lax.rem(me * rows, 128) + t, mask_ref[t].astype(F32), vec)
    recv_m[x, core, plane] = vec.astype(BF16)


    def grouped(lo, hi, fn, size=2):
        def step(i, carry):
            fn([lo + i * size + e for e in range(size)])
            return carry

        lax.fori_loop(0, (hi - lo) // size, step, 0)

    def start_norm(batch):
        normed = [layer_norm(v.astype(F32), g1_ref[...]) for v in [x_ref[r] for r in batch]]
        for r, v in zip(batch, normed):
            a_ref[r] = v
        part = [bias_rows(bw1_ref[...], r, rows, v) for r, v in zip(batch, normed)]
        first_ref[...] = first_ref[...] + sum(part[1:], part[0])

    with jax.named_scope("norm"):
        first_ref[...] = jnp.zeros_like(first_ref)
        grouped(0, rows, start_norm)
        recv_a[x, core, plane] = first_ref[...].astype(BF16)

    with jax.named_scope("barrier"):
        pl.semaphore_wait(barrier, planes - 1 + xs - 1 + 1)
    g.first(0, recv_m)
    g.first_upper(1, recv_a)
    def turn_weights(w_ref, gb_ref):
        wt_ref[...] = w_ref[...].astype(F32).T.astype(BF16)
        column = jnp.broadcast_to(gb_ref[...], (128, ch)).T
        for b in range(tq // 128):
            gc_ref[:, b * 128 : (b + 1) * 128] = column

    def project(batch, w_ref):
        normed = [a_ref[r] for r in batch]
        for r, v in zip(batch, [nn(v, w_ref[:, ch : 2 * ch]) for v in normed]):
            k_ref[r] = v.astype(BF16)
        for r, v in zip(batch, [nt(wt_ref[:ch], v) for v in normed]):
            q = (v * QSCALE).astype(BF16)
            for b in range(2 * xs):
                to = (b % xs * 2 + b // xs) * 128
                q_ref[r, :, to : to + 128] = q[:, b * 128 : (b + 1) * 128]
        for r, v in zip(batch, [nt(wt_ref[2 * ch : 3 * ch], v) for v in normed]):
            v_ref[r] = v.astype(BF16)

    def both(t, size):
        return [pl.ds(pl.multiple_of((t + e * xs) * size, size), size) for e in range(2)]

    def mixed(batch, t, ow_ref):
        a = [jnp.concatenate([a_ref[r, span, :] for span in both(t, 128)], axis=0) for r in batch]
        gl = [nt(wt_ref[3 * ch :], v) for v in a]
        gated = [o_ref[r] * jax.nn.sigmoid(v + gc_ref[...]) for r, v in zip(batch, gl)]
        gated = [v.T.astype(BF16) for v in gated]
        return [nn(v, ow_ref[...]) for v in gated]

    def batches(fn):
        def run(i, carry):
            fn([i * 8 + e for e in range(8)])
            return carry

        lax.fori_loop(0, rows // 8, run, 0)

    turn_weights(w1_ref, gb1_ref)

    with jax.named_scope("project"):
        grouped(0, rows, lambda batch: project(batch, w1_ref))
    with jax.named_scope("mask2"):
        g.second(0, recv_m, recv_m)
    with jax.named_scope("lower"):
        g.first_lower(1, recv_a)
    with jax.named_scope("mask3"):
        g.third_far(0, recv_m)
        g.third_near(0, lambda step: recv_m)
    with jax.named_scope("a2"):
        g.split_one(1, recv_a)
    with jax.named_scope("mask4"):
        g.handed(0, 5, recv_m, 0)
        g.handed(0, 6, recv_m, xs // 2)
        g.handed(0, 7, recv_m, 1)
        g.handed(0, 8, recv_m, xs - 1)

    for b in range(2 * xs):
        part = recv_m[b % xs, :, b // xs * ny : (b // xs + 1) * ny].astype(F32)
        mask = jnp.sum(jnp.sum(part, axis=0), axis=0)[:1]
        kb = (mask - 1.0) * BIG
        kb_ref[:, b * 128 : (b + 1) * 128] = kb
        kc_ref[b * 128 : (b + 1) * 128, :] = jnp.broadcast_to(kb, (128, 128)).T

    def start_bias(t, heads):
        for e in range(2):
            lo, hi = heads[0] * rows, (heads[-1] + 1) * rows
            blocks = [
                recv_a[t, c, e * ny : (e + 1) * ny, lo:hi].astype(F32) for c in range(2)
            ]
            for h in heads:
                part = jnp.concatenate(
                    [
                        b[:, h * rows - lo : (h + 1) * rows - lo, :].reshape(64, res)
                        for b in blocks
                    ], axis=0
                )
                to = slice(e * 128, (e + 1) * 128)
                bias_ref[t, h, :, to] = ((part + kb_ref[...]) * LOG2E).T

    def stage(r, z):
        st_ref[:, pl.ds(pl.multiple_of(r * rows, rows), rows), :] = z.reshape(
            tq // rows, rows, ch
        )

    def stage_turned(r, z):
        st_ref[:, pl.ds(r, rows, stride=rows), :] = z.reshape(tq // rows, rows, ch)

    mine = out_ref.at[:, pl.ds(pl.multiple_of(me * rows, rows), rows), :]

    def load(src, t):
        for e, span in enumerate(both(t, run)):
            src[span] = st_ref[e * run : (e + 1) * run].astype(BF16).reshape(run, *src.shape[1:])

    def spread(kind, src, dst, t):
        def send(v):
            c, p = lax.rem(v, 2), v // 2
            to = place(t, c, p)
            d = to[0] * ny + to[1]
            return pltpu.make_async_remote_copy(
                src_ref=src.at[d],
                dst_ref=dst,
                send_sem=zsem.at[kind, 0],
                recv_sem=zsem.at[kind, 1],
                device_id=to,
                device_id_type=MESH,
            )

        here = plane * 2 + core

        @pl.when(t != x)
        def _():
            send(here).start()

        @pl.loop(1, 2 * run)
        def _(u):
            send(lax.rem(here + u, 2 * run)).start()

    def settle(kind, part, sent):
        copy = pltpu.make_async_remote_copy(
            src_ref=part,
            dst_ref=part,
            send_sem=zsem.at[kind, 0],
            recv_sem=zsem.at[kind, 1],
            device_id=place(x, 1 - core, plane),
            device_id_type=MESH,
        )
        copy.wait_send() if sent else copy.wait_recv()

    def step_blocks(buf, s):
        return buf.at[pl.ds(0, 2 * run - (1 if s == 0 else 0))]

    near = 1 + core * (xs - 2)

    def tile_of(s, step=0, swap=False):
        side = xs - near if swap else near
        away = jnp.where(s == 0, 0, jnp.where(s == 1, xs // 2, jnp.where(s == 2, side, xs - side)))
        return lax.rem(x + step + away, xs)

    def rise_second(s):
        t = tile_of(s)
        g.second(2 + s, recv_b.at[t], recv_b.at[tile_of(s, xs // 2)])

    def rise_third(s):
        g.third_far(2 + s, recv_b.at[tile_of(s, xs // 2)])
        g.third_near(2 + s, lambda step: recv_b.at[tile_of(s, step)])

    def start_tile(s, carry, alone=False):
        t = tile_of(s)

        @pl.when(s == 1)
        def _():
            with jax.named_scope("wait1"):
                g.handed(1, 6, recv_a, xs // 2)

        @pl.when(s == 2)
        def _():
            with jax.named_scope("wait2"):
                g.handed(1, 7 + core, recv_a, near)

        @pl.when(s == 3)
        def _():
            with jax.named_scope("wait3"):
                g.handed(1, 8 - core, recv_a, xs - near)

        def attend(heads, after):
            with jax.named_scope("biasa"):
                start_bias(t, heads)
            with jax.named_scope("att1"):
                attend_tile(
                    ck, group, t, q_ref, k_ref, v_ref, bias_ref, s_ref, o_ref, after, heads
                )

        def start_finish(batch):
            out = mixed(batch, t, ow1_ref)
            old = [jnp.concatenate([x_ref[r, p, :] for p in both(t, 128)], axis=0) for r in batch]
            z1 = [(u.astype(F32) + v).astype(BF16).astype(F32) for u, v in zip(old, out)]
            for r, v in zip(batch, z1):
                stage(r, v)
            normed = [layer_norm(v, g2_ref[...]) for v in z1]
            part = [bias_rows(bw2_ref[...], r, rows, v) for r, v in zip(batch, normed)]
            rise_ref[...] = rise_ref[...] + sum(part[1:], part[0])

        def start_after(i):
            @pl.when((s == 1) & (i == rows // group - 1))
            def _():
                with jax.named_scope("near1"):
                    g.third_near_split(1, recv_a)

            @pl.when((s > 0) & (i == 0))
            def _():
                with jax.named_scope("rise2"):
                    rise_second(s - 1)

            @pl.when((s > 1) & (i == rows // group - 1))
            def _():
                with jax.named_scope("rise3"):
                    rise_third(s - 2)

        if alone:
            nothing = lambda i: None
            with jax.named_scope("wait0"):
                g.handed_half(1, 9, recv_a, 0)
            attend((0, 1), nothing)
            with jax.named_scope("a3"):
                g.split_two(1, recv_a)
                g.handed_half(1, 5, recv_a, 1)
            attend((2, 3), nothing)
        else:
            attend((0, 1, 2, 3), start_after)
        with jax.named_scope("tail1"):
            rise_ref[...] = jnp.zeros_like(rise_ref)
            batches(start_finish)
        recv_b[t, x, core, plane] = rise_ref[...].astype(BF16)
        with jax.named_scope("ship1"):
            g.first(2 + s, recv_b.at[t])

        if alone:
            with jax.named_scope("far1"):
                g.third_far(1, recv_a)

        with jax.named_scope("ship1"):
            load(send_z, t)
            spread(s, send_z, recv_z.at[me], t)

        return carry

    start_tile(0, 0, True)
    lax.fori_loop(1, xs, start_tile, 0)
    turn_weights(w2_ref, gb2_ref)
    recv_z[me] = send_z[me]

    def end_prepare(px):
        for span in both(px, run):
            zs_ref[span] = recv_z[span].astype(F32)
        places = both(px, 128)
        lanes = pl.ds(pl.multiple_of(px * tq, tq), tq)

        def columns(batch):
            z1 = [
                jnp.concatenate(
                    [
                        zs_ref[span, pl.ds(d, rows, stride=rows), :].reshape(128, ch)
                        for span in both(px, run)
                    ],
                    axis=0,
                )
                for d in batch
            ]
            normed = [layer_norm(v, g2_ref[...]) for v in z1]
            keys = [nn(v, w2_ref[:, ch : 2 * ch]).astype(BF16) for v in normed]
            queries = [(nt(wt_ref[:ch], v) * QSCALE).astype(BF16) for v in normed]
            values = [nt(wt_ref[2 * ch : 3 * ch], v).astype(BF16) for v in normed]
            for d, u, k, q, v in zip(batch, normed, keys, queries, values):
                q_ref[d, :, lanes] = q
                for e, span in enumerate(places):
                    part = slice(e * 128, (e + 1) * 128)
                    a_ref[d, span, :] = u[part]
                    k_ref[d, span, :] = k[part]
                    v_ref[d, :, span] = v[:, part]

        grouped(0, rows, columns, 4)

    with jax.named_scope("early"):
        for s in range(2):
            settle(s, step_blocks(recv_z, s), False)
        end_prepare(x)
        end_prepare(g.at(xs // 2))
    with jax.named_scope("rise2e"):
        rise_second(xs - 1)
    with jax.named_scope("rise3d"):
        rise_third(xs - 2)
    with jax.named_scope("waitz"):
        for s in range(2, xs):
            settle(s, step_blocks(recv_z, s), False)
    with jax.named_scope("late1"):
        end_prepare(g.at(1))
    with jax.named_scope("rise3e"):
        rise_third(xs - 1)
    with jax.named_scope("late2"):
        end_prepare(g.at(xs - 1))

    def rise_done(s, carry):
        g.handed(2 + s, 5, recv_b.at[tile_of(s, 0, True)], 0)
        g.handed(2 + s, 6, recv_b.at[tile_of(s, xs // 2, True)], xs // 2)
        g.handed(2 + s, 7, recv_b.at[tile_of(s, 1, True)], 1)
        g.handed(2 + s, 8, recv_b.at[tile_of(s, xs - 1, True)], xs - 1)
        return carry

    with jax.named_scope("handed"):
        lax.fori_loop(0, xs, rise_done, 0)

    def end_bias(t):
        def keys_of(b, carry):
            e, c = lax.rem(b // 2, 2), lax.rem(b, 2)
            keys = pl.ds(pl.multiple_of((e * 2 * xs + b // 4 * 2 + c) * 64, 64), 64)
            kc = kc_ref[keys, :]
            block = recv_b[t, b // 4, c, pl.ds(e * ny, ny)].astype(F32)
            for h in range(HEADS):
                part = block[:, h * rows : (h + 1) * rows, :].reshape(64, tq)
                for w in range(tq // 128):
                    to = slice(w * 128, (w + 1) * 128)
                    bias_ref[t, h, keys, to] = (part[:, to] + kc) * LOG2E
            return carry

        lax.fori_loop(0, 4 * xs, keys_of, 0)

    def end_tile(s, carry):
        t = tile_of(lax.rem(s + 1, xs))
        with jax.named_scope("biasb"):
            end_bias(t)

        def end_finish(batch):
            out = mixed(batch, t, ow2_ref)
            z1 = [
                jnp.concatenate(
                    [
                        zs_ref[span, pl.ds(r, rows, stride=rows), :].reshape(128, ch)
                        for span in both(t, run)
                    ],
                    axis=0,
                )
                for r in batch
            ]
            z2 = [(u + v).astype(BF16).astype(F32) for u, v in zip(z1, out)]
            normed = [layer_norm(v, g3_ref[...]) for v in z2]
            hid = [nn(v, ti_ref[...]) + tb_ref[...] for v in normed]
            hid = [jnp.maximum(v, 0.0).astype(BF16) for v in hid]
            last = [nn(v, to_ref[...]) for v in hid]
            for r, u, v in zip(batch, z2, last):
                stage_turned(r, u + v)

        with jax.named_scope("att2"):
            attend_tile(
                ck, group, t, q_ref, k_ref, v_ref, bias_ref, s_ref, o_ref,
                lambda r: None, (0, 1, 2, 3),
            )
        with jax.named_scope("tail2"):
            batches(end_finish)
        with jax.named_scope("ship2"):
            load(send_o, t)
            spread(xs, send_o, mine, t)
        return carry

    lax.fori_loop(0, xs, end_tile, 0)
    with jax.named_scope("drain"):
        g.drain(0, recv_m)
        g.drain_split(1, recv_a)

        def drain_rise(s, carry):
            g.drain(2 + s, recv_b.at[tile_of(s)])
            return carry

        lax.fori_loop(0, xs, drain_rise, 0)
    with jax.named_scope("waito"):
        own = pltpu.make_async_copy(send_o.at[me], mine, zsem.at[xs + 1, 0])
        own.start()
        for s in range(xs):
            settle(s, step_blocks(send_z, s), True)
        settle(xs, send_o.at[pl.ds(0, n - 1)], True)
        settle(xs, out_ref.at[:, pl.ds(0, res - rows), :], False)
        own.wait()


def solution(mesh):
    nx, ny = mesh.shape["gx"], mesh.shape["gy"]
    n, xs = nx * ny, nx // 4

    def local(x, mask, g1, w1, gb1, bw1, ow1, g2, w2, gb2, bw2, ow2, g3, ti, tb, to):
        rows, res, ch = x.shape
        tq, ck = res // xs, 512
        vmem = pl.BlockSpec(memory_space=pltpu.VMEM)
        row = lambda t: t.reshape(1, -1)
        return pl.pallas_call(
            functools.partial(kernel, nx, ny, ck, min(rows, 4)),
            out_shape=jax.ShapeDtypeStruct(x.shape, x.dtype),
            in_specs=[vmem, pl.BlockSpec(memory_space=pltpu.SMEM)] + [vmem] * 14,
            out_specs=pl.BlockSpec(memory_space=pl.ANY),
            scratch_shapes=[
                pltpu.VMEM((rows, ch, res), BF16),
                pltpu.VMEM((rows, res, ch), BF16),
                pltpu.VMEM((rows, ch, res), BF16),
                pltpu.VMEM((4 * ch, ch), BF16),
                pltpu.VMEM((xs, HEADS, res, tq), F32),
                pltpu.VMEM((1, res), F32),
                pltpu.VMEM((res, 128), F32),
                pltpu.VMEM((n, rows * rows, ch), F32),
                pltpu.VMEM((tq // rows, rows * rows, ch), F32),
                pltpu.VMEM((HEADS * rows, tq), F32),
                pltpu.VMEM((HEADS * rows, res), F32),
                pltpu.VMEM((ch, tq), F32),
                pltpu.VMEM((2 * res, tq), F32),
                pltpu.VMEM((rows, ch, tq), F32),
                pltpu.VMEM((xs, 2, 2 * ny, 16, 128), BF16),
                pltpu.VMEM((xs, 2, 2 * ny, HEADS * rows, res), BF16),
                pltpu.VMEM((xs, xs, 2, 2 * ny, HEADS * rows, tq), BF16),
                pltpu.VMEM((n, rows * rows, ch), BF16),
                pltpu.VMEM((n, rows * rows, ch), BF16),
                pltpu.VMEM((n, rows, rows, ch), BF16),
                pltpu.VMEM((rows, res, ch), BF16),
                pltpu.SemaphoreType.DMA((2 + xs, 13)),
                pltpu.SemaphoreType.DMA((2 + xs, 13)),
                pltpu.SemaphoreType.DMA((2 + xs, 2)),
            ],
            compiler_params=pltpu.CompilerParams(
                collective_id=0, has_side_effects=True, vmem_limit_bytes=67_043_328,
            ),
        )(
            x, mask, row(g1), w1, row(gb1), bw1.T, ow1, row(g2), w2,
            row(gb2), bw2.T, ow2, row(g3), ti, row(tb), to,
        )

    placed = (P(("gx", "gy"), None, None), P(("gx", "gy"))) + (P(),) * 14
    return jax.shard_map(
        local, mesh=mesh, in_specs=placed, out_specs=P(("gx", "gy"), None, None), check_vma=False
    )
```

```python
import functools
import math

import jax
import jax.numpy as jnp
from jax import lax
from jax.experimental import pallas as pl
from jax.experimental.pallas import tpu as pltpu
from jax.sharding import PartitionSpec as P

HEADS = 4
HEAD_DIM = 32
BIG = 1000000000.0
LOG2E = math.log2(math.e)
QSCALE = HEAD_DIM ** (-0.5) * LOG2E
MESH = pl.DeviceIdType.MESH
F32 = jnp.float32
BF16 = jnp.bfloat16


def nn(a, b):
    return lax.dot_general(a, b, (((1,), (0,)), ((), ())), preferred_element_type=F32)


def nt(a, b):
    return lax.dot_general(a, b, (((1,), (1,)), ((), ())), preferred_element_type=F32)


def layer_norm(x, gain):
    mean = jnp.mean(x, axis=-1, keepdims=True)
    cent = x - mean
    var = jnp.mean(cent * cent, axis=-1, keepdims=True)
    return (cent * lax.rsqrt(var + 1e-05) * gain).astype(BF16)


def bias_rows(w, r, rows, normed):
    shape = (HEADS * rows, HEADS)
    place = lax.broadcasted_iota(jnp.int32, shape, 0) == (
        lax.broadcasted_iota(jnp.int32, shape, 1) * rows + r
    )
    spread = nn(place.astype(F32).astype(BF16), w).astype(BF16)
    return nt(spread, normed)


def attend_tile(ck, group, t, q_ref, k_ref, v_ref, bias_ref, s_ref, o_ref, after, heads):
    rows, res, ch = k_ref.shape
    pairs = len(heads)
    tq = s_ref.shape[1]
    s_refs = [s_ref.at[:res], s_ref.at[res:]]
    lanes = pl.ds(pl.multiple_of(t * tq, tq), tq)
    chunks = res // ck

    def query(r, h):
        q = q_ref[r, :, lanes]
        row = lax.broadcasted_iota(jnp.int32, q.shape, 0)
        return jnp.where((row >= h * HEAD_DIM) & (row < (h + 1) * HEAD_DIM), q, jnp.zeros_like(q))

    def score(r, h, c, q, top):
        span = slice(c * ck, (c + 1) * ck)
        s = nn(k_ref[r, span, :], q) + bias_ref[t, h, span, :]
        s_refs[h % 2][span, :] = s
        m = jnp.max(s.reshape(ck // 8, 8, tq), axis=0)
        return m if top is None else jnp.maximum(top, m)

    def mix(r, h, c, top, acc):
        span = slice(c * ck, (c + 1) * ck)
        w = jnp.exp2((s_refs[h % 2][span, :] - top).astype(BF16))
        v = jnp.concatenate(
            [v_ref[r, h * HEAD_DIM : (h + 1) * HEAD_DIM, span], jnp.ones((16, ck), BF16)], axis=0
        )
        o = nn(v, w)
        return o if acc is None else acc + o

    q, top = query(0, heads[0]), None
    for c in range(chunks):
        top = score(0, heads[0], c, q, top)

    def row(r, top):
        outs = []
        for at, h in enumerate(heads):
            peak = jnp.max(top, axis=0, keepdims=True)
            nh = heads[(at + 1) % pairs]
            nr = r if at < pairs - 1 else jnp.minimum(r + 1, rows - 1)
            q, top, acc = query(nr, nh), None, None
            for c in range(chunks):
                top = score(nr, nh, c, q, top)
                acc = mix(r, h, c, peak, acc)
            outs.append(acc[:HEAD_DIM] / acc[HEAD_DIM : HEAD_DIM + 1])
        span = slice(heads[0] * HEAD_DIM, (heads[-1] + 1) * HEAD_DIM)
        o_ref[r, span, :] = jnp.concatenate(outs, axis=0)
        return top

    def body(i, top):
        for e in range(group):
            top = row(i * group + e, top)
        after(i)
        return top

    lax.fori_loop(0, rows // group, body, top)


class Gather:
    def __init__(self, place, ssem, rsem):
        self.place, self.ssem, self.rsem = place, ssem, rsem

    def copy(self, inst, kind, src, dst, to):
        return pltpu.make_async_remote_copy(
            src_ref=src,
            dst_ref=dst,
            send_sem=self.ssem.at[inst, kind],
            recv_sem=self.rsem.at[inst, kind],
            device_id=self.place(*to),
            device_id_type=MESH,
        )

    def setup(self, me, sizes):
        self.x, self.core, self.plane = me
        self.xs, self.planes = sizes
        self.other = 1 - self.core

    def at(self, step):
        return lax.rem(self.x + step, self.xs)

    def fan(self, inst, kind, slot):
        @pl.loop(1, self.planes)
        def _(u):
            p = lax.rem(self.plane + u, self.planes)
            self.copy(inst, kind, slot, slot, (self.x, self.core, p)).start()

    def fanned(self, inst, kind, buf):
        rest = buf.at[self.x, self.core, pl.ds(0, self.planes - 1)]
        return self.copy(inst, kind, rest, rest, (self.x, self.other, self.plane))

    def line(self, inst, kind, buf, step):
        part = buf.at[self.x, self.core]
        return self.copy(inst, kind, part, part, (self.at(step), self.core, self.plane))

    def hand(self, inst, kind, buf, step, core=None):
        part = buf.at[self.at(step), self.core if core is None else core]
        return self.copy(inst, kind, part, part, (self.x, self.other, self.plane))

    def far(self, inst, slot):
        half = self.xs // 2
        return self.copy(inst, 1, slot, slot, (self.at(half), self.core, self.plane))

    def first(self, inst, buf):
        slot = buf.at[self.x, self.core, self.plane]
        self.far(inst, slot).start()
        self.fan(inst, 0, slot)

    def halves(self, buf, planes):
        half = buf.shape[3] // 2
        return [buf.at[self.x, self.core, planes, pl.ds(e * half, half)] for e in range(2)]

    def piece(self, inst, kind, part):
        return self.copy(inst, kind, part, part, (self.x, self.other, self.plane))

    def first_upper(self, inst, buf):
        self.fan(inst, 0, self.halves(buf, self.plane)[0])
        self.far(inst, buf.at[self.x, self.core, self.plane]).start()

    def first_lower(self, inst, buf):
        self.fan(inst, 10, self.halves(buf, self.plane)[1])
        slot = buf.at[self.at(self.xs // 2), self.core, self.plane]
        self.far(inst, slot).wait_recv()
        self.fan(inst, 2, slot)

    def split_one(self, inst, buf):
        self.piece(inst, 0, self.halves(buf, pl.ds(0, self.planes - 1))[0]).wait_recv()
        upper = self.halves(buf, pl.ds(0, self.planes))[0]
        self.piece(inst, 9, upper).start()
        self.line_part(inst, 3, upper, 1).start()
        self.line_part(inst, 4, upper, self.xs - 1).start()

    def line_part(self, inst, kind, part, step):
        return self.copy(inst, kind, part, part, (self.at(step), self.core, self.plane))

    def split_two(self, inst, buf):
        self.piece(inst, 10, self.halves(buf, pl.ds(0, self.planes - 1))[1]).wait_recv()
        lower = self.halves(buf, pl.ds(0, self.planes))[1]
        self.piece(inst, 5, lower).start()
        self.line_part(inst, 11, lower, 1).start()
        self.line_part(inst, 12, lower, self.xs - 1).start()

    def handed_half(self, inst, kind, buf, e):
        half = buf.shape[3] // 2
        part = buf.at[self.x, self.other, :, pl.ds(e * half, half)]
        self.piece(inst, kind, part).wait_recv()

    def drain_split(self, inst, buf):
        self.far(inst, buf.at[self.x, self.core, self.plane]).wait_send()
        for e, (fan, hand) in enumerate(((0, 9), (10, 5))):
            self.piece(inst, fan, self.halves(buf, pl.ds(0, self.planes - 1))[e]).wait_send()
            self.piece(inst, hand, self.halves(buf, pl.ds(0, self.planes))[e]).wait_send()
        self.fanned(inst, 2, buf).wait_send()
        for e, part in enumerate(self.halves(buf, pl.ds(0, self.planes))):
            self.line_part(inst, 3 + 8 * e, part, 1).wait_send()
            self.line_part(inst, 4 + 8 * e, part, 1).wait_send()
        for kind in (6, 7, 8):
            self.hand(inst, kind, buf, 0).wait_send()

    def second(self, inst, buf, buf_far):
        slot = buf_far.at[self.at(self.xs // 2), self.core, self.plane]
        self.far(inst, slot).wait_recv()
        self.fan(inst, 2, slot)
        self.fanned(inst, 0, buf).wait_recv()
        self.hand(inst, 5, buf, 0).start()
        self.line(inst, 3, buf, 1).start()
        self.line(inst, 4, buf, self.xs - 1).start()

    def third_far(self, inst, buf_far):
        self.fanned(inst, 2, buf_far).wait_recv()
        self.hand(inst, 6, buf_far, self.xs // 2).start()

    def third_near(self, inst, buf_of):
        for step in (1 + self.other * (self.xs - 2), 1 + self.core * (self.xs - 2)):
            down = (step - 1) // (self.xs - 2)
            buf = buf_of(step)
            self.line(inst, 4 - down, buf, 1).wait_recv()
            self.hand(inst, 7 + down, buf, step).start()

    def third_near_split(self, inst, buf):
        for step in (1 + self.other * (self.xs - 2), 1 + self.core * (self.xs - 2)):
            down = (step - 1) // (self.xs - 2)
            for e, part in enumerate(self.halves(buf, pl.ds(0, self.planes))):
                self.line_part(inst, 4 + 8 * e - down, part, 1).wait_recv()
            self.hand(inst, 7 + down, buf, step).start()

    def handed(self, inst, kind, buf, step):
        self.hand(inst, kind, buf, step, self.other).wait_recv()

    def drain(self, inst, buf):
        slot = buf.at[self.x, self.core, self.plane]
        self.far(inst, slot).wait_send()
        self.fanned(inst, 0, buf).wait_send()
        self.fanned(inst, 2, buf).wait_send()
        self.line(inst, 3, buf, 1).wait_send()
        self.line(inst, 4, buf, 1).wait_send()
        for kind in (5, 6, 7, 8):
            self.hand(inst, kind, buf, 0).wait_send()


def kernel(
    nx,
    ny,
    ck,
    group,
    x_ref,
    mask_ref,
    g1_ref,
    w1_ref,
    gb1_ref,
    bw1_ref,
    ow1_ref,
    g2_ref,
    w2_ref,
    gb2_ref,
    bw2_ref,
    ow2_ref,
    g3_ref,
    ti_ref,
    tb_ref,
    to_ref,
    out_ref,
    q_ref,
    k_ref,
    v_ref,
    wt_ref,
    bias_ref,
    kb_ref,
    kc_ref,
    zs_ref,
    st_ref,
    rise_ref,
    first_ref,
    gc_ref,
    s_ref,
    o_ref,
    recv_m,
    recv_a,
    recv_b,
    send_z,
    recv_z,
    send_o,
    a_ref,
    ssem,
    rsem,
    zsem,
):
    n = nx * ny
    xs, planes = nx // 4, 2 * ny
    rows, res, ch = x_ref.shape
    tq = res // xs
    gx, gy = lax.axis_index("gx"), lax.axis_index("gy")
    me = gx * ny + gy
    core = lax.rem(gx, 2)
    x = lax.rem(gx // 2, xs)
    low = gx // (2 * xs)
    plane = low * ny + gy
    run = 2 * ny

    def place(x, core, plane):
        return (plane // ny * (2 * xs) + x * 2 + core, lax.rem(plane, ny))

    g = Gather(place, ssem, rsem)
    g.setup((x, core, plane), (xs, planes))
    barrier = pltpu.get_barrier_semaphore()

    def greet(*to):
        pl.semaphore_signal(barrier, inc=1, device_id=place(*to), device_id_type=MESH)

    for u in range(1, planes):
        greet(x, core, lax.rem(plane + u, planes))
    for u in range(1, xs):
        greet(g.at(u), core, plane)
    greet(x, 1 - core, plane)

    lane = lax.broadcasted_iota(jnp.int32, (16, 128), 1)
    vec = jnp.zeros((16, 128), F32)
    for t in range(rows):
        vec = jnp.where(lane == lax.rem(me * rows, 128) + t, mask_ref[t].astype(F32), vec)
    recv_m[x, core, plane] = vec.astype(BF16)


    def grouped(lo, hi, fn, size=2):
        def step(i, carry):
            fn([lo + i * size + e for e in range(size)])
            return carry

        lax.fori_loop(0, (hi - lo) // size, step, 0)

    def start_norm(batch):
        normed = [layer_norm(v.astype(F32), g1_ref[...]) for v in [x_ref[r] for r in batch]]
        for r, v in zip(batch, normed):
            a_ref[r] = v
        part = [bias_rows(bw1_ref[...], r, rows, v) for r, v in zip(batch, normed)]
        first_ref[...] = first_ref[...] + sum(part[1:], part[0])

    with jax.named_scope("norm"):
        first_ref[...] = jnp.zeros_like(first_ref)
        grouped(0, rows, start_norm)
        recv_a[x, core, plane] = first_ref[...].astype(BF16)

    with jax.named_scope("barrier"):
        pl.semaphore_wait(barrier, planes - 1 + xs - 1 + 1)
    g.first(0, recv_m)
    g.first_upper(1, recv_a)
    def turn_weights(w_ref, gb_ref):
        wt_ref[...] = w_ref[...].astype(F32).T.astype(BF16)
        column = jnp.broadcast_to(gb_ref[...], (128, ch)).T
        for b in range(tq // 128):
            gc_ref[:, b * 128 : (b + 1) * 128] = column

    def project(batch, w_ref):
        normed = [a_ref[r] for r in batch]
        for r, v in zip(batch, [nn(v, w_ref[:, ch : 2 * ch]) for v in normed]):
            k_ref[r] = v.astype(BF16)
        for r, v in zip(batch, [nt(wt_ref[:ch], v) for v in normed]):
            q = (v * QSCALE).astype(BF16)
            for b in range(2 * xs):
                to = (b % xs * 2 + b // xs) * 128
                q_ref[r, :, to : to + 128] = q[:, b * 128 : (b + 1) * 128]
        for r, v in zip(batch, [nt(wt_ref[2 * ch : 3 * ch], v) for v in normed]):
            v_ref[r] = v.astype(BF16)

    def both(t, size):
        return [pl.ds(pl.multiple_of((t + e * xs) * size, size), size) for e in range(2)]

    def mixed(batch, t, ow_ref):
        a = [jnp.concatenate([a_ref[r, span, :] for span in both(t, 128)], axis=0) for r in batch]
        gl = [nt(wt_ref[3 * ch :], v) for v in a]
        gated = [o_ref[r] * jax.nn.sigmoid(v + gc_ref[...]) for r, v in zip(batch, gl)]
        gated = [v.T.astype(BF16) for v in gated]
        return [nn(v, ow_ref[...]) for v in gated]

    def batches(fn):
        def run(i, carry):
            fn([i * 8 + e for e in range(8)])
            return carry

        lax.fori_loop(0, rows // 8, run, 0)

    turn_weights(w1_ref, gb1_ref)

    with jax.named_scope("project"):
        grouped(0, rows, lambda batch: project(batch, w1_ref))
    with jax.named_scope("mask2"):
        g.second(0, recv_m, recv_m)
    with jax.named_scope("lower"):
        g.first_lower(1, recv_a)
    with jax.named_scope("mask3"):
        g.third_far(0, recv_m)
        g.third_near(0, lambda step: recv_m)
    with jax.named_scope("a2"):
        g.split_one(1, recv_a)
    with jax.named_scope("mask4"):
        g.handed(0, 5, recv_m, 0)
        g.handed(0, 6, recv_m, xs // 2)
        g.handed(0, 7, recv_m, 1)
        g.handed(0, 8, recv_m, xs - 1)

    for b in range(2 * xs):
        part = recv_m[b % xs, :, b // xs * ny : (b // xs + 1) * ny].astype(F32)
        mask = jnp.sum(jnp.sum(part, axis=0), axis=0)[:1]
        kb = (mask - 1.0) * BIG
        kb_ref[:, b * 128 : (b + 1) * 128] = kb
        kc_ref[b * 128 : (b + 1) * 128, :] = jnp.broadcast_to(kb, (128, 128)).T

    def start_bias(t, heads):
        for e in range(2):
            lo, hi = heads[0] * rows, (heads[-1] + 1) * rows
            blocks = [
                recv_a[t, c, e * ny : (e + 1) * ny, lo:hi].astype(F32) for c in range(2)
            ]
            for h in heads:
                part = jnp.concatenate(
                    [
                        b[:, h * rows - lo : (h + 1) * rows - lo, :].reshape(64, res)
                        for b in blocks
                    ], axis=0
                )
                to = slice(e * 128, (e + 1) * 128)
                bias_ref[t, h, :, to] = ((part + kb_ref[...]) * LOG2E).T

    def stage(r, z):
        st_ref[:, pl.ds(pl.multiple_of(r * rows, rows), rows), :] = z.reshape(
            tq // rows, rows, ch
        )

    def stage_turned(r, z):
        st_ref[:, pl.ds(r, rows, stride=rows), :] = z.reshape(tq // rows, rows, ch)

    mine = out_ref.at[:, pl.ds(pl.multiple_of(me * rows, rows), rows), :]

    def load(src, t):
        for e, span in enumerate(both(t, run)):
            src[span] = st_ref[e * run : (e + 1) * run].astype(BF16).reshape(run, *src.shape[1:])

    def spread(kind, src, dst, t):
        def send(v):
            c, p = lax.rem(v, 2), v // 2
            to = place(t, c, p)
            d = to[0] * ny + to[1]
            return pltpu.make_async_remote_copy(
                src_ref=src.at[d],
                dst_ref=dst,
                send_sem=zsem.at[kind, 0],
                recv_sem=zsem.at[kind, 1],
                device_id=to,
                device_id_type=MESH,
            )

        here = plane * 2 + core

        own = jnp.where(t == x, 1, 0)

        def some(i, carry):
            for e in range(8):
                send(lax.rem(here + own + i * 8 + e, 2 * run)).start()
            return carry

        @pl.when(t != x)
        def _():
            lax.fori_loop(0, 2 * run // 8, some, 0)

        @pl.when(t == x)
        def _():
            lax.fori_loop(0, 2 * run // 8 - 1, some, 0)
            for u in range(2 * run - 8, 2 * run - 1):
                send(lax.rem(here + 1 + u, 2 * run)).start()

    def settle(kind, part, sent):
        copy = pltpu.make_async_remote_copy(
            src_ref=part,
            dst_ref=part,
            send_sem=zsem.at[kind, 0],
            recv_sem=zsem.at[kind, 1],
            device_id=place(x, 1 - core, plane),
            device_id_type=MESH,
        )
        copy.wait_send() if sent else copy.wait_recv()

    def step_blocks(buf, s):
        return buf.at[pl.ds(0, 2 * run - (1 if s == 0 else 0))]

    near = 1 + core * (xs - 2)

    def tile_of(s, step=0, swap=False):
        side = xs - near if swap else near
        away = jnp.where(s == 0, 0, jnp.where(s == 1, xs // 2, jnp.where(s == 2, side, xs - side)))
        return lax.rem(x + step + away, xs)

    def rise_second(s):
        t = tile_of(s)
        g.second(2 + s, recv_b.at[t], recv_b.at[tile_of(s, xs // 2)])

    def rise_third(s):
        g.third_far(2 + s, recv_b.at[tile_of(s, xs // 2)])
        g.third_near(2 + s, lambda step: recv_b.at[tile_of(s, step)])

    def start_tile(s, carry, alone=False):
        t = tile_of(s)

        @pl.when(s == 1)
        def _():
            with jax.named_scope("wait1"):
                g.handed(1, 6, recv_a, xs // 2)

        @pl.when(s == 2)
        def _():
            with jax.named_scope("wait2"):
                g.handed(1, 7 + core, recv_a, near)

        @pl.when(s == 3)
        def _():
            with jax.named_scope("wait3"):
                g.handed(1, 8 - core, recv_a, xs - near)

        def attend(heads, after):
            with jax.named_scope("biasa"):
                start_bias(t, heads)
            with jax.named_scope("att1"):
                attend_tile(
                    ck, group, t, q_ref, k_ref, v_ref, bias_ref, s_ref, o_ref, after, heads
                )

        def start_finish(batch):
            out = mixed(batch, t, ow1_ref)
            old = [jnp.concatenate([x_ref[r, p, :] for p in both(t, 128)], axis=0) for r in batch]
            z1 = [(u.astype(F32) + v).astype(BF16).astype(F32) for u, v in zip(old, out)]
            for r, v in zip(batch, z1):
                stage(r, v)
            normed = [layer_norm(v, g2_ref[...]) for v in z1]
            part = [bias_rows(bw2_ref[...], r, rows, v) for r, v in zip(batch, normed)]
            rise_ref[...] = rise_ref[...] + sum(part[1:], part[0])

        def start_after(i):
            @pl.when((s == 1) & (i == rows // group - 1))
            def _():
                with jax.named_scope("near1"):
                    g.third_near_split(1, recv_a)

            @pl.when((s > 0) & (i == 0))
            def _():
                with jax.named_scope("rise2"):
                    rise_second(s - 1)

            @pl.when((s > 1) & (i == rows // group - 1))
            def _():
                with jax.named_scope("rise3"):
                    rise_third(s - 2)

        if alone:
            nothing = lambda i: None
            with jax.named_scope("wait0"):
                g.handed_half(1, 9, recv_a, 0)
            attend((0, 1), nothing)
            with jax.named_scope("a3"):
                g.split_two(1, recv_a)
                g.handed_half(1, 5, recv_a, 1)
            attend((2, 3), nothing)
        else:
            attend((0, 1, 2, 3), start_after)
        with jax.named_scope("tail1"):
            rise_ref[...] = jnp.zeros_like(rise_ref)
            batches(start_finish)
        recv_b[t, x, core, plane] = rise_ref[...].astype(BF16)
        with jax.named_scope("ship1"):
            g.first(2 + s, recv_b.at[t])

        if alone:
            with jax.named_scope("far1"):
                g.third_far(1, recv_a)

        with jax.named_scope("ship1"):
            load(send_z, t)
            spread(s, send_z, recv_z.at[me], t)

        return carry

    start_tile(0, 0, True)
    lax.fori_loop(1, xs, start_tile, 0)
    turn_weights(w2_ref, gb2_ref)
    recv_z[me] = send_z[me]

    def end_prepare(px):
        for span in both(px, run):
            zs_ref[span] = recv_z[span].astype(F32)
        places = both(px, 128)
        lanes = pl.ds(pl.multiple_of(px * tq, tq), tq)

        def columns(batch):
            z1 = [
                jnp.concatenate(
                    [
                        zs_ref[span, pl.ds(d, rows, stride=rows), :].reshape(128, ch)
                        for span in both(px, run)
                    ],
                    axis=0,
                )
                for d in batch
            ]
            normed = [layer_norm(v, g2_ref[...]) for v in z1]
            keys = [nn(v, w2_ref[:, ch : 2 * ch]).astype(BF16) for v in normed]
            queries = [(nt(wt_ref[:ch], v) * QSCALE).astype(BF16) for v in normed]
            values = [nt(wt_ref[2 * ch : 3 * ch], v).astype(BF16) for v in normed]
            for d, u, k, q, v in zip(batch, normed, keys, queries, values):
                q_ref[d, :, lanes] = q
                for e, span in enumerate(places):
                    part = slice(e * 128, (e + 1) * 128)
                    a_ref[d, span, :] = u[part]
                    k_ref[d, span, :] = k[part]
                    v_ref[d, :, span] = v[:, part]

        grouped(0, rows, columns, 4)

    with jax.named_scope("early"):
        for s in range(2):
            settle(s, step_blocks(recv_z, s), False)
        end_prepare(x)
        end_prepare(g.at(xs // 2))
    with jax.named_scope("rise2e"):
        rise_second(xs - 1)
    with jax.named_scope("rise3d"):
        rise_third(xs - 2)
    with jax.named_scope("waitz"):
        for s in range(2, xs):
            settle(s, step_blocks(recv_z, s), False)
    with jax.named_scope("late1"):
        end_prepare(g.at(1))
    with jax.named_scope("rise3e"):
        rise_third(xs - 1)
    with jax.named_scope("late2"):
        end_prepare(g.at(xs - 1))

    def rise_done(s, carry):
        g.handed(2 + s, 5, recv_b.at[tile_of(s, 0, True)], 0)
        g.handed(2 + s, 6, recv_b.at[tile_of(s, xs // 2, True)], xs // 2)
        g.handed(2 + s, 7, recv_b.at[tile_of(s, 1, True)], 1)
        g.handed(2 + s, 8, recv_b.at[tile_of(s, xs - 1, True)], xs - 1)
        return carry

    with jax.named_scope("handed"):
        lax.fori_loop(0, xs, rise_done, 0)

    def end_bias(t):
        def keys_of(b, carry):
            e, c = lax.rem(b // 2, 2), lax.rem(b, 2)
            keys = pl.ds(pl.multiple_of((e * 2 * xs + b // 4 * 2 + c) * 64, 64), 64)
            kc = kc_ref[keys, :]
            block = recv_b[t, b // 4, c, pl.ds(e * ny, ny)].astype(F32)
            for h in range(HEADS):
                part = block[:, h * rows : (h + 1) * rows, :].reshape(64, tq)
                for w in range(tq // 128):
                    to = slice(w * 128, (w + 1) * 128)
                    bias_ref[t, h, keys, to] = (part[:, to] + kc) * LOG2E
            return carry

        lax.fori_loop(0, 4 * xs, keys_of, 0)

    def end_tile(s, carry):
        t = tile_of(lax.rem(s + 1, xs))
        with jax.named_scope("biasb"):
            end_bias(t)

        def end_finish(batch):
            out = mixed(batch, t, ow2_ref)
            z1 = [
                jnp.concatenate(
                    [
                        zs_ref[span, pl.ds(r, rows, stride=rows), :].reshape(128, ch)
                        for span in both(t, run)
                    ],
                    axis=0,
                )
                for r in batch
            ]
            z2 = [(u + v).astype(BF16).astype(F32) for u, v in zip(z1, out)]
            normed = [layer_norm(v, g3_ref[...]) for v in z2]
            hid = [nn(v, ti_ref[...]) + tb_ref[...] for v in normed]
            hid = [jnp.maximum(v, 0.0).astype(BF16) for v in hid]
            last = [nn(v, to_ref[...]) for v in hid]
            for r, u, v in zip(batch, z2, last):
                stage_turned(r, u + v)

        with jax.named_scope("att2"):
            attend_tile(
                ck, rows, t, q_ref, k_ref, v_ref, bias_ref, s_ref, o_ref,
                lambda r: None, (0, 1, 2, 3),
            )
        with jax.named_scope("tail2"):
            batches(end_finish)
        with jax.named_scope("ship2"):
            load(send_o, t)
            spread(xs, send_o, mine, t)
        return carry

    lax.fori_loop(0, xs, end_tile, 0)
    with jax.named_scope("drain"):
        g.drain(0, recv_m)
        g.drain_split(1, recv_a)

        def drain_rise(s, carry):
            g.drain(2 + s, recv_b.at[tile_of(s)])
            return carry

        lax.fori_loop(0, xs, drain_rise, 0)
    with jax.named_scope("waito"):
        own = pltpu.make_async_copy(send_o.at[me], mine, zsem.at[xs + 1, 0])
        own.start()
        for s in range(xs):
            settle(s, step_blocks(send_z, s), True)
        settle(xs, send_o.at[pl.ds(0, n - 1)], True)
        settle(xs, out_ref.at[:, pl.ds(0, res - rows), :], False)
        own.wait()


def solution(mesh):
    nx, ny = mesh.shape["gx"], mesh.shape["gy"]
    n, xs = nx * ny, nx // 4

    def local(x, mask, g1, w1, gb1, bw1, ow1, g2, w2, gb2, bw2, ow2, g3, ti, tb, to):
        rows, res, ch = x.shape
        tq, ck = res // xs, 512
        vmem = pl.BlockSpec(memory_space=pltpu.VMEM)
        row = lambda t: t.reshape(1, -1)
        return pl.pallas_call(
            functools.partial(kernel, nx, ny, ck, min(rows, 4)),
            out_shape=jax.ShapeDtypeStruct(x.shape, x.dtype),
            in_specs=[vmem, pl.BlockSpec(memory_space=pltpu.SMEM)] + [vmem] * 14,
            out_specs=pl.BlockSpec(memory_space=pl.ANY),
            scratch_shapes=[
                pltpu.VMEM((rows, ch, res), BF16),
                pltpu.VMEM((rows, res, ch), BF16),
                pltpu.VMEM((rows, ch, res), BF16),
                pltpu.VMEM((4 * ch, ch), BF16),
                pltpu.VMEM((xs, HEADS, res, tq), F32),
                pltpu.VMEM((1, res), F32),
                pltpu.VMEM((res, 128), F32),
                pltpu.VMEM((n, rows * rows, ch), F32),
                pltpu.VMEM((tq // rows, rows * rows, ch), F32),
                pltpu.VMEM((HEADS * rows, tq), F32),
                pltpu.VMEM((HEADS * rows, res), F32),
                pltpu.VMEM((ch, tq), F32),
                pltpu.VMEM((2 * res, tq), F32),
                pltpu.VMEM((rows, ch, tq), F32),
                pltpu.VMEM((xs, 2, 2 * ny, 16, 128), BF16),
                pltpu.VMEM((xs, 2, 2 * ny, HEADS * rows, res), BF16),
                pltpu.VMEM((xs, xs, 2, 2 * ny, HEADS * rows, tq), BF16),
                pltpu.VMEM((n, rows * rows, ch), BF16),
                pltpu.VMEM((n, rows * rows, ch), BF16),
                pltpu.VMEM((n, rows, rows, ch), BF16),
                pltpu.VMEM((rows, res, ch), BF16),
                pltpu.SemaphoreType.DMA((2 + xs, 13)),
                pltpu.SemaphoreType.DMA((2 + xs, 13)),
                pltpu.SemaphoreType.DMA((2 + xs, 2)),
            ],
            compiler_params=pltpu.CompilerParams(
                collective_id=0, has_side_effects=True, vmem_limit_bytes=67_043_328,
            ),
        )(
            x, mask, row(g1), w1, row(gb1), bw1.T, ow1, row(g2), w2,
            row(gb2), bw2.T, ow2, row(g3), ti, row(tb), to,
        )

    placed = (P(("gx", "gy"), None, None), P(("gx", "gy"))) + (P(),) * 14
    return jax.shard_map(
        local, mesh=mesh, in_specs=placed, out_specs=P(("gx", "gy"), None, None), check_vma=False
    )
```

```python
import functools
import math

import jax
import jax.numpy as jnp
from jax import lax
from jax.experimental import pallas as pl
from jax.experimental.pallas import tpu as pltpu
from jax.sharding import PartitionSpec as P

HEADS = 4
HEAD_DIM = 32
BIG = 1000000000.0
LOG2E = math.log2(math.e)
QSCALE = HEAD_DIM ** (-0.5) * LOG2E
MESH = pl.DeviceIdType.MESH
F32 = jnp.float32
BF16 = jnp.bfloat16


def nn(a, b):
    return lax.dot_general(a, b, (((1,), (0,)), ((), ())), preferred_element_type=F32)


def nt(a, b):
    return lax.dot_general(a, b, (((1,), (1,)), ((), ())), preferred_element_type=F32)


def layer_norm(x, gain):
    mean = jnp.mean(x, axis=-1, keepdims=True)
    cent = x - mean
    var = jnp.mean(cent * cent, axis=-1, keepdims=True)
    return (cent * lax.rsqrt(var + 1e-05) * gain).astype(BF16)


def bias_rows(w, r, rows, normed):
    shape = (HEADS * rows, HEADS)
    place = lax.broadcasted_iota(jnp.int32, shape, 0) == (
        lax.broadcasted_iota(jnp.int32, shape, 1) * rows + r
    )
    spread = nn(place.astype(F32).astype(BF16), w).astype(BF16)
    return nt(spread, normed)


def attend_tile(ck, group, t, q_ref, k_ref, v_ref, bias_ref, s_ref, o_ref, after, heads):
    rows, res, ch = k_ref.shape
    pairs = len(heads)
    tq = s_ref.shape[1]
    s_refs = [s_ref.at[:res], s_ref.at[res:]]
    lanes = pl.ds(pl.multiple_of(t * tq, tq), tq)
    chunks = res // ck

    def query(r, h):
        q = q_ref[r, :, lanes]
        row = lax.broadcasted_iota(jnp.int32, q.shape, 0)
        return jnp.where((row >= h * HEAD_DIM) & (row < (h + 1) * HEAD_DIM), q, jnp.zeros_like(q))

    def score(r, h, c, q, top):
        span = slice(c * ck, (c + 1) * ck)
        s = nn(k_ref[r, span, :], q) + bias_ref[t, h, span, :]
        s_refs[h % 2][span, :] = s
        m = jnp.max(s.reshape(ck // 8, 8, tq), axis=0)
        return m if top is None else jnp.maximum(top, m)

    def mix(r, h, c, top, acc):
        span = slice(c * ck, (c + 1) * ck)
        w = jnp.exp2((s_refs[h % 2][span, :] - top).astype(BF16))
        v = jnp.concatenate(
            [v_ref[r, h * HEAD_DIM : (h + 1) * HEAD_DIM, span], jnp.ones((16, ck), BF16)], axis=0
        )
        o = nn(v, w)
        return o if acc is None else acc + o

    q, top = query(0, heads[0]), None
    for c in range(chunks):
        top = score(0, heads[0], c, q, top)

    def row(r, top):
        outs = []
        for at, h in enumerate(heads):
            peak = jnp.max(top, axis=0, keepdims=True)
            nh = heads[(at + 1) % pairs]
            nr = r if at < pairs - 1 else jnp.minimum(r + 1, rows - 1)
            q, top, acc = query(nr, nh), None, None
            for c in range(chunks):
                top = score(nr, nh, c, q, top)
                acc = mix(r, h, c, peak, acc)
            outs.append(acc[:HEAD_DIM] / acc[HEAD_DIM : HEAD_DIM + 1])
        span = slice(heads[0] * HEAD_DIM, (heads[-1] + 1) * HEAD_DIM)
        o_ref[r, span, :] = jnp.concatenate(outs, axis=0)
        return top

    def body(i, top):
        for e in range(group):
            top = row(i * group + e, top)
        after(i)
        return top

    lax.fori_loop(0, rows // group, body, top)


class Gather:
    def __init__(self, place, ssem, rsem):
        self.place, self.ssem, self.rsem = place, ssem, rsem

    def copy(self, inst, kind, src, dst, to):
        return pltpu.make_async_remote_copy(
            src_ref=src,
            dst_ref=dst,
            send_sem=self.ssem.at[inst, kind],
            recv_sem=self.rsem.at[inst, kind],
            device_id=self.place(*to),
            device_id_type=MESH,
        )

    def setup(self, me, sizes):
        self.x, self.core, self.plane = me
        self.xs, self.planes = sizes
        self.other = 1 - self.core

    def at(self, step):
        return lax.rem(self.x + step, self.xs)

    def fan(self, inst, kind, slot):
        @pl.loop(1, self.planes)
        def _(u):
            p = lax.rem(self.plane + u, self.planes)
            self.copy(inst, kind, slot, slot, (self.x, self.core, p)).start()

    def fanned(self, inst, kind, buf):
        rest = buf.at[self.x, self.core, pl.ds(0, self.planes - 1)]
        return self.copy(inst, kind, rest, rest, (self.x, self.other, self.plane))

    def line(self, inst, kind, buf, step):
        part = buf.at[self.x, self.core]
        return self.copy(inst, kind, part, part, (self.at(step), self.core, self.plane))

    def hand(self, inst, kind, buf, step, core=None):
        part = buf.at[self.at(step), self.core if core is None else core]
        return self.copy(inst, kind, part, part, (self.x, self.other, self.plane))

    def far(self, inst, slot):
        half = self.xs // 2
        return self.copy(inst, 1, slot, slot, (self.at(half), self.core, self.plane))

    def first(self, inst, buf):
        slot = buf.at[self.x, self.core, self.plane]
        self.far(inst, slot).start()
        self.fan(inst, 0, slot)

    def halves(self, buf, planes):
        half = buf.shape[3] // 2
        return [buf.at[self.x, self.core, planes, pl.ds(e * half, half)] for e in range(2)]

    def piece(self, inst, kind, part):
        return self.copy(inst, kind, part, part, (self.x, self.other, self.plane))

    def first_upper(self, inst, buf):
        self.fan(inst, 0, self.halves(buf, self.plane)[0])
        self.far(inst, buf.at[self.x, self.core, self.plane]).start()

    def first_lower(self, inst, buf):
        self.fan(inst, 10, self.halves(buf, self.plane)[1])
        slot = buf.at[self.at(self.xs // 2), self.core, self.plane]
        self.far(inst, slot).wait_recv()
        self.fan(inst, 2, slot)

    def split_one(self, inst, buf):
        self.piece(inst, 0, self.halves(buf, pl.ds(0, self.planes - 1))[0]).wait_recv()
        upper = self.halves(buf, pl.ds(0, self.planes))[0]
        self.piece(inst, 9, upper).start()
        self.line_part(inst, 3, upper, 1).start()
        self.line_part(inst, 4, upper, self.xs - 1).start()

    def line_part(self, inst, kind, part, step):
        return self.copy(inst, kind, part, part, (self.at(step), self.core, self.plane))

    def split_two(self, inst, buf):
        self.piece(inst, 10, self.halves(buf, pl.ds(0, self.planes - 1))[1]).wait_recv()
        lower = self.halves(buf, pl.ds(0, self.planes))[1]
        self.piece(inst, 5, lower).start()
        self.line_part(inst, 11, lower, 1).start()
        self.line_part(inst, 12, lower, self.xs - 1).start()

    def handed_half(self, inst, kind, buf, e):
        half = buf.shape[3] // 2
        part = buf.at[self.x, self.other, :, pl.ds(e * half, half)]
        self.piece(inst, kind, part).wait_recv()

    def drain_split(self, inst, buf):
        self.far(inst, buf.at[self.x, self.core, self.plane]).wait_send()
        for e, (fan, hand) in enumerate(((0, 9), (10, 5))):
            self.piece(inst, fan, self.halves(buf, pl.ds(0, self.planes - 1))[e]).wait_send()
            self.piece(inst, hand, self.halves(buf, pl.ds(0, self.planes))[e]).wait_send()
        self.fanned(inst, 2, buf).wait_send()
        for e, part in enumerate(self.halves(buf, pl.ds(0, self.planes))):
            self.line_part(inst, 3 + 8 * e, part, 1).wait_send()
            self.line_part(inst, 4 + 8 * e, part, 1).wait_send()
        for kind in (6, 7, 8):
            self.hand(inst, kind, buf, 0).wait_send()

    def second(self, inst, buf, buf_far):
        slot = buf_far.at[self.at(self.xs // 2), self.core, self.plane]
        self.far(inst, slot).wait_recv()
        self.fan(inst, 2, slot)
        self.fanned(inst, 0, buf).wait_recv()
        self.hand(inst, 5, buf, 0).start()
        self.line(inst, 3, buf, 1).start()
        self.line(inst, 4, buf, self.xs - 1).start()

    def third_far(self, inst, buf_far):
        self.fanned(inst, 2, buf_far).wait_recv()
        self.hand(inst, 6, buf_far, self.xs // 2).start()

    def third_near(self, inst, buf_of):
        for step in (1 + self.other * (self.xs - 2), 1 + self.core * (self.xs - 2)):
            down = (step - 1) // (self.xs - 2)
            buf = buf_of(step)
            self.line(inst, 4 - down, buf, 1).wait_recv()
            self.hand(inst, 7 + down, buf, step).start()

    def third_near_split(self, inst, buf):
        for step in (1 + self.other * (self.xs - 2), 1 + self.core * (self.xs - 2)):
            down = (step - 1) // (self.xs - 2)
            for e, part in enumerate(self.halves(buf, pl.ds(0, self.planes))):
                self.line_part(inst, 4 + 8 * e - down, part, 1).wait_recv()
            self.hand(inst, 7 + down, buf, step).start()

    def handed(self, inst, kind, buf, step):
        self.hand(inst, kind, buf, step, self.other).wait_recv()

    def drain(self, inst, buf):
        slot = buf.at[self.x, self.core, self.plane]
        self.far(inst, slot).wait_send()
        self.fanned(inst, 0, buf).wait_send()
        self.fanned(inst, 2, buf).wait_send()
        self.line(inst, 3, buf, 1).wait_send()
        self.line(inst, 4, buf, 1).wait_send()
        for kind in (5, 6, 7, 8):
            self.hand(inst, kind, buf, 0).wait_send()


def kernel(
    nx,
    ny,
    ck,
    group,
    x_ref,
    mask_ref,
    g1_ref,
    w1_ref,
    gb1_ref,
    bw1_ref,
    ow1_ref,
    g2_ref,
    w2_ref,
    gb2_ref,
    bw2_ref,
    ow2_ref,
    g3_ref,
    ti_ref,
    tb_ref,
    to_ref,
    out_ref,
    q_ref,
    k_ref,
    v_ref,
    wt_ref,
    bias_ref,
    kb_ref,
    kc_ref,
    zs_ref,
    st_ref,
    rise_ref,
    first_ref,
    gc_ref,
    s_ref,
    o_ref,
    recv_m,
    recv_a,
    recv_b,
    send_z,
    recv_z,
    send_o,
    a_ref,
    ssem,
    rsem,
    zsem,
):
    n = nx * ny
    xs, planes = nx // 4, 2 * ny
    rows, res, ch = x_ref.shape
    tq = res // xs
    gx, gy = lax.axis_index("gx"), lax.axis_index("gy")
    me = gx * ny + gy
    core = lax.rem(gx, 2)
    x = lax.rem(gx // 2, xs)
    low = gx // (2 * xs)
    plane = low * ny + gy
    run = 2 * ny

    def place(x, core, plane):
        return (plane // ny * (2 * xs) + x * 2 + core, lax.rem(plane, ny))

    g = Gather(place, ssem, rsem)
    g.setup((x, core, plane), (xs, planes))
    barrier = pltpu.get_barrier_semaphore()

    def greet(*to):
        pl.semaphore_signal(barrier, inc=1, device_id=place(*to), device_id_type=MESH)

    for u in range(1, planes):
        greet(x, core, lax.rem(plane + u, planes))
    for u in range(1, xs):
        greet(g.at(u), core, plane)
    greet(x, 1 - core, plane)

    lane = lax.broadcasted_iota(jnp.int32, (16, 128), 1)
    vec = jnp.zeros((16, 128), F32)
    for t in range(rows):
        vec = jnp.where(lane == lax.rem(me * rows, 128) + t, mask_ref[t].astype(F32), vec)
    recv_m[x, core, plane] = vec.astype(BF16)


    def grouped(lo, hi, fn, size=2):
        def step(i, carry):
            fn([lo + i * size + e for e in range(size)])
            return carry

        lax.fori_loop(0, (hi - lo) // size, step, 0)

    def start_norm(batch):
        normed = [layer_norm(v.astype(F32), g1_ref[...]) for v in [x_ref[r] for r in batch]]
        for r, v in zip(batch, normed):
            a_ref[r] = v
        part = [bias_rows(bw1_ref[...], r, rows, v) for r, v in zip(batch, normed)]
        first_ref[...] = first_ref[...] + sum(part[1:], part[0])

    with jax.named_scope("norm"):
        first_ref[...] = jnp.zeros_like(first_ref)
        grouped(0, rows, start_norm)
        recv_a[x, core, plane] = first_ref[...].astype(BF16)

    with jax.named_scope("barrier"):
        pl.semaphore_wait(barrier, planes - 1 + xs - 1 + 1)
    g.first(0, recv_m)
    g.first_upper(1, recv_a)
    def turn_weights(w_ref, gb_ref):
        wt_ref[...] = w_ref[...].astype(F32).T.astype(BF16)
        column = jnp.broadcast_to(gb_ref[...], (128, ch)).T
        for b in range(tq // 128):
            gc_ref[:, b * 128 : (b + 1) * 128] = column

    def project(batch, w_ref):
        normed = [a_ref[r] for r in batch]
        for r, v in zip(batch, [nn(v, w_ref[:, ch : 2 * ch]) for v in normed]):
            k_ref[r] = v.astype(BF16)
        for r, v in zip(batch, [nt(wt_ref[:ch], v) for v in normed]):
            q = (v * QSCALE).astype(BF16)
            for b in range(2 * xs):
                to = (b % xs * 2 + b // xs) * 128
                q_ref[r, :, to : to + 128] = q[:, b * 128 : (b + 1) * 128]
        for r, v in zip(batch, [nt(wt_ref[2 * ch : 3 * ch], v) for v in normed]):
            v_ref[r] = v.astype(BF16)

    def both(t, size):
        return [pl.ds(pl.multiple_of((t + e * xs) * size, size), size) for e in range(2)]

    def mixed(batch, t, ow_ref):
        a = [jnp.concatenate([a_ref[r, span, :] for span in both(t, 128)], axis=0) for r in batch]
        gl = [nt(wt_ref[3 * ch :], v) for v in a]
        gated = [o_ref[r] * jax.nn.sigmoid(v + gc_ref[...]) for r, v in zip(batch, gl)]
        gated = [v.T.astype(BF16) for v in gated]
        return [nn(v, ow_ref[...]) for v in gated]

    def batches(fn):
        def run(i, carry):
            fn([i * 8 + e for e in range(8)])
            return carry

        lax.fori_loop(0, rows // 8, run, 0)

    turn_weights(w1_ref, gb1_ref)

    with jax.named_scope("project"):
        grouped(0, rows, lambda batch: project(batch, w1_ref))
    with jax.named_scope("mask2"):
        g.second(0, recv_m, recv_m)
    with jax.named_scope("lower"):
        g.first_lower(1, recv_a)
    with jax.named_scope("mask3"):
        g.third_far(0, recv_m)
        g.third_near(0, lambda step: recv_m)
    with jax.named_scope("a2"):
        g.split_one(1, recv_a)
    with jax.named_scope("mask4"):
        g.handed(0, 5, recv_m, 0)
        g.handed(0, 6, recv_m, xs // 2)
        g.handed(0, 7, recv_m, 1)
        g.handed(0, 8, recv_m, xs - 1)

    for b in range(2 * xs):
        part = recv_m[b % xs, :, b // xs * ny : (b // xs + 1) * ny].astype(F32)
        mask = jnp.sum(jnp.sum(part, axis=0), axis=0)[:1]
        kb = (mask - 1.0) * BIG
        kb_ref[:, b * 128 : (b + 1) * 128] = kb
        kc_ref[b * 128 : (b + 1) * 128, :] = jnp.broadcast_to(kb, (128, 128)).T

    def start_bias(t, heads):
        for e in range(2):
            lo, hi = heads[0] * rows, (heads[-1] + 1) * rows
            blocks = [
                recv_a[t, c, e * ny : (e + 1) * ny, lo:hi].astype(F32) for c in range(2)
            ]
            for h in heads:
                part = jnp.concatenate(
                    [
                        b[:, h * rows - lo : (h + 1) * rows - lo, :].reshape(64, res)
                        for b in blocks
                    ], axis=0
                )
                to = slice(e * 128, (e + 1) * 128)
                bias_ref[t, h, :, to] = ((part + kb_ref[...]) * LOG2E).T

    def stage(r, z):
        st_ref[:, pl.ds(pl.multiple_of(r * rows, rows), rows), :] = z.reshape(
            tq // rows, rows, ch
        )

    def stage_turned(r, z):
        st_ref[:, pl.ds(r, rows, stride=rows), :] = z.reshape(tq // rows, rows, ch)

    mine = out_ref.at[:, pl.ds(pl.multiple_of(me * rows, rows), rows), :]

    def load(src, t):
        for e, span in enumerate(both(t, run)):
            src[span] = st_ref[e * run : (e + 1) * run].astype(BF16).reshape(run, *src.shape[1:])

    def spread(kind, src, dst, t):
        def send(v):
            c, p = lax.rem(v, 2), v // 2
            to = place(t, c, p)
            d = to[0] * ny + to[1]
            return pltpu.make_async_remote_copy(
                src_ref=src.at[d],
                dst_ref=dst,
                send_sem=zsem.at[kind, 0],
                recv_sem=zsem.at[kind, 1],
                device_id=to,
                device_id_type=MESH,
            )

        here = plane * 2 + core

        own = jnp.where(t == x, 1, 0)

        def some(i, carry):
            for e in range(4):
                send(lax.rem(here + own + i * 4 + e, 2 * run)).start()
            return carry

        @pl.when(t != x)
        def _():
            lax.fori_loop(0, 2 * run // 4, some, 0)

        @pl.when(t == x)
        def _():
            lax.fori_loop(0, 2 * run // 4 - 1, some, 0)
            for u in range(2 * run - 4, 2 * run - 1):
                send(lax.rem(here + 1 + u, 2 * run)).start()

    def settle(kind, part, sent):
        copy = pltpu.make_async_remote_copy(
            src_ref=part,
            dst_ref=part,
            send_sem=zsem.at[kind, 0],
            recv_sem=zsem.at[kind, 1],
            device_id=place(x, 1 - core, plane),
            device_id_type=MESH,
        )
        copy.wait_send() if sent else copy.wait_recv()

    def step_blocks(buf, s):
        return buf.at[pl.ds(0, 2 * run - (1 if s == 0 else 0))]

    near = 1 + core * (xs - 2)

    def tile_of(s, step=0, swap=False):
        side = xs - near if swap else near
        away = jnp.where(s == 0, 0, jnp.where(s == 1, xs // 2, jnp.where(s == 2, side, xs - side)))
        return lax.rem(x + step + away, xs)

    def rise_second(s):
        t = tile_of(s)
        g.second(2 + s, recv_b.at[t], recv_b.at[tile_of(s, xs // 2)])

    def rise_third(s):
        g.third_far(2 + s, recv_b.at[tile_of(s, xs // 2)])
        g.third_near(2 + s, lambda step: recv_b.at[tile_of(s, step)])

    def start_tile(s, carry, alone=False):
        t = tile_of(s)

        @pl.when(s == 1)
        def _():
            with jax.named_scope("wait1"):
                g.handed(1, 6, recv_a, xs // 2)

        @pl.when(s == 2)
        def _():
            with jax.named_scope("wait2"):
                g.handed(1, 7 + core, recv_a, near)

        @pl.when(s == 3)
        def _():
            with jax.named_scope("wait3"):
                g.handed(1, 8 - core, recv_a, xs - near)

        def attend(heads, after):
            with jax.named_scope("biasa"):
                start_bias(t, heads)
            with jax.named_scope("att1"):
                attend_tile(
                    ck, 2 if alone else group, t, q_ref, k_ref, v_ref, bias_ref, s_ref, o_ref, after, heads
                )

        def start_finish(batch):
            out = mixed(batch, t, ow1_ref)
            old = [jnp.concatenate([x_ref[r, p, :] for p in both(t, 128)], axis=0) for r in batch]
            z1 = [(u.astype(F32) + v).astype(BF16).astype(F32) for u, v in zip(old, out)]
            for r, v in zip(batch, z1):
                stage(r, v)
            normed = [layer_norm(v, g2_ref[...]) for v in z1]
            part = [bias_rows(bw2_ref[...], r, rows, v) for r, v in zip(batch, normed)]
            rise_ref[...] = rise_ref[...] + sum(part[1:], part[0])

        def start_after(i):
            @pl.when((s == 1) & (i == rows // group - 1))
            def _():
                with jax.named_scope("near1"):
                    g.third_near_split(1, recv_a)

            @pl.when((s > 0) & (i == 0))
            def _():
                with jax.named_scope("rise2"):
                    rise_second(s - 1)

            @pl.when((s > 1) & (i == rows // group - 1))
            def _():
                with jax.named_scope("rise3"):
                    rise_third(s - 2)

        if alone:
            nothing = lambda i: None
            with jax.named_scope("wait0"):
                g.handed_half(1, 9, recv_a, 0)
            attend((0, 1), nothing)
            with jax.named_scope("a3"):
                g.split_two(1, recv_a)
                g.handed_half(1, 5, recv_a, 1)
            attend((2, 3), nothing)
        else:
            attend((0, 1, 2, 3), start_after)
        with jax.named_scope("tail1"):
            rise_ref[...] = jnp.zeros_like(rise_ref)
            batches(start_finish)
        recv_b[t, x, core, plane] = rise_ref[...].astype(BF16)
        with jax.named_scope("ship1"):
            g.first(2 + s, recv_b.at[t])

        if alone:
            with jax.named_scope("far1"):
                g.third_far(1, recv_a)

        with jax.named_scope("ship1"):
            load(send_z, t)
            spread(s, send_z, recv_z.at[me], t)

        return carry

    start_tile(0, 0, True)
    lax.fori_loop(1, xs, start_tile, 0)
    turn_weights(w2_ref, gb2_ref)
    recv_z[me] = send_z[me]

    def end_prepare(px):
        for span in both(px, run):
            zs_ref[span] = recv_z[span].astype(F32)
        places = both(px, 128)
        lanes = pl.ds(pl.multiple_of(px * tq, tq), tq)

        def columns(batch):
            z1 = [
                jnp.concatenate(
                    [
                        zs_ref[span, pl.ds(d, rows, stride=rows), :].reshape(128, ch)
                        for span in both(px, run)
                    ],
                    axis=0,
                )
                for d in batch
            ]
            normed = [layer_norm(v, g2_ref[...]) for v in z1]
            keys = [nn(v, w2_ref[:, ch : 2 * ch]).astype(BF16) for v in normed]
            queries = [(nt(wt_ref[:ch], v) * QSCALE).astype(BF16) for v in normed]
            values = [nt(wt_ref[2 * ch : 3 * ch], v).astype(BF16) for v in normed]
            for d, u, k, q, v in zip(batch, normed, keys, queries, values):
                q_ref[d, :, lanes] = q
                for e, span in enumerate(places):
                    part = slice(e * 128, (e + 1) * 128)
                    a_ref[d, span, :] = u[part]
                    k_ref[d, span, :] = k[part]
                    v_ref[d, :, span] = v[:, part]

        grouped(0, rows, columns, 4)

    with jax.named_scope("early"):
        for s in range(2):
            settle(s, step_blocks(recv_z, s), False)
        end_prepare(x)
        end_prepare(g.at(xs // 2))
    with jax.named_scope("rise2e"):
        rise_second(xs - 1)
    with jax.named_scope("rise3d"):
        rise_third(xs - 2)
    with jax.named_scope("waitz"):
        for s in range(2, xs):
            settle(s, step_blocks(recv_z, s), False)
    with jax.named_scope("late1"):
        end_prepare(g.at(1))
    with jax.named_scope("rise3e"):
        rise_third(xs - 1)
    with jax.named_scope("late2"):
        end_prepare(g.at(xs - 1))

    def rise_done(s, carry):
        g.handed(2 + s, 5, recv_b.at[tile_of(s, 0, True)], 0)
        g.handed(2 + s, 6, recv_b.at[tile_of(s, xs // 2, True)], xs // 2)
        g.handed(2 + s, 7, recv_b.at[tile_of(s, 1, True)], 1)
        g.handed(2 + s, 8, recv_b.at[tile_of(s, xs - 1, True)], xs - 1)
        return carry

    with jax.named_scope("handed"):
        lax.fori_loop(0, xs, rise_done, 0)

    def end_bias(t):
        def keys_of(b, carry):
            e, c = lax.rem(b // 2, 2), lax.rem(b, 2)
            keys = pl.ds(pl.multiple_of((e * 2 * xs + b // 4 * 2 + c) * 64, 64), 64)
            kc = kc_ref[keys, :]
            block = recv_b[t, b // 4, c, pl.ds(e * ny, ny)].astype(F32)
            for h in range(HEADS):
                part = block[:, h * rows : (h + 1) * rows, :].reshape(64, tq)
                for w in range(tq // 128):
                    to = slice(w * 128, (w + 1) * 128)
                    bias_ref[t, h, keys, to] = (part[:, to] + kc) * LOG2E
            return carry

        lax.fori_loop(0, 4 * xs, keys_of, 0)

    def end_tile(s, carry):
        t = tile_of(lax.rem(s + 1, xs))
        with jax.named_scope("biasb"):
            end_bias(t)

        def end_finish(batch):
            out = mixed(batch, t, ow2_ref)
            z1 = [
                jnp.concatenate(
                    [
                        zs_ref[span, pl.ds(r, rows, stride=rows), :].reshape(128, ch)
                        for span in both(t, run)
                    ],
                    axis=0,
                )
                for r in batch
            ]
            z2 = [(u + v).astype(BF16).astype(F32) for u, v in zip(z1, out)]
            normed = [layer_norm(v, g3_ref[...]) for v in z2]
            hid = [nn(v, ti_ref[...]) + tb_ref[...] for v in normed]
            hid = [jnp.maximum(v, 0.0).astype(BF16) for v in hid]
            last = [nn(v, to_ref[...]) for v in hid]
            for r, u, v in zip(batch, z2, last):
                stage_turned(r, u + v)

        with jax.named_scope("att2"):
            attend_tile(
                ck, group, t, q_ref, k_ref, v_ref, bias_ref, s_ref, o_ref,
                lambda r: None, (0, 1, 2, 3),
            )
        with jax.named_scope("tail2"):
            batches(end_finish)
        with jax.named_scope("ship2"):
            load(send_o, t)
            spread(xs, send_o, mine, t)
        return carry

    lax.fori_loop(0, xs, end_tile, 0)
    with jax.named_scope("drain"):
        g.drain(0, recv_m)
        g.drain_split(1, recv_a)

        def drain_rise(s, carry):
            g.drain(2 + s, recv_b.at[tile_of(s)])
            return carry

        lax.fori_loop(0, xs, drain_rise, 0)
    with jax.named_scope("waito"):
        own = pltpu.make_async_copy(send_o.at[me], mine, zsem.at[xs + 1, 0])
        own.start()
        for s in range(xs):
            settle(s, step_blocks(send_z, s), True)
        settle(xs, send_o.at[pl.ds(0, n - 1)], True)
        settle(xs, out_ref.at[:, pl.ds(0, res - rows), :], False)
        own.wait()


def solution(mesh):
    nx, ny = mesh.shape["gx"], mesh.shape["gy"]
    n, xs = nx * ny, nx // 4

    def local(x, mask, g1, w1, gb1, bw1, ow1, g2, w2, gb2, bw2, ow2, g3, ti, tb, to):
        rows, res, ch = x.shape
        tq, ck = res // xs, 512
        vmem = pl.BlockSpec(memory_space=pltpu.VMEM)
        row = lambda t: t.reshape(1, -1)
        return pl.pallas_call(
            functools.partial(kernel, nx, ny, ck, min(rows, 4)),
            out_shape=jax.ShapeDtypeStruct(x.shape, x.dtype),
            in_specs=[vmem, pl.BlockSpec(memory_space=pltpu.SMEM)] + [vmem] * 14,
            out_specs=pl.BlockSpec(memory_space=pl.ANY),
            scratch_shapes=[
                pltpu.VMEM((rows, ch, res), BF16),
                pltpu.VMEM((rows, res, ch), BF16),
                pltpu.VMEM((rows, ch, res), BF16),
                pltpu.VMEM((4 * ch, ch), BF16),
                pltpu.VMEM((xs, HEADS, res, tq), F32),
                pltpu.VMEM((1, res), F32),
                pltpu.VMEM((res, 128), F32),
                pltpu.VMEM((n, rows * rows, ch), F32),
                pltpu.VMEM((tq // rows, rows * rows, ch), F32),
                pltpu.VMEM((HEADS * rows, tq), F32),
                pltpu.VMEM((HEADS * rows, res), F32),
                pltpu.VMEM((ch, tq), F32),
                pltpu.VMEM((2 * res, tq), F32),
                pltpu.VMEM((rows, ch, tq), F32),
                pltpu.VMEM((xs, 2, 2 * ny, 16, 128), BF16),
                pltpu.VMEM((xs, 2, 2 * ny, HEADS * rows, res), BF16),
                pltpu.VMEM((xs, xs, 2, 2 * ny, HEADS * rows, tq), BF16),
                pltpu.VMEM((n, rows * rows, ch), BF16),
                pltpu.VMEM((n, rows * rows, ch), BF16),
                pltpu.VMEM((n, rows, rows, ch), BF16),
                pltpu.VMEM((rows, res, ch), BF16),
                pltpu.SemaphoreType.DMA((2 + xs, 13)),
                pltpu.SemaphoreType.DMA((2 + xs, 13)),
                pltpu.SemaphoreType.DMA((2 + xs, 2)),
            ],
            compiler_params=pltpu.CompilerParams(
                collective_id=0, has_side_effects=True, vmem_limit_bytes=67_043_328,
            ),
        )(
            x, mask, row(g1), w1, row(gb1), bw1.T, ow1, row(g2), w2,
            row(gb2), bw2.T, ow2, row(g3), ti, row(tb), to,
        )

    placed = (P(("gx", "gy"), None, None), P(("gx", "gy"))) + (P(),) * 14
    return jax.shard_map(
        local, mesh=mesh, in_specs=placed, out_specs=P(("gx", "gy"), None, None), check_vma=False
    )
```
